32 devices in a mesh: dp: 2 (over x), tp: 16 (over z, y, core).
Axes of the slice: x: 2, y: 2, z: 4, core: 2. Of those that a mesh axis runs over, the one named last changes fastest.
Arguments:
- x: bfloat16 [16, 384, 2048], P('dp', 'tp'), parts along dimension 0
- k_cache: bfloat16 [16, 4096, 16, 128], P('dp', None, 'tp'), parts along dimension 0
- v_cache: bfloat16 [16, 4096, 16, 128], P('dp', None, 'tp'), parts along dimension 0
- prefix_len: int32 [16], P('dp'), parts along dimension 0
- valid_len: int32 [16], P('dp'), parts along dimension 0
- g_attn: bfloat16 [2048], replicated
- w_q: bfloat16 [2048, 2048], P(None, 'tp')
- b_q: bfloat16 [2048], P('tp')
- w_k: bfloat16 [2048, 2048], P(None, 'tp')
- b_k: bfloat16 [2048], P('tp')
- w_v: bfloat16 [2048, 2048], P(None, 'tp')
- b_v: bfloat16 [2048], P('tp')
- w_o: bfloat16 [2048, 2048], P('tp')
- g_mlp: bfloat16 [2048], replicated
- w_gate: bfloat16 [2048, 5504], P(None, 'tp')
- w_up: bfloat16 [2048, 5504], P(None, 'tp')
- w_down: bfloat16 [5504, 2048], P('tp')
Outputs:
- output 1: bfloat16 [16, 384, 2048], P('dp', 'tp'), parts along dimension 0
- output 2: bfloat16 [16, 4096, 16, 128], P('dp', None, 'tp'), parts along dimension 0
- output 3: bfloat16 [16, 4096, 16, 128], P('dp', None, 'tp'), parts along dimension 0
There are 2 independent parts. The reference program is written for one: setup_inputs(seed, part) draws one part's arguments, and reference() takes and returns one part's arrays. A program takes and returns all parts, laid end to end along the dimension named above; an argument that names none is the same for every part.
All inputs are finite; a program needn't handle non-finite values.
Results may differ from the reference program's by a relative error of at most 0.0189305.
Values are sent between devices in bfloat16 or wider.
A program may use at most 1 GiB of HBM per device.

```python
import jax
import jax.numpy as jnp
from jax import lax

REQUESTS = 8
CHUNK_LEN = 384
CACHE_SLOTS = 4096
MODEL_DIM = 2048
NUM_HEADS = 16
KV_HEADS = 16
KV_STORE = 16
HEAD_DIM = 128
FFN_DIM = 5504

ROPE_THETA = 1.0e6
NORM_EPS = 1.0e-6
GROUP_SIZE = NUM_HEADS // KV_STORE
KV_REPEAT = KV_STORE // KV_HEADS


def draw_lengths(key):
    keys = jax.random.split(key, 4)
    prefix = jax.random.randint(keys[0], (REQUESTS,), 0, CACHE_SLOTS - CHUNK_LEN + 1)
    valid = jax.random.randint(keys[1], (REQUESTS,), 1, CHUNK_LEN + 1)
    req_ids = jnp.arange(REQUESTS)
    longest = jax.random.randint(keys[2], (), 0, REQUESTS)
    fullest = jax.random.randint(keys[3], (), 0, REQUESTS)
    prefix = jnp.where(req_ids == longest, CACHE_SLOTS - CHUNK_LEN, prefix)
    valid = jnp.where(req_ids == fullest, CHUNK_LEN, valid)
    return prefix.astype(jnp.int32), valid.astype(jnp.int32)


def gauss(key, shape, scale):
    return jax.random.normal(key, shape, jnp.float32) * scale


def kv_copies(values, axis):
    return jnp.repeat(values, KV_REPEAT, axis=axis)


def setup_inputs(seed: int = 0, part: int = 0) -> dict:
    shared = jax.random.split(jax.random.key(seed), 12)
    local = jax.random.split(jax.random.fold_in(jax.random.key(seed + 1), part), 5)
    prefix, valid = draw_lengths(local[0])
    q_cols = NUM_HEADS * HEAD_DIM
    kv_cols = KV_STORE * HEAD_DIM
    hidden = gauss(local[1], (REQUESTS, CHUNK_LEN, MODEL_DIM), 1.0)
    k_cache = kv_copies(gauss(local[2], (REQUESTS, CACHE_SLOTS, KV_HEADS, HEAD_DIM), 1.0), 2)
    v_mean = gauss(local[3], (REQUESTS, 1, KV_HEADS, HEAD_DIM), 1.0)
    v_cache = kv_copies(v_mean + gauss(local[4], (REQUESTS, CACHE_SLOTS, KV_HEADS, HEAD_DIM), 1.5), 2)
    w_k = kv_copies(gauss(shared[3], (MODEL_DIM, KV_HEADS, HEAD_DIM), MODEL_DIM ** -0.5), 1)
    b_k = kv_copies(gauss(shared[4], (KV_HEADS, HEAD_DIM), 1.0), 0)
    w_v = kv_copies(gauss(shared[5], (MODEL_DIM, KV_HEADS, HEAD_DIM), MODEL_DIM ** -0.5), 1)
    b_v = kv_copies(gauss(shared[6], (KV_HEADS, HEAD_DIM), 1.0), 0)
    return {
        "x": hidden.astype(jnp.bfloat16),
        "k_cache": k_cache.astype(jnp.bfloat16),
        "v_cache": v_cache.astype(jnp.bfloat16),
        "prefix_len": prefix,
        "valid_len": valid,
        "g_attn": (1.0 + gauss(shared[0], (MODEL_DIM,), 0.3)).astype(jnp.bfloat16),
        "w_q": gauss(shared[1], (MODEL_DIM, q_cols), 1.5 * MODEL_DIM ** -0.5).astype(jnp.bfloat16),
        "b_q": gauss(shared[2], (q_cols,), 1.0).astype(jnp.bfloat16),
        "w_k": w_k.reshape(MODEL_DIM, kv_cols).astype(jnp.bfloat16),
        "b_k": b_k.reshape(kv_cols).astype(jnp.bfloat16),
        "w_v": w_v.reshape(MODEL_DIM, kv_cols).astype(jnp.bfloat16),
        "b_v": b_v.reshape(kv_cols).astype(jnp.bfloat16),
        "w_o": gauss(shared[7], (q_cols, MODEL_DIM), q_cols ** -0.5).astype(jnp.bfloat16),
        "g_mlp": (1.0 + gauss(shared[8], (MODEL_DIM,), 0.3)).astype(jnp.bfloat16),
        "w_gate": gauss(shared[9], (MODEL_DIM, FFN_DIM), MODEL_DIM ** -0.5).astype(jnp.bfloat16),
        "w_up": gauss(shared[10], (MODEL_DIM, FFN_DIM), MODEL_DIM ** -0.5).astype(jnp.bfloat16),
        "w_down": gauss(shared[11], (FFN_DIM, MODEL_DIM), 1.5 * FFN_DIM ** -0.5).astype(jnp.bfloat16),
    }


def rms_norm(hidden, gain):
    wide_vals = hidden.astype(jnp.float32)
    inv_rms = lax.rsqrt(jnp.mean(wide_vals * wide_vals, axis=-1, keepdims=True) + NORM_EPS)
    return (wide_vals * inv_rms * gain.astype(jnp.float32)).astype(jnp.bfloat16)


def rotate_heads(heads, positions):
    half = heads.shape[-1] // 2
    inv_freq = ROPE_THETA ** (-(jnp.arange(half, dtype=jnp.float32) * 2.0) / heads.shape[-1])
    angles = positions.astype(jnp.float32)[..., None] * inv_freq
    cos_t = jnp.cos(angles)[..., None, :]
    sin_t = jnp.sin(angles)[..., None, :]
    wide = heads.astype(jnp.float32)
    first_half = wide[..., :half]
    second_half = wide[..., half:]
    rotated = jnp.concatenate([first_half * cos_t - second_half * sin_t, second_half * cos_t + first_half * sin_t], axis=-1)
    return rotated.astype(jnp.bfloat16)


def project(hidden, weight, bias):
    total = jnp.dot(hidden, weight, preferred_element_type=jnp.float32)
    return (total + bias.astype(jnp.float32)).astype(jnp.bfloat16)


def reference(x, k_cache, v_cache, prefix_len, valid_len, g_attn, w_q, b_q, w_k, b_k, w_v, b_v, w_o, g_mlp, w_gate, w_up, w_down):
    row_ids = jnp.arange(CHUNK_LEN)
    slot_ids = jnp.arange(CACHE_SLOTS)

    def one_request(req_args):
        hidden, k_rows, v_rows, start, count = req_args
        positions = start + row_ids
        normed = rms_norm(hidden, g_attn)
        queries = rotate_heads(project(normed, w_q, b_q).reshape(CHUNK_LEN, NUM_HEADS, HEAD_DIM), positions)
        keys_new = rotate_heads(project(normed, w_k, b_k).reshape(CHUNK_LEN, KV_STORE, HEAD_DIM), positions)
        values_new = project(normed, w_v, b_v).reshape(CHUNK_LEN, KV_STORE, HEAD_DIM)
        keep = (row_ids < count)[:, None, None]
        k_old = lax.dynamic_slice_in_dim(k_rows, start, CHUNK_LEN, axis=0)
        v_old = lax.dynamic_slice_in_dim(v_rows, start, CHUNK_LEN, axis=0)
        k_rows = lax.dynamic_update_slice_in_dim(k_rows, jnp.where(keep, keys_new, k_old), start, axis=0)
        v_rows = lax.dynamic_update_slice_in_dim(v_rows, jnp.where(keep, values_new, v_old), start, axis=0)
        limit = start + jnp.minimum(row_ids, count - 1)
        visible = slot_ids[None, :] <= limit[:, None]
        query_groups = queries.reshape(CHUNK_LEN, KV_STORE, GROUP_SIZE, HEAD_DIM)

        def one_head(head_args):
            q_head, k_head, v_head = head_args
            scores = jnp.einsum("cgd,sd->gcs", q_head.astype(jnp.float32), k_head.astype(jnp.float32)) * HEAD_DIM ** -0.5
            scores = jnp.where(visible[None], scores, -1.0e30)
            attn_probs = jax.nn.softmax(scores, axis=-1).astype(jnp.bfloat16)
            mixed = jnp.einsum("gcs,sd->cgd", attn_probs.astype(jnp.float32), v_head.astype(jnp.float32))
            return mixed.astype(jnp.bfloat16)

        heads_out = lax.map(one_head, (jnp.moveaxis(query_groups, 1, 0), jnp.moveaxis(k_rows, 1, 0), jnp.moveaxis(v_rows, 1, 0)))
        attended = jnp.moveaxis(heads_out, 0, 1).reshape(CHUNK_LEN, NUM_HEADS * HEAD_DIM)
        attn_out = jnp.dot(attended, w_o, preferred_element_type=jnp.float32).astype(jnp.bfloat16)
        resid_mid = (hidden.astype(jnp.float32) + attn_out.astype(jnp.float32)).astype(jnp.bfloat16)
        normed_mlp = rms_norm(resid_mid, g_mlp)
        gate = jnp.dot(normed_mlp, w_gate, preferred_element_type=jnp.float32)
        up_proj = jnp.dot(normed_mlp, w_up, preferred_element_type=jnp.float32)
        hidden_act = (jax.nn.silu(gate) * up_proj).astype(jnp.bfloat16)
        down = jnp.dot(hidden_act, w_down, preferred_element_type=jnp.float32).astype(jnp.bfloat16)
        result = (resid_mid.astype(jnp.float32) + down.astype(jnp.float32)).astype(jnp.bfloat16)
        return result, k_rows, v_rows

    x_out, k_out, v_out = lax.map(one_request, (x, k_cache, v_cache, prefix_len, valid_len))
    return x_out, k_out, v_out
```

```python
import functools
import jax
import jax.numpy as jnp
from jax import lax
from jax.experimental import pallas as pl
from jax.experimental.pallas import tpu as pltpu
from jax.sharding import PartitionSpec as P

ROPE_THETA = 1.0e6
NORM_EPS = 1.0e-6
KV_BLOCK = 512
UPDATE_ROWS = 400
LOG2_E = 1.4426950408889634


MESH_ID = pl.DeviceIdType.MESH
LINE = 4
CHUNKS = 4
TO_UPPER, TO_LOWER, TO_OTHER_LINE, TO_TWIN = range(4)
ARRIVAL = ((0, 1, 2, 3), (1, 0, 2, 3), (2, 1, 3, 0), (3, 2, 1, 0))


def scaled_norm(wide_vals, gain):
    inv_rms = lax.rsqrt(jnp.mean(wide_vals * wide_vals, axis=-1, keepdims=True) + NORM_EPS)
    return (wide_vals * inv_rms * gain).astype(jnp.bfloat16)


def place():
    me = lax.axis_index("tp")
    return lax.axis_index("dp"), me // 4, (me // 2) % 2, me % 2


def chip_at(table, z, m):
    packed = [sum(v << (2 * i) for i, v in enumerate(row)) for row in table]
    code = jnp.where(z == 0, packed[0], jnp.where(z == 1, packed[1], jnp.where(z == 2, packed[2], packed[3])))
    return (code >> (2 * m)) & 3


def greet(devices_of):
    dp, z, y, c = devices_of
    barrier = pltpu.get_barrier_semaphore()

    @pl.when(z > 0)
    def _():
        pl.semaphore_signal(barrier, 1, device_id=(dp, (z - 1) * 4 + y * 2 + c), device_id_type=MESH_ID)

    @pl.when(z < LINE - 1)
    def _():
        pl.semaphore_signal(barrier, 1, device_id=(dp, (z + 1) * 4 + y * 2 + c), device_id_type=MESH_ID)

    pl.semaphore_signal(barrier, 1, device_id=(dp, z * 4 + (1 - y) * 2 + c), device_id_type=MESH_ID)
    pl.semaphore_signal(barrier, 1, device_id=(dp, z * 4 + y * 2 + 1 - c), device_id_type=MESH_ID)
    pl.semaphore_wait(barrier, 2 + (z + 3) // 4 + (6 - z) // 4)


class RowGather:
    def __init__(self, buf, send_sem, recv_sem, where):
        self.buf, self.send_sem, self.recv_sem = buf, send_sem, recv_sem
        self.dp, self.z, self.y, self.c = where
        self.rows = buf.shape[0] // 16
        self.piece = self.rows // CHUNKS

    def copy(self, block, j, way, device):
        rows = pl.ds(pl.multiple_of(block * self.rows + j * self.piece, 16), self.piece)
        return pltpu.make_async_remote_copy(
            src_ref=self.buf.at[rows],
            dst_ref=self.buf.at[rows],
            send_sem=self.send_sem.at[way],
            recv_sem=self.recv_sem.at[block * CHUNKS + j],
            device_id=(self.dp, device),
            device_id_type=MESH_ID,
        )

    def arrived(self, block, j):
        self.copy(block, j, 0, 0).wait_recv()

    def spread(self, block, j, zc, ups):
        y, c = self.y, self.c
        if ups[0] and zc < LINE - 1:
            self.copy(block, j, TO_UPPER, (zc + 1) * 4 + y * 2 + c).start()
        if ups[1] and zc > 0:
            self.copy(block, j, TO_LOWER, (zc - 1) * 4 + y * 2 + c).start()
        self.copy(block, j, TO_OTHER_LINE, zc * 4 + (1 - y) * 2 + c).start()
        self.copy(block, j, TO_TWIN, zc * 4 + y * 2 + 1 - c).start()

    def across(self, zc, m):
        y, c = self.y, self.c
        block = ARRIVAL[zc][m] * 4 + (1 - y) * 2 + c
        for j in range(CHUNKS):
            self.arrived(block, j)
            self.copy(block, j, TO_TWIN, zc * 4 + y * 2 + 1 - c).start()

    def early(self):
        for zc in range(LINE):

            @pl.when(self.z == zc)
            def _(zc=zc):
                y, c = self.y, self.c
                for j in range(CHUNKS):
                    self.spread(zc * 4 + y * 2 + c, j, zc, (True, True))
                for far in range(1, LINE):
                    for j in range(CHUNKS):
                        if zc - far >= 0:
                            block = (zc - far) * 4 + y * 2 + c
                            self.arrived(block, j)
                            self.spread(block, j, zc, (True, False))
                        if zc + far < LINE:
                            block = (zc + far) * 4 + y * 2 + c
                            self.arrived(block, j)
                            self.spread(block, j, zc, (False, True))
                    self.across(zc, far - 1)

    def late(self):
        for zc in range(LINE):

            @pl.when(self.z == zc)
            def _(zc=zc):
                self.across(zc, LINE - 1)

    def twin_arrived(self, block):
        for j in range(CHUNKS):
            self.arrived(block, j)

    def drain(self):
        def sent(way, blocks):
            rows = pl.ds(0, blocks * self.rows)
            pltpu.make_async_remote_copy(
                src_ref=self.buf.at[rows],
                dst_ref=self.buf.at[rows],
                send_sem=self.send_sem.at[way],
                recv_sem=self.recv_sem.at[0],
                device_id=(self.dp, 0),
                device_id_type=MESH_ID,
            ).wait_send()

        for zc in range(LINE):

            @pl.when(self.z == zc)
            def _(zc=zc):
                if zc < LINE - 1:
                    sent(TO_UPPER, zc + 1)
                if zc > 0:
                    sent(TO_LOWER, LINE - zc)

        sent(TO_OTHER_LINE, LINE)
        sent(TO_TWIN, 2 * LINE)


def project_body(x_ref, gain_ref, w_ref, bias_ref, base_cos_ref, base_sin_ref, step_cos_ref, step_sin_ref, q_ref, k_ref, v_ref, rows_buf, send_sem, recv_sem):
    where = place()
    dp, z, y, c = where
    rows = x_ref.shape[0]
    head_dim = q_ref.shape[1]
    own_tokens = step_cos_ref.shape[0] // 16
    me = z * 4 + y * 2 + c
    own = pl.ds(pl.multiple_of(me * rows, 16), rows)
    rows_buf[own, :] = scaled_norm(x_ref[...].astype(jnp.float32), gain_ref[...].astype(jnp.float32))
    greet(where)
    gather = RowGather(rows_buf, send_sem, recv_sem, where)
    gather.early()

    def compute(block):
        at = pl.ds(pl.multiple_of(block * rows, 16), rows)
        out = jnp.dot(rows_buf[at, :], w_ref[...], preferred_element_type=jnp.float32)
        out = (out + bias_ref[...].astype(jnp.float32)).astype(jnp.bfloat16)
        steps = pl.ds(pl.multiple_of(block * own_tokens, 8), own_tokens)
        step_cos, step_sin = step_cos_ref[steps, :][None], step_sin_ref[steps, :][None]
        base_cos, base_sin = base_cos_ref[...][:, None, :], base_sin_ref[...][:, None, :]
        cos_t = (base_cos * step_cos - base_sin * step_sin).reshape(rows, head_dim)
        sin_t = (base_sin * step_cos + base_cos * step_sin).reshape(rows, head_dim)
        lane = lax.broadcasted_iota(jnp.int32, (rows, head_dim), 1)
        sin_t = jnp.where(lane < head_dim // 2, -sin_t, sin_t)
        for ref, i in ((q_ref, 0), (k_ref, 1)):
            wide = out[:, i * head_dim:(i + 1) * head_dim].astype(jnp.float32)
            ref[at, :] = (wide * cos_t + pltpu.roll(wide, head_dim // 2, 1) * sin_t).astype(jnp.bfloat16)
        v_ref[at, :] = out[:, 2 * head_dim:]

    def chip(place_z, line):
        compute(place_z * 4 + line * 2 + c)
        twin = place_z * 4 + line * 2 + 1 - c
        gather.twin_arrived(twin)
        compute(twin)

    @pl.loop(0, 6)
    def _(m):
        chip(chip_at(ARRIVAL, z, m % 4), (y + m // 4) % 2)

    gather.late()

    @pl.loop(2, 4)
    def _(m):
        chip(chip_at(ARRIVAL, z, m), 1 - y)

    gather.drain()


def project_all(x_rows, gain, w_all, bias_all, prefix):
    n_req, own_tokens, width = x_rows.shape
    rows = n_req * own_tokens
    head_dim = w_all.shape[1] // 3
    half = head_dim // 2
    inv_freq = ROPE_THETA ** (-(jnp.arange(half, dtype=jnp.float32) * 2.0) / head_dim)
    inv_freq = jnp.concatenate([inv_freq, inv_freq])[None, :]
    base = prefix.astype(jnp.float32)[:, None] * inv_freq
    step = jnp.arange(16 * own_tokens, dtype=jnp.float32)[:, None] * inv_freq
    vmem = pl.BlockSpec(memory_space=pltpu.VMEM)
    out = jax.ShapeDtypeStruct((16 * rows, head_dim), jnp.bfloat16)
    outs = pl.pallas_call(
        project_body,
        out_shape=(out, out, out),
        in_specs=[vmem] * 8,
        out_specs=(vmem,) * 3,
        scratch_shapes=[
            pltpu.VMEM((16 * rows, width), jnp.bfloat16),
            pltpu.SemaphoreType.DMA((4,)),
            pltpu.SemaphoreType.DMA((16 * CHUNKS,)),
        ],
        compiler_params=pltpu.CompilerParams(collective_id=0, has_side_effects=True, vmem_limit_bytes=40 * 2**20),
        cost_estimate=pl.CostEstimate(flops=2 * 16 * rows * width * 3 * head_dim, bytes_accessed=4 * rows * width, transcendentals=0),
        name="project",
    )(x_rows.reshape(rows, width), gain[None, :], w_all, bias_all[None, :], jnp.cos(base), jnp.sin(base), jnp.cos(step), jnp.sin(step))
    return tuple(o.reshape(16, n_req, own_tokens, head_dim) for o in outs)


def token_rows(ref):
    rows = ref[:, 0].astype(jnp.float32)
    return rows.reshape(rows.shape[0] * rows.shape[1], rows.shape[2])


def attention_body(prefix_ref, valid_ref, q_ref, kn_ref, vn_ref, k_ref, v_ref, o_ref, ko_ref, vo_ref, scores, top, total, acc):
    req = pl.program_id(0)
    start = prefix_ref[req]
    count = valid_ref[req]
    head_dim = q_ref.shape[3]
    n_tokens = q_ref.shape[0] * q_ref.shape[2]
    slots = k_ref.shape[1]
    ko_ref[...] = k_ref[...]
    vo_ref[...] = v_ref[...]
    base = pl.multiple_of(jnp.minimum((start // 16) * 16, slots - UPDATE_ROWS), 16)
    shift = start - base
    row = lax.broadcasted_iota(jnp.int32, (UPDATE_ROWS, head_dim), 0) - shift
    keep = (row >= 0) & (row < count)
    for src, dst in ((kn_ref, ko_ref), (vn_ref, vo_ref)):
        fresh = jnp.concatenate([token_rows(src), jnp.zeros((UPDATE_ROWS - n_tokens, head_dim), jnp.float32)], axis=0)
        fresh = pltpu.roll(fresh, shift, 0)
        old = dst[0, pl.ds(base, UPDATE_ROWS), :].astype(jnp.float32)
        dst[0, pl.ds(base, UPDATE_ROWS), :] = jnp.where(keep, fresh, old).astype(jnp.bfloat16)

    n_open = (start + 1) // KV_BLOCK
    n_used = pl.cdiv(start + count, KV_BLOCK)
    queries = token_rows(q_ref).astype(jnp.bfloat16)
    lanes = KV_BLOCK // 128
    top[...] = jnp.full_like(top, -1.0e30)

    def score(blk, masked):
        keys = ko_ref[0, pl.ds(pl.multiple_of(blk * KV_BLOCK, KV_BLOCK), KV_BLOCK), :]
        s = lax.dot_general(queries, keys, (((1,), (1,)), ((), ())), preferred_element_type=jnp.float32)
        if masked:
            col = lax.broadcasted_iota(jnp.int32, (n_tokens, KV_BLOCK), 1) + blk * KV_BLOCK
            row_id = lax.broadcasted_iota(jnp.int32, (n_tokens, KV_BLOCK), 0)
            s = jnp.where(col <= start + jnp.minimum(row_id, count - 1), s, -1.0e30)
        scores[blk] = s
        best = top[...]
        for j in range(lanes):
            best = jnp.maximum(best, s[:, j * 128:(j + 1) * 128])
        top[...] = best

    pl.loop(0, n_open)(lambda blk: score(blk, False))
    pl.loop(n_open, n_used)(lambda blk: score(blk, True))
    top[...] = jnp.broadcast_to(jnp.max(top[...], axis=1, keepdims=True), top.shape)
    total[...] = jnp.zeros_like(total)
    acc[...] = jnp.zeros_like(acc)

    @pl.loop(0, n_used)
    def _(blk):
        best = top[...]
        part = total[...]
        pieces = []
        for j in range(lanes):
            e = jnp.exp2((scores[blk, :, j * 128:(j + 1) * 128] - best) * (LOG2_E * head_dim ** -0.5))
            part = part + e
            pieces.append(e.astype(jnp.bfloat16))
        total[...] = part
        vals = vo_ref[0, pl.ds(pl.multiple_of(blk * KV_BLOCK, KV_BLOCK), KV_BLOCK), :]
        acc[...] += jnp.dot(jnp.concatenate(pieces, axis=1), vals, preferred_element_type=jnp.float32)

    mixed = acc[...] / jnp.sum(total[...], axis=1, keepdims=True)
    o_ref[:, 0] = mixed.reshape(o_ref.shape[0], o_ref.shape[2], head_dim).astype(jnp.bfloat16)


def attend(queries, keys_new, values_new, k_cache, v_cache, prefix, valid):
    owners, n_req, own_tokens, head_dim = queries.shape
    n_tokens = owners * own_tokens
    slots = k_cache.shape[1]
    new_spec = pl.BlockSpec((owners, 1, own_tokens, head_dim), lambda r, *_: (0, r, 0, 0))
    cache_spec = pl.BlockSpec((1, slots, head_dim), lambda r, *_: (r, 0, 0))
    cache_out = jax.ShapeDtypeStruct(k_cache.shape, jnp.bfloat16)
    return pl.pallas_call(
        attention_body,
        out_shape=(jax.ShapeDtypeStruct(queries.shape, jnp.bfloat16), cache_out, cache_out),
        grid_spec=pltpu.PrefetchScalarGridSpec(
            num_scalar_prefetch=2,
            grid=(n_req,),
            in_specs=[new_spec, new_spec, new_spec, cache_spec, cache_spec],
            out_specs=(new_spec, cache_spec, cache_spec),
            scratch_shapes=[
                pltpu.VMEM((slots // KV_BLOCK, n_tokens, KV_BLOCK), jnp.float32),
                pltpu.VMEM((n_tokens, 128), jnp.float32),
                pltpu.VMEM((n_tokens, 128), jnp.float32),
                pltpu.VMEM((n_tokens, head_dim), jnp.float32),
            ],
        ),
        compiler_params=pltpu.CompilerParams(dimension_semantics=("arbitrary",), vmem_limit_bytes=40 * 2**20),
        cost_estimate=pl.CostEstimate(flops=2 * 2 * n_req * n_tokens * slots * head_dim, bytes_accessed=8 * n_req * slots * head_dim, transcendentals=n_req * n_tokens * slots),
        name="attend",
    )(prefix, valid, queries, keys_new, values_new, k_cache, v_cache)


def mlp_partial(normed_full, w_gate, w_up, w_down):
    gate = jnp.einsum("rcd,df->rcf", normed_full, w_gate, preferred_element_type=jnp.float32)
    up_proj = jnp.einsum("rcd,df->rcf", normed_full, w_up, preferred_element_type=jnp.float32)
    hidden_act = (jax.nn.silu(gate) * up_proj).astype(jnp.bfloat16)
    return jnp.einsum("rcf,fd->rcd", hidden_act, w_down, preferred_element_type=jnp.float32).astype(jnp.bfloat16)


def rms_norm(hidden, gain):
    return scaled_norm(hidden.astype(jnp.float32), gain.astype(jnp.float32))


def add_rounded(first, second):
    return (first.astype(jnp.float32) + second.astype(jnp.float32)).astype(jnp.bfloat16)


def solution(mesh):
    row_spec = P("dp", "tp", None)
    cache_spec = P("dp", None, "tp", None)
    req_spec = P("dp")
    rep_spec = P(None)
    col_spec = P(None, "tp")
    bias_spec = P("tp")
    down_spec = P("tp", None)

    def layer(x_rows, k_cache, v_cache, prefix, valid, g_attn, w_q, b_q, w_k, b_k, w_v, b_v, w_o, g_mlp, w_gate, w_up, w_down):
        n_req, own_tokens, width = x_rows.shape
        w_all = jnp.concatenate([w_q, w_k, w_v], axis=1)
        bias_all = jnp.concatenate([b_q, b_k, b_v])
        queries, keys_new, values_new = project_all(x_rows, g_attn, w_all, bias_all, prefix)
        flat = (k_cache.shape[0], k_cache.shape[1], k_cache.shape[3])
        attended, k_out, v_out = attend(queries, keys_new, values_new, k_cache.reshape(flat), v_cache.reshape(flat), prefix, valid)
        attended = jnp.moveaxis(attended, 0, 1).reshape(n_req, 16 * own_tokens, flat[2])
        attn_part = jnp.einsum("rcn,nd->rcd", attended, w_o, preferred_element_type=jnp.float32).astype(jnp.bfloat16)
        attn_rows = lax.psum_scatter(attn_part, "tp", scatter_dimension=1, tiled=True)
        resid_mid = add_rounded(x_rows, attn_rows)
        normed_mlp = rms_norm(resid_mid, g_mlp)
        mlp_full = lax.all_gather(normed_mlp, "tp", axis=1, tiled=True)
        down_part = mlp_partial(mlp_full, w_gate, w_up, w_down)
        down_rows = lax.psum_scatter(down_part, "tp", scatter_dimension=1, tiled=True)
        return add_rounded(resid_mid, down_rows), k_out.reshape(k_cache.shape), v_out.reshape(v_cache.shape)

    in_specs = (row_spec, cache_spec, cache_spec, req_spec, req_spec, rep_spec, col_spec, bias_spec, col_spec, bias_spec, col_spec, bias_spec, down_spec, rep_spec, col_spec, col_spec, down_spec)
    return jax.shard_map(layer, mesh=mesh, in_specs=in_specs, out_specs=(row_spec, cache_spec, cache_spec), check_vma=False)
```

```python
import functools
import jax
import jax.numpy as jnp
from jax import lax
from jax.experimental import pallas as pl
from jax.experimental.pallas import tpu as pltpu
from jax.sharding import PartitionSpec as P

ROPE_THETA = 1.0e6
NORM_EPS = 1.0e-6
KV_BLOCK = 512
UPDATE_ROWS = 400
LOG2_E = 1.4426950408889634


MESH_ID = pl.DeviceIdType.MESH
LINE = 4
CHUNKS = 4
TO_UPPER, TO_LOWER, TO_OTHER_LINE, TO_TWIN = range(4)
ARRIVAL = ((0, 1, 2, 3), (1, 0, 2, 3), (2, 1, 3, 0), (3, 2, 1, 0))


def scaled_norm(wide_vals, gain):
    inv_rms = lax.rsqrt(jnp.mean(wide_vals * wide_vals, axis=-1, keepdims=True) + NORM_EPS)
    return (wide_vals * inv_rms * gain).astype(jnp.bfloat16)


def place():
    me = lax.axis_index("tp")
    return lax.axis_index("dp"), me // 4, (me // 2) % 2, me % 2


def chip_at(table, z, m):
    packed = [sum(v << (2 * i) for i, v in enumerate(row)) for row in table]
    code = jnp.where(z == 0, packed[0], jnp.where(z == 1, packed[1], jnp.where(z == 2, packed[2], packed[3])))
    return (code >> (2 * m)) & 3


def greet(devices_of):
    dp, z, y, c = devices_of
    barrier = pltpu.get_barrier_semaphore()

    @pl.when(z > 0)
    def _():
        pl.semaphore_signal(barrier, 1, device_id=(dp, (z - 1) * 4 + y * 2 + c), device_id_type=MESH_ID)

    @pl.when(z < LINE - 1)
    def _():
        pl.semaphore_signal(barrier, 1, device_id=(dp, (z + 1) * 4 + y * 2 + c), device_id_type=MESH_ID)

    pl.semaphore_signal(barrier, 1, device_id=(dp, z * 4 + (1 - y) * 2 + c), device_id_type=MESH_ID)
    pl.semaphore_signal(barrier, 1, device_id=(dp, z * 4 + y * 2 + 1 - c), device_id_type=MESH_ID)
    pl.semaphore_wait(barrier, 2 + (z + 3) // 4 + (6 - z) // 4)


class RowGather:
    def __init__(self, buf, send_sem, recv_sem, where):
        self.buf, self.send_sem, self.recv_sem = buf, send_sem, recv_sem
        self.dp, self.z, self.y, self.c = where
        self.rows = buf.shape[0] // 16
        self.piece = self.rows // CHUNKS

    def copy(self, block, j, way, device):
        rows = pl.ds(pl.multiple_of(block * self.rows + j * self.piece, 16), self.piece)
        return pltpu.make_async_remote_copy(
            src_ref=self.buf.at[rows],
            dst_ref=self.buf.at[rows],
            send_sem=self.send_sem.at[way],
            recv_sem=self.recv_sem.at[block * CHUNKS + j],
            device_id=(self.dp, device),
            device_id_type=MESH_ID,
        )

    def arrived(self, block, j):
        self.copy(block, j, 0, 0).wait_recv()

    def spread(self, block, j, zc, ups):
        y, c = self.y, self.c
        if ups[0] and zc < LINE - 1:
            self.copy(block, j, TO_UPPER, (zc + 1) * 4 + y * 2 + c).start()
        if ups[1] and zc > 0:
            self.copy(block, j, TO_LOWER, (zc - 1) * 4 + y * 2 + c).start()
        self.copy(block, j, TO_OTHER_LINE, zc * 4 + (1 - y) * 2 + c).start()
        self.copy(block, j, TO_TWIN, zc * 4 + y * 2 + 1 - c).start()

    def across(self, zc, m):
        y, c = self.y, self.c
        block = ARRIVAL[zc][m] * 4 + (1 - y) * 2 + c
        for j in range(CHUNKS):
            self.arrived(block, j)
            self.copy(block, j, TO_TWIN, zc * 4 + y * 2 + 1 - c).start()

    def early(self):
        for zc in range(LINE):

            @pl.when(self.z == zc)
            def _(zc=zc):
                y, c = self.y, self.c
                for j in range(CHUNKS):
                    self.spread(zc * 4 + y * 2 + c, j, zc, (True, True))
                for far in range(1, LINE):
                    for j in range(CHUNKS):
                        if zc - far >= 0:
                            block = (zc - far) * 4 + y * 2 + c
                            self.arrived(block, j)
                            self.spread(block, j, zc, (True, False))
                        if zc + far < LINE:
                            block = (zc + far) * 4 + y * 2 + c
                            self.arrived(block, j)
                            self.spread(block, j, zc, (False, True))
                    self.across(zc, far - 1)

    def late(self):
        for zc in range(LINE):

            @pl.when(self.z == zc)
            def _(zc=zc):
                self.across(zc, LINE - 1)

    def twin_arrived(self, block):
        for j in range(CHUNKS):
            self.arrived(block, j)

    def drain(self):
        def sent(way, blocks):
            rows = pl.ds(0, blocks * self.rows)
            pltpu.make_async_remote_copy(
                src_ref=self.buf.at[rows],
                dst_ref=self.buf.at[rows],
                send_sem=self.send_sem.at[way],
                recv_sem=self.recv_sem.at[0],
                device_id=(self.dp, 0),
                device_id_type=MESH_ID,
            ).wait_send()

        for zc in range(LINE):

            @pl.when(self.z == zc)
            def _(zc=zc):
                if zc < LINE - 1:
                    sent(TO_UPPER, zc + 1)
                if zc > 0:
                    sent(TO_LOWER, LINE - zc)

        sent(TO_OTHER_LINE, LINE)
        sent(TO_TWIN, 2 * LINE)


def project_body(x_ref, gain_ref, w_ref, bias_ref, base_cos_ref, base_sin_ref, step_cos_ref, step_sin_ref, q_ref, k_ref, v_ref, rows_buf, send_sem, recv_sem):
    where = place()
    dp, z, y, c = where
    rows = x_ref.shape[0]
    head_dim = q_ref.shape[1]
    own_tokens = step_cos_ref.shape[0] // 16
    me = z * 4 + y * 2 + c
    own = pl.ds(pl.multiple_of(me * rows, 16), rows)
    rows_buf[own, :] = scaled_norm(x_ref[...].astype(jnp.float32), gain_ref[...].astype(jnp.float32))
    greet(where)
    gather = RowGather(rows_buf, send_sem, recv_sem, where)
    gather.early()

    def compute(block):
        at = pl.ds(pl.multiple_of(block * rows, 16), rows)
        out = jnp.dot(rows_buf[at, :], w_ref[...], preferred_element_type=jnp.float32)
        out = (out + bias_ref[...].astype(jnp.float32)).astype(jnp.bfloat16)
        steps = pl.ds(pl.multiple_of(block * own_tokens, 8), own_tokens)
        step_cos, step_sin = step_cos_ref[steps, :][None], step_sin_ref[steps, :][None]
        base_cos, base_sin = base_cos_ref[...][:, None, :], base_sin_ref[...][:, None, :]
        cos_t = (base_cos * step_cos - base_sin * step_sin).reshape(rows, head_dim)
        sin_t = (base_sin * step_cos + base_cos * step_sin).reshape(rows, head_dim)
        lane = lax.broadcasted_iota(jnp.int32, (rows, head_dim), 1)
        sin_t = jnp.where(lane < head_dim // 2, -sin_t, sin_t)
        for ref, i in ((q_ref, 0), (k_ref, 1)):
            wide = out[:, i * head_dim:(i + 1) * head_dim].astype(jnp.float32)
            ref[at, :] = (wide * cos_t + pltpu.roll(wide, head_dim // 2, 1) * sin_t).astype(jnp.bfloat16)
        v_ref[at, :] = out[:, 2 * head_dim:]

    def chip(place_z, line):
        compute(place_z * 4 + line * 2 + c)
        twin = place_z * 4 + line * 2 + 1 - c
        gather.twin_arrived(twin)
        compute(twin)

    @pl.loop(0, 6)
    def _(m):
        chip(chip_at(ARRIVAL, z, m % 4), (y + m // 4) % 2)

    gather.late()

    @pl.loop(2, 4)
    def _(m):
        chip(chip_at(ARRIVAL, z, m), 1 - y)

    gather.drain()


def project_all(x_rows, gain, w_all, bias_all, prefix):
    n_req, own_tokens, width = x_rows.shape
    rows = n_req * own_tokens
    head_dim = w_all.shape[1] // 3
    half = head_dim // 2
    inv_freq = ROPE_THETA ** (-(jnp.arange(half, dtype=jnp.float32) * 2.0) / head_dim)
    inv_freq = jnp.concatenate([inv_freq, inv_freq])[None, :]
    base = prefix.astype(jnp.float32)[:, None] * inv_freq
    step = jnp.arange(16 * own_tokens, dtype=jnp.float32)[:, None] * inv_freq
    vmem = pl.BlockSpec(memory_space=pltpu.VMEM)
    out = jax.ShapeDtypeStruct((16 * rows, head_dim), jnp.bfloat16)
    outs = pl.pallas_call(
        project_body,
        out_shape=(out, out, out),
        in_specs=[vmem] * 8,
        out_specs=(vmem,) * 3,
        scratch_shapes=[
            pltpu.VMEM((16 * rows, width), jnp.bfloat16),
            pltpu.SemaphoreType.DMA((4,)),
            pltpu.SemaphoreType.DMA((16 * CHUNKS,)),
        ],
        compiler_params=pltpu.CompilerParams(collective_id=0, has_side_effects=True, vmem_limit_bytes=40 * 2**20),
        cost_estimate=pl.CostEstimate(flops=2 * 16 * rows * width * 3 * head_dim, bytes_accessed=4 * rows * width, transcendentals=0),
        name="project",
    )(x_rows.reshape(rows, width), gain[None, :], w_all, bias_all[None, :], jnp.cos(base), jnp.sin(base), jnp.cos(step), jnp.sin(step))
    return tuple(o.reshape(16, n_req, own_tokens, head_dim) for o in outs)


def token_rows(ref):
    rows = ref[:, 0].astype(jnp.float32)
    return rows.reshape(rows.shape[0] * rows.shape[1], rows.shape[2])


def attention_body(prefix_ref, valid_ref, q_ref, kn_ref, vn_ref, k_ref, v_ref, o_ref, ko_ref, vo_ref, scores, top, total, acc):
    req = pl.program_id(0)
    start = prefix_ref[req]
    count = valid_ref[req]
    head_dim = q_ref.shape[3]
    n_tokens = q_ref.shape[0] * q_ref.shape[2]
    slots = k_ref.shape[1]
    ko_ref[...] = k_ref[...]
    vo_ref[...] = v_ref[...]
    base = pl.multiple_of(jnp.minimum((start // 16) * 16, slots - UPDATE_ROWS), 16)
    shift = start - base
    row = lax.broadcasted_iota(jnp.int32, (UPDATE_ROWS, head_dim), 0) - shift
    keep = (row >= 0) & (row < count)
    for src, dst in ((kn_ref, ko_ref), (vn_ref, vo_ref)):
        fresh = jnp.concatenate([token_rows(src), jnp.zeros((UPDATE_ROWS - n_tokens, head_dim), jnp.float32)], axis=0)
        fresh = pltpu.roll(fresh, shift, 0)
        old = dst[0, pl.ds(base, UPDATE_ROWS), :].astype(jnp.float32)
        dst[0, pl.ds(base, UPDATE_ROWS), :] = jnp.where(keep, fresh, old).astype(jnp.bfloat16)

    n_open = (start + 1) // KV_BLOCK
    n_used = pl.cdiv(start + count, KV_BLOCK)
    queries = token_rows(q_ref).astype(jnp.bfloat16)
    lanes = KV_BLOCK // 128
    top[...] = jnp.full_like(top, -1.0e30)

    def score(blk, masked):
        keys = ko_ref[0, pl.ds(pl.multiple_of(blk * KV_BLOCK, KV_BLOCK), KV_BLOCK), :]
        s = lax.dot_general(queries, keys, (((1,), (1,)), ((), ())), preferred_element_type=jnp.float32)
        if masked:
            col = lax.broadcasted_iota(jnp.int32, (n_tokens, KV_BLOCK), 1) + blk * KV_BLOCK
            row_id = lax.broadcasted_iota(jnp.int32, (n_tokens, KV_BLOCK), 0)
            s = jnp.where(col <= start + jnp.minimum(row_id, count - 1), s, -1.0e30)
        scores[blk] = s
        best = top[...]
        for j in range(lanes):
            best = jnp.maximum(best, s[:, j * 128:(j + 1) * 128])
        top[...] = best

    pl.loop(0, n_open)(lambda blk: score(blk, False))
    pl.loop(n_open, n_used)(lambda blk: score(blk, True))
    top[...] = jnp.broadcast_to(jnp.max(top[...], axis=1, keepdims=True), top.shape)
    total[...] = jnp.zeros_like(total)
    acc[...] = jnp.zeros_like(acc)

    @pl.loop(0, n_used)
    def _(blk):
        best = top[...]
        part = total[...]
        pieces = []
        for j in range(lanes):
            e = jnp.exp2((scores[blk, :, j * 128:(j + 1) * 128] - best) * (LOG2_E * head_dim ** -0.5))
            part = part + e
            pieces.append(e.astype(jnp.bfloat16))
        total[...] = part
        vals = vo_ref[0, pl.ds(pl.multiple_of(blk * KV_BLOCK, KV_BLOCK), KV_BLOCK), :]
        acc[...] += jnp.dot(jnp.concatenate(pieces, axis=1), vals, preferred_element_type=jnp.float32)

    mixed = acc[...] / jnp.sum(total[...], axis=1, keepdims=True)
    o_ref[:, 0] = mixed.reshape(o_ref.shape[0], o_ref.shape[2], head_dim).astype(jnp.bfloat16)


def attend(queries, keys_new, values_new, k_cache, v_cache, prefix, valid):
    owners, n_req, own_tokens, head_dim = queries.shape
    n_tokens = owners * own_tokens
    slots = k_cache.shape[1]
    new_spec = pl.BlockSpec((owners, 1, own_tokens, head_dim), lambda r, *_: (0, r, 0, 0))
    cache_spec = pl.BlockSpec((1, slots, head_dim), lambda r, *_: (r, 0, 0))
    cache_out = jax.ShapeDtypeStruct(k_cache.shape, jnp.bfloat16)
    return pl.pallas_call(
        attention_body,
        out_shape=(jax.ShapeDtypeStruct(queries.shape, jnp.bfloat16), cache_out, cache_out),
        grid_spec=pltpu.PrefetchScalarGridSpec(
            num_scalar_prefetch=2,
            grid=(n_req,),
            in_specs=[new_spec, new_spec, new_spec, cache_spec, cache_spec],
            out_specs=(new_spec, cache_spec, cache_spec),
            scratch_shapes=[
                pltpu.VMEM((slots // KV_BLOCK, n_tokens, KV_BLOCK), jnp.float32),
                pltpu.VMEM((n_tokens, 128), jnp.float32),
                pltpu.VMEM((n_tokens, 128), jnp.float32),
                pltpu.VMEM((n_tokens, head_dim), jnp.float32),
            ],
        ),
        compiler_params=pltpu.CompilerParams(dimension_semantics=("arbitrary",), vmem_limit_bytes=40 * 2**20),
        cost_estimate=pl.CostEstimate(flops=2 * 2 * n_req * n_tokens * slots * head_dim, bytes_accessed=8 * n_req * slots * head_dim, transcendentals=n_req * n_tokens * slots),
        name="attend",
    )(prefix, valid, queries, keys_new, values_new, k_cache, v_cache)


REDUCE = ((2, 3, 1, 0), (2, 3, 0, 1), (1, 0, 3, 2), (1, 0, 2, 3))
COMPUTE = tuple((r[0], r[2], r[3], r[1]) for r in REDUCE)


def finish_body(o_ref, x_ref, gain_ref, w_gate_ref, w_up_ref, w_down_ref, w_o_ref, out_ref,
                rows_buf, part, attended, resid, acc, from_twin, from_line, from_lower, from_upper,
                gather_send, gather_recv, reduce_send, twin_recv, line_recv, lower_recv, upper_recv, swap_send, swap_recv, local_sem):
    where = place()
    dp, z, y, c = where
    rows, width = x_ref.shape
    head_dim = o_ref.shape[1]
    me = z * 4 + y * 2 + c
    piece = rows // CHUNKS
    load = pltpu.make_async_copy(w_o_ref, part.at[pl.ds(0, w_o_ref.shape[0])], local_sem)
    load.start()
    barrier = pltpu.get_barrier_semaphore()
    for k in range(1, 16):
        pl.semaphore_signal(barrier, 1, device_id=(dp, (me + k) % 16), device_id_type=MESH_ID)
    pl.semaphore_wait(barrier, 15)

    def block_rows(block):
        return pl.ds(pl.multiple_of(block * rows, 16), rows)

    mine = pl.ds(pl.multiple_of(me * head_dim, 128), head_dim)
    for k in range(1, 16):
        other = (me + k) % 16
        pltpu.make_async_remote_copy(
            src_ref=o_ref.at[block_rows(other)], dst_ref=attended.at[:, mine], send_sem=swap_send, recv_sem=swap_recv,
            device_id=(dp, other), device_id_type=MESH_ID).start()
    attended[:, mine] = o_ref[block_rows(me), :]
    load.wait()
    others = o_ref.at[pl.ds(0, 15 * rows)]
    swap = pltpu.make_async_remote_copy(src_ref=others, dst_ref=others, send_sem=swap_send, recv_sem=swap_recv, device_id=(dp, 0), device_id_type=MESH_ID)
    swap.wait_recv()
    swap.wait_send()

    @pl.loop(0, width // 256)
    def _(n):
        cols = pl.ds(pl.multiple_of(n * 256, 256), 256)
        out = jnp.dot(attended[...], part[pl.ds(0, w_o_ref.shape[0]), cols], preferred_element_type=jnp.float32).astype(jnp.bfloat16)
        resid[:, cols] = (x_ref[:, cols].astype(jnp.float32) + out.astype(jnp.float32)).astype(jnp.bfloat16)

    rows_buf[block_rows(me), :] = scaled_norm(resid[...].astype(jnp.float32), gain_ref[...].astype(jnp.float32))
    gather = RowGather(rows_buf, gather_send, gather_recv, where)
    gather.early()

    def partial_sums(block):
        hidden = rows_buf[block_rows(block), :]
        dims = (((1,), (1,)), ((), ()))
        gate = lax.dot_general(hidden, w_gate_ref[...], dims, preferred_element_type=jnp.float32)
        up = lax.dot_general(hidden, w_up_ref[...], dims, preferred_element_type=jnp.float32)
        act = (jax.nn.silu(gate) * up).astype(jnp.bfloat16)
        part[block_rows(block), :] = jnp.dot(act, w_down_ref[...], preferred_element_type=jnp.float32).astype(jnp.bfloat16)

    def twin_copy(block, slot):
        return pltpu.make_async_remote_copy(
            src_ref=part.at[block_rows(block)], dst_ref=from_twin.at[block_rows(slot)], send_sem=reduce_send.at[TO_TWIN], recv_sem=twin_recv.at[slot],
            device_id=(dp, z * 4 + y * 2 + 1 - c), device_id_type=MESH_ID)

    def piece_copy(dest, line, j, way, buf, sems, device):
        return pltpu.make_async_remote_copy(
            src_ref=part.at[pl.ds(pl.multiple_of((dest * 4 + line * 2 + c) * rows + j * piece, 16), piece)],
            dst_ref=buf.at[pl.ds(pl.multiple_of(dest * rows + j * piece, 16), piece)],
            send_sem=reduce_send.at[way], recv_sem=sems.at[dest * CHUNKS + j], device_id=(dp, device), device_id_type=MESH_ID)

    def line_send(dest):
        for j in range(CHUNKS):
            piece_copy(dest, 1 - y, j, TO_OTHER_LINE, from_line, line_recv, z * 4 + (1 - y) * 2 + c).start()

    @pl.loop(0, 8)
    def _(m):
        is_own = (m >= 1) & (m <= 4)
        at = jnp.where(is_own, chip_at(ARRIVAL, z, (m + 3) % 4), chip_at(COMPUTE, z, m % 4))
        line = jnp.where(is_own, y, 1 - y)
        pl.when(m == 7)(gather.late)
        block = at * 4 + line * 2 + c
        twin = at * 4 + line * 2 + 1 - c
        gather.twin_arrived(twin)
        partial_sums(twin)
        twin_copy(twin, at * 2 + line).start()
        partial_sums(block)
        twin_copy(block, at * 2 + line).wait_recv()
        total = part[block_rows(block), :].astype(jnp.float32) + from_twin[block_rows(at * 2 + line), :].astype(jnp.float32)
        part[block_rows(block), :] = total.astype(jnp.bfloat16)

        @pl.when((m == 0) | (m == 7))
        def _():
            line_send(at)

    line_send(chip_at(REDUCE, z, 2))
    line_send(chip_at(REDUCE, z, 3))

    @pl.loop(0, LINE * CHUNKS)
    def _(step):
        dest = chip_at(REDUCE, z, step // CHUNKS)
        j = step % CHUNKS
        here = pl.ds(pl.multiple_of((dest * 4 + y * 2 + c) * rows + j * piece, 16), piece)
        slot = pl.ds(pl.multiple_of(dest * rows + j * piece, 16), piece)
        piece_copy(dest, y, j, TO_OTHER_LINE, from_line, line_recv, me).wait_recv()
        acc[...] = part[here, :].astype(jnp.float32) + from_line[slot, :].astype(jnp.float32)

        @pl.when((dest >= z) & (z > 0))
        def _():
            piece_copy(dest, y, j, TO_UPPER, from_lower, lower_recv, me).wait_recv()
            acc[...] += from_lower[slot, :].astype(jnp.float32)

        @pl.when((dest <= z) & (z < LINE - 1))
        def _():
            piece_copy(dest, y, j, TO_LOWER, from_upper, upper_recv, me).wait_recv()
            acc[...] += from_upper[slot, :].astype(jnp.float32)

        @pl.when(dest != z)
        def _():
            part[here, :] = acc[...].astype(jnp.bfloat16)

        @pl.when(dest > z)
        def _():
            piece_copy(dest, y, j, TO_UPPER, from_lower, lower_recv, (z + 1) * 4 + y * 2 + c).start()

        @pl.when(dest < z)
        def _():
            piece_copy(dest, y, j, TO_LOWER, from_upper, upper_recv, (z - 1) * 4 + y * 2 + c).start()

        @pl.when(dest == z)
        def _():
            out = pl.ds(pl.multiple_of(j * piece, 16), piece)
            down = acc[...].astype(jnp.bfloat16).astype(jnp.float32)
            out_ref[out, :] = (resid[out, :].astype(jnp.float32) + down).astype(jnp.bfloat16)

    gather.drain()

    def sent(way, blocks):
        span = pl.ds(0, blocks * rows)
        pltpu.make_async_remote_copy(
            src_ref=part.at[span], dst_ref=part.at[span], send_sem=reduce_send.at[way], recv_sem=twin_recv.at[0],
            device_id=(dp, 0), device_id_type=MESH_ID).wait_send()

    for zc in range(LINE):

        @pl.when(z == zc)
        def _(zc=zc):
            if zc < LINE - 1:
                sent(TO_UPPER, LINE - 1 - zc)
            if zc > 0:
                sent(TO_LOWER, zc)

    sent(TO_OTHER_LINE, LINE)
    sent(TO_TWIN, 2 * LINE)


def finish(attended, x_rows, gain, w_gate, w_up, w_down, w_o):
    n_req, own_tokens, width = x_rows.shape
    rows = n_req * own_tokens
    head_dim = attended.shape[-1]
    vmem = pl.BlockSpec(memory_space=pltpu.VMEM)
    bf16, f32 = jnp.bfloat16, jnp.float32
    dma = pltpu.SemaphoreType.DMA
    out = pl.pallas_call(
        finish_body,
        out_shape=jax.ShapeDtypeStruct((rows, width), bf16),
        in_specs=[vmem] * 6 + [pl.BlockSpec(memory_space=pl.ANY)],
        out_specs=vmem,
        scratch_shapes=[
            pltpu.VMEM((16 * rows, width), bf16),
            pltpu.VMEM((16 * rows, width), bf16),
            pltpu.VMEM((rows, width), bf16),
            pltpu.VMEM((rows, width), bf16),
            pltpu.VMEM((rows // CHUNKS, width), f32),
            pltpu.VMEM((8 * rows, width), bf16),
            pltpu.VMEM((4 * rows, width), bf16),
            pltpu.VMEM((4 * rows, width), bf16),
            pltpu.VMEM((4 * rows, width), bf16),
            dma((4,)), dma((16 * CHUNKS,)), dma((4,)), dma((8,)), dma((4 * CHUNKS,)), dma((4 * CHUNKS,)), dma((4 * CHUNKS,)), dma, dma, dma,
        ],
        compiler_params=pltpu.CompilerParams(collective_id=1, has_side_effects=True, vmem_limit_bytes=62 * 2**20),
        cost_estimate=pl.CostEstimate(flops=2 * rows * width * (width + 16 * 3 * w_down.shape[0]), bytes_accessed=4 * width * width, transcendentals=0),
        name="finish",
    )(attended.reshape(16 * rows, head_dim), x_rows.reshape(rows, width), gain[None, :], w_gate.T, w_up.T, w_down, w_o)
    return out.reshape(x_rows.shape)


def solution(mesh):
    row_spec = P("dp", "tp", None)
    cache_spec = P("dp", None, "tp", None)
    req_spec = P("dp")
    rep_spec = P(None)
    col_spec = P(None, "tp")
    bias_spec = P("tp")
    down_spec = P("tp", None)

    def layer(x_rows, k_cache, v_cache, prefix, valid, g_attn, w_q, b_q, w_k, b_k, w_v, b_v, w_o, g_mlp, w_gate, w_up, w_down):
        w_all = jnp.concatenate([w_q, w_k, w_v], axis=1)
        bias_all = jnp.concatenate([b_q, b_k, b_v])
        w_o_full = lax.all_gather(w_o, "tp", axis=0, tiled=True)
        queries, keys_new, values_new = project_all(x_rows, g_attn, w_all, bias_all, prefix)
        flat = (k_cache.shape[0], k_cache.shape[1], k_cache.shape[3])
        attended, k_out, v_out = attend(queries, keys_new, values_new, k_cache.reshape(flat), v_cache.reshape(flat), prefix, valid)
        x_out = finish(attended, x_rows, g_mlp, w_gate, w_up, w_down, w_o_full)
        return x_out, k_out.reshape(k_cache.shape), v_out.reshape(v_cache.shape)

    in_specs = (row_spec, cache_spec, cache_spec, req_spec, req_spec, rep_spec, col_spec, bias_spec, col_spec, bias_spec, col_spec, bias_spec, down_spec, rep_spec, col_spec, col_spec, down_spec)
    return jax.shard_map(layer, mesh=mesh, in_specs=in_specs, out_specs=(row_spec, cache_spec, cache_spec), check_vma=False)
```

```python
import functools
import jax
import jax.numpy as jnp
from jax import lax
from jax.experimental import pallas as pl
from jax.experimental.pallas import tpu as pltpu
from jax.sharding import PartitionSpec as P

ROPE_THETA = 1.0e6
NORM_EPS = 1.0e-6
KV_BLOCK = 512
UPDATE_ROWS = 400
LOG2_E = 1.4426950408889634


MESH_ID = pl.DeviceIdType.MESH
LINE = 4
CHUNKS = 6
ALONG_FIRST = CHUNKS - 1
TO_UPPER, TO_LOWER, TO_OTHER_LINE, TO_TWIN, TO_OTHER_GROUP = range(5)
ARRIVAL = ((0, 1, 2, 3), (1, 0, 2, 3), (2, 1, 3, 0), (3, 2, 1, 0))


def scaled_norm(wide_vals, gain):
    inv_rms = lax.rsqrt(jnp.mean(wide_vals * wide_vals, axis=-1, keepdims=True) + NORM_EPS)
    return (wide_vals * inv_rms * gain).astype(jnp.bfloat16)


def place():
    me = lax.axis_index("tp")
    return lax.axis_index("dp"), me // 4, (me // 2) % 2, me % 2


def chip_at(table, z, m):
    packed = [sum(v << (2 * i) for i, v in enumerate(row)) for row in table]
    code = jnp.where(z == 0, packed[0], jnp.where(z == 1, packed[1], jnp.where(z == 2, packed[2], packed[3])))
    return (code >> (2 * m)) & 3


def has(way, zc):
    return zc < LINE - 1 if way == TO_UPPER else zc > 0


def target(way, zc, y, c):
    return {TO_UPPER: (zc + 1) * 4 + y * 2 + c, TO_LOWER: (zc - 1) * 4 + y * 2 + c, TO_OTHER_LINE: zc * 4 + (1 - y) * 2 + c, TO_TWIN: zc * 4 + y * 2 + 1 - c}[way]


def greet(where):
    dp, z, y, c = where
    barrier = pltpu.get_barrier_semaphore()
    pl.when(z > 0)(lambda: pl.semaphore_signal(barrier, 1, device_id=(dp, target(TO_LOWER, z, y, c)), device_id_type=MESH_ID))
    pl.when(z < LINE - 1)(lambda: pl.semaphore_signal(barrier, 1, device_id=(dp, target(TO_UPPER, z, y, c)), device_id_type=MESH_ID))
    for way in (TO_OTHER_LINE, TO_TWIN):
        pl.semaphore_signal(barrier, 1, device_id=(dp, target(way, z, y, c)), device_id_type=MESH_ID)
    pl.semaphore_signal(barrier, 1, device_id=(1 - dp, z * 4 + y * 2 + c), device_id_type=MESH_ID)


def meet(where):
    dp, z, y, c = where
    pl.semaphore_wait(pltpu.get_barrier_semaphore(), 3 + (z + 3) // 4 + (6 - z) // 4)


class RowGather:
    def __init__(self, buf, send_sem, recv_sem, where, weights=None):
        self.buf, self.send_sem, self.recv_sem, self.weights = buf, send_sem, recv_sem, weights
        self.dp, self.z, self.y, self.c = where
        self.rows = buf.shape[0] // 16
        self.piece = self.rows // CHUNKS

    def copy(self, block, j, way, device):
        rows = pl.ds(pl.multiple_of(block * self.rows + j * self.piece, 16), self.piece)
        return pltpu.make_async_remote_copy(
            src_ref=self.buf.at[rows],
            dst_ref=self.buf.at[rows],
            send_sem=self.send_sem.at[way],
            recv_sem=self.recv_sem.at[block * CHUNKS + j],
            device_id=(self.dp, device),
            device_id_type=MESH_ID,
        )

    def arrived(self, block, j):
        self.copy(block, j, 0, 0).wait_recv()

    def spread(self, block, j, zc, ways):
        for way in ways:
            self.copy(block, j, way, target(way, zc, self.y, self.c)).start()

    def line_block(self, zc, far, way_in):
        at = zc - far if way_in == TO_UPPER else zc + far
        return at * 4 + self.y * 2 + self.c, at * 4 + (1 - self.y) * 2 + self.c

    def start(self):
        for zc in range(LINE):

            @pl.when(self.z == zc)
            def _(zc=zc):
                own, other = self.line_block(zc, 0, TO_UPPER)
                along = tuple(way for way in (TO_UPPER, TO_LOWER) if has(way, zc))
                self.spread(own, CHUNKS - 1, zc, (TO_OTHER_LINE,) + along + (TO_TWIN,))
                for j in range(ALONG_FIRST):
                    self.spread(own, j, zc, along + (TO_OTHER_LINE, TO_TWIN))
                if self.weights is not None:
                    self.weights.own(zc, along)
                self.arrived(other, CHUNKS - 1)
                self.spread(other, CHUNKS - 1, zc, along + (TO_TWIN,))

    def across(self, zc, m):
        block = ARRIVAL[zc][m] * 4 + (1 - self.y) * 2 + self.c
        for j in range(ALONG_FIRST):
            self.arrived(block, j)
            self.spread(block, j, zc, (TO_TWIN,))
        if self.weights is not None:
            self.weights.pass_on(block, zc, ())

    def step(self, s):
        for far in range(1, LINE + 1):
            for zc in range(LINE):

                @pl.when((self.z == zc) & (s == far - 1))
                def _(zc=zc, far=far):
                    ways = [way for way in (TO_UPPER, TO_LOWER) if 0 <= (zc - far if way == TO_UPPER else zc + far) < LINE]
                    for j in (CHUNKS - 1,) + tuple(range(ALONG_FIRST)):
                        for way in ways:
                            block = self.line_block(zc, far, way)[0]
                            onward = (way,) if has(way, zc) else ()
                            self.arrived(block, j)
                            self.spread(block, j, zc, onward + ((TO_OTHER_LINE,) if j < ALONG_FIRST else ()) + (TO_TWIN,))
                    for way in ways:
                        onward = (way,) if has(way, zc) else ()
                        block, other = self.line_block(zc, far, way)
                        if self.weights is not None:
                            self.weights.pass_on(block, zc, onward + (TO_OTHER_LINE,))
                        self.arrived(other, CHUNKS - 1)
                        self.spread(other, CHUNKS - 1, zc, onward + (TO_TWIN,))
                    self.across(zc, far - 1)

    def twin_arrived(self, block):
        for j in range(CHUNKS):
            self.arrived(block, j)

    def drain(self):
        def sent(way, pieces):
            rows = pl.ds(0, pieces * self.piece)
            pltpu.make_async_remote_copy(
                src_ref=self.buf.at[rows],
                dst_ref=self.buf.at[rows],
                send_sem=self.send_sem.at[way],
                recv_sem=self.recv_sem.at[0],
                device_id=(self.dp, 0),
                device_id_type=MESH_ID,
            ).wait_send()

        for zc in range(LINE):

            @pl.when(self.z == zc)
            def _(zc=zc):
                if zc < LINE - 1:
                    sent(TO_UPPER, (zc + 1) * (CHUNKS + 1))
                if zc > 0:
                    sent(TO_LOWER, (LINE - zc) * (CHUNKS + 1))

        sent(TO_OTHER_LINE, LINE * ALONG_FIRST + 1)
        sent(TO_TWIN, 2 * LINE * CHUNKS)


class WeightGather:
    def __init__(self, own_ref, full, send_sem, recv_sem, local_sem, where):
        self.own_ref, self.full, self.send_sem, self.recv_sem, self.local_sem = own_ref, full, send_sem, recv_sem, local_sem
        self.dp, self.z, self.y, self.c = where
        self.half = own_ref.shape[0] // 2

    def rows(self, block, half):
        return pl.ds(pl.multiple_of((block * 2 + half) * self.half, 16), self.half)

    def copy(self, src, block, half, way, device, group):
        return pltpu.make_async_remote_copy(
            src_ref=src,
            dst_ref=self.full.at[self.rows(block, half)],
            send_sem=self.send_sem.at[way],
            recv_sem=self.recv_sem.at[block * 2 + half],
            device_id=(group, device),
            device_id_type=MESH_ID,
        )

    def keep(self):
        block = self.z * 4 + self.y * 2 + self.c
        rows = pl.ds(pl.multiple_of(block * 2 * self.half, 16), 2 * self.half)
        return pltpu.make_async_copy(self.own_ref, self.full.at[rows], self.local_sem)

    def own(self, zc, along):
        block = zc * 4 + self.y * 2 + self.c
        mine = self.own_ref.at[pl.ds(pl.multiple_of(self.dp * self.half, 16), self.half)]
        for way in along + (TO_OTHER_LINE,):
            self.copy(mine, block, self.dp, way, target(way, zc, self.y, self.c), self.dp).start()
        for half in range(2):
            src = self.own_ref.at[pl.ds(half * self.half, self.half)]
            self.copy(src, block, half, TO_TWIN, target(TO_TWIN, zc, self.y, self.c), self.dp).start()

    def pass_on(self, block, zc, ways):
        held = self.full.at[self.rows(block, self.dp)]
        self.copy(held, block, self.dp, 0, 0, self.dp).wait_recv()
        for way in ways + (TO_TWIN,):
            self.copy(held, block, self.dp, way, target(way, zc, self.y, self.c), self.dp).start()
        me = zc * 4 + self.y * 2 + self.c
        self.copy(held, block, self.dp, TO_OTHER_GROUP, me, 1 - self.dp).start()

    def finish(self):
        me = self.z * 4 + self.y * 2 + self.c
        for k in range(1, 8):
            block = (me + 2 * k) % 16
            half = 1 - self.dp
            held = self.full.at[self.rows(block, half)]
            self.copy(held, block, half, 0, 0, self.dp).wait_recv()
            self.copy(held, block, half, TO_TWIN, me + 1 - 2 * self.c, self.dp).start()
        for k in range(8):
            block = (me + 2 * k) % 16 + 1 - 2 * self.c
            for half in range(2):
                self.copy(self.full.at[self.rows(block, half)], block, half, 0, 0, self.dp).wait_recv()

        def sent(way, halves):
            rows = pl.ds(0, halves * self.half)
            pltpu.make_async_remote_copy(
                src_ref=self.full.at[rows], dst_ref=self.full.at[rows], send_sem=self.send_sem.at[way], recv_sem=self.recv_sem.at[0],
                device_id=(self.dp, 0), device_id_type=MESH_ID).wait_send()

        for zc in range(LINE):

            @pl.when(self.z == zc)
            def _(zc=zc):
                if zc < LINE - 1:
                    sent(TO_UPPER, zc + 1)
                if zc > 0:
                    sent(TO_LOWER, LINE - zc)

        sent(TO_OTHER_LINE, LINE)
        sent(TO_TWIN, 16)
        sent(TO_OTHER_GROUP, 7)
        self.keep().wait()


def stage_chips(s):
    return jnp.where(s == 0, 0, 2 * s + 1), jnp.where(s == LINE - 1, 8, 2 * s + 3)


def chip_in_order(n, z, y):
    own = (n < 2) | (n == 3) | (n == 5)
    m = jnp.where(own, (n + 1) // 2, (n - 1) // 2)
    return chip_at(ARRIVAL, z, m), jnp.where(own, y, 1 - y)


def project_body(x_ref, gain_ref, wq_ref, wk_ref, wv_ref, bias_ref, base_cos_ref, base_sin_ref, step_cos_ref, step_sin_ref, w_o_ref,
                 q_ref, k_ref, v_ref, w_o_full, rows_buf, w_buf, send_sem, recv_sem, w_send, w_recv, local_sem):
    where = place()
    dp, z, y, c = where
    rows = x_ref.shape[0]
    head_dim = q_ref.shape[1]
    own_tokens = step_cos_ref.shape[0] // 16
    me = z * 4 + y * 2 + c
    own = pl.ds(pl.multiple_of(me * rows, 16), rows)
    greet(where)
    weights = WeightGather(w_o_ref, w_o_full, w_send, w_recv, local_sem, where)
    weights.keep().start()
    rows_buf[own, :] = scaled_norm(x_ref[...].astype(jnp.float32), gain_ref[...].astype(jnp.float32))
    meet(where)
    gather = RowGather(rows_buf, send_sem, recv_sem, where, weights)
    gather.start()
    for i, ref in enumerate((wq_ref, wk_ref, wv_ref)):
        w_buf[:, i * head_dim:(i + 1) * head_dim] = ref[...]

    def compute(block):
        at = pl.ds(pl.multiple_of(block * rows, 16), rows)
        out = jnp.dot(rows_buf[at, :], w_buf[...], preferred_element_type=jnp.float32)
        out = (out + bias_ref[...].astype(jnp.float32)).astype(jnp.bfloat16)
        steps = pl.ds(pl.multiple_of(block * own_tokens, 8), own_tokens)
        step_cos, step_sin = step_cos_ref[steps, :][None], step_sin_ref[steps, :][None]
        base_cos, base_sin = base_cos_ref[...][:, None, :], base_sin_ref[...][:, None, :]
        cos_t = (base_cos * step_cos - base_sin * step_sin).reshape(rows, head_dim)
        sin_t = (base_sin * step_cos + base_cos * step_sin).reshape(rows, head_dim)
        lane = lax.broadcasted_iota(jnp.int32, (rows, head_dim), 1)
        sin_t = jnp.where(lane < head_dim // 2, -sin_t, sin_t)
        for ref, i in ((q_ref, 0), (k_ref, 1)):
            wide = out[:, i * head_dim:(i + 1) * head_dim].astype(jnp.float32)
            ref[at, :] = (wide * cos_t + pltpu.roll(wide, head_dim // 2, 1) * sin_t).astype(jnp.bfloat16)
        v_ref[at, :] = out[:, 2 * head_dim:]

    @pl.loop(0, LINE)
    def _(s):
        gather.step(s)

        @pl.loop(*stage_chips(s))
        def _(n):
            at, line = chip_in_order(n, z, y)
            compute(at * 4 + line * 2 + c)
            twin = at * 4 + line * 2 + 1 - c
            gather.twin_arrived(twin)
            compute(twin)

    weights.finish()
    gather.drain()


def project_all(x_rows, gain, w_q, w_k, w_v, bias_all, w_o, prefix):
    n_req, own_tokens, width = x_rows.shape
    rows = n_req * own_tokens
    head_dim = w_q.shape[1]
    half = head_dim // 2
    inv_freq = ROPE_THETA ** (-(jnp.arange(half, dtype=jnp.float32) * 2.0) / head_dim)
    inv_freq = jnp.concatenate([inv_freq, inv_freq])[None, :]
    base = prefix.astype(jnp.float32)[:, None] * inv_freq
    step = jnp.arange(16 * own_tokens, dtype=jnp.float32)[:, None] * inv_freq
    vmem = pl.BlockSpec(memory_space=pltpu.VMEM)
    hbm = pl.BlockSpec(memory_space=pltpu.HBM)
    out = jax.ShapeDtypeStruct((16 * rows, head_dim), jnp.bfloat16)
    dma = pltpu.SemaphoreType.DMA
    *outs, w_o_full = pl.pallas_call(
        project_body,
        out_shape=(out, out, out, jax.ShapeDtypeStruct((16 * w_o.shape[0], w_o.shape[1]), jnp.bfloat16)),
        in_specs=[vmem] * 11,
        out_specs=(vmem,) * 3 + (hbm,),
        scratch_shapes=[
            pltpu.VMEM((16 * rows, width), jnp.bfloat16),
            pltpu.VMEM((width, 3 * head_dim), jnp.bfloat16),
            dma((4,)), dma((16 * CHUNKS,)), dma((5,)), dma((32,)), dma,
        ],
        compiler_params=pltpu.CompilerParams(collective_id=0, has_side_effects=True, vmem_limit_bytes=40 * 2**20),
        cost_estimate=pl.CostEstimate(flops=2 * 16 * rows * width * 3 * head_dim, bytes_accessed=4 * rows * width, transcendentals=0),
        name="project",
    )(x_rows.reshape(rows, width), gain[None, :], w_q, w_k, w_v, bias_all[None, :], jnp.cos(base), jnp.sin(base), jnp.cos(step), jnp.sin(step), w_o)
    return tuple(o.reshape(16, n_req, own_tokens, head_dim) for o in outs), w_o_full


def token_rows(ref):
    rows = ref[:, 0].astype(jnp.float32)
    return rows.reshape(rows.shape[0] * rows.shape[1], rows.shape[2])


def attention_body(prefix_ref, valid_ref, q_ref, kn_ref, vn_ref, k_ref, v_ref, o_ref, ko_ref, vo_ref, scores, top, total, acc):
    req = pl.program_id(0)
    start = prefix_ref[req]
    count = valid_ref[req]
    head_dim = q_ref.shape[3]
    n_tokens = q_ref.shape[0] * q_ref.shape[2]
    slots = k_ref.shape[1]
    ko_ref[...] = k_ref[...]
    vo_ref[...] = v_ref[...]
    base = pl.multiple_of(jnp.minimum((start // 16) * 16, slots - UPDATE_ROWS), 16)
    shift = start - base
    row = lax.broadcasted_iota(jnp.int32, (UPDATE_ROWS, head_dim), 0) - shift
    keep = (row >= 0) & (row < count)
    for src, dst in ((kn_ref, ko_ref), (vn_ref, vo_ref)):
        fresh = jnp.concatenate([token_rows(src), jnp.zeros((UPDATE_ROWS - n_tokens, head_dim), jnp.float32)], axis=0)
        fresh = pltpu.roll(fresh, shift, 0)
        old = dst[0, pl.ds(base, UPDATE_ROWS), :].astype(jnp.float32)
        dst[0, pl.ds(base, UPDATE_ROWS), :] = jnp.where(keep, fresh, old).astype(jnp.bfloat16)

    n_open = (start + 1) // KV_BLOCK
    n_used = pl.cdiv(start + count, KV_BLOCK)
    queries = token_rows(q_ref).astype(jnp.bfloat16)
    lanes = KV_BLOCK // 128
    top[...] = jnp.full_like(top, -1.0e30)

    def score(blk, masked):
        keys = ko_ref[0, pl.ds(pl.multiple_of(blk * KV_BLOCK, KV_BLOCK), KV_BLOCK), :]
        s = lax.dot_general(queries, keys, (((1,), (1,)), ((), ())), preferred_element_type=jnp.float32)
        if masked:
            col = lax.broadcasted_iota(jnp.int32, (n_tokens, KV_BLOCK), 1) + blk * KV_BLOCK
            row_id = lax.broadcasted_iota(jnp.int32, (n_tokens, KV_BLOCK), 0)
            s = jnp.where(col <= start + jnp.minimum(row_id, count - 1), s, -1.0e30)
        scores[blk] = s
        best = top[...]
        for j in range(lanes):
            best = jnp.maximum(best, s[:, j * 128:(j + 1) * 128])
        top[...] = best

    pl.loop(0, n_open)(lambda blk: score(blk, False))
    pl.loop(n_open, n_used)(lambda blk: score(blk, True))
    top[...] = jnp.broadcast_to(jnp.max(top[...], axis=1, keepdims=True), top.shape)
    total[...] = jnp.zeros_like(total)
    acc[...] = jnp.zeros_like(acc)

    @pl.loop(0, n_used)
    def _(blk):
        best = top[...]
        part = total[...]
        pieces = []
        for j in range(lanes):
            e = jnp.exp2((scores[blk, :, j * 128:(j + 1) * 128] - best) * (LOG2_E * head_dim ** -0.5))
            part = part + e
            pieces.append(e.astype(jnp.bfloat16))
        total[...] = part
        vals = vo_ref[0, pl.ds(pl.multiple_of(blk * KV_BLOCK, KV_BLOCK), KV_BLOCK), :]
        acc[...] += jnp.dot(jnp.concatenate(pieces, axis=1), vals, preferred_element_type=jnp.float32)

    mixed = acc[...] / jnp.sum(total[...], axis=1, keepdims=True)
    o_ref[:, 0] = mixed.reshape(o_ref.shape[0], o_ref.shape[2], head_dim).astype(jnp.bfloat16)


def attend(queries, keys_new, values_new, k_cache, v_cache, prefix, valid):
    owners, n_req, own_tokens, head_dim = queries.shape
    n_tokens = owners * own_tokens
    slots = k_cache.shape[1]
    new_spec = pl.BlockSpec((owners, 1, own_tokens, head_dim), lambda r, *_: (0, r, 0, 0))
    cache_spec = pl.BlockSpec((1, slots, head_dim), lambda r, *_: (r, 0, 0))
    cache_out = jax.ShapeDtypeStruct(k_cache.shape, jnp.bfloat16)
    return pl.pallas_call(
        attention_body,
        out_shape=(jax.ShapeDtypeStruct(queries.shape, jnp.bfloat16), cache_out, cache_out),
        grid_spec=pltpu.PrefetchScalarGridSpec(
            num_scalar_prefetch=2,
            grid=(n_req,),
            in_specs=[new_spec, new_spec, new_spec, cache_spec, cache_spec],
            out_specs=(new_spec, cache_spec, cache_spec),
            scratch_shapes=[
                pltpu.VMEM((slots // KV_BLOCK, n_tokens, KV_BLOCK), jnp.float32),
                pltpu.VMEM((n_tokens, 128), jnp.float32),
                pltpu.VMEM((n_tokens, 128), jnp.float32),
                pltpu.VMEM((n_tokens, head_dim), jnp.float32),
            ],
        ),
        compiler_params=pltpu.CompilerParams(dimension_semantics=("arbitrary",), vmem_limit_bytes=40 * 2**20),
        cost_estimate=pl.CostEstimate(flops=2 * 2 * n_req * n_tokens * slots * head_dim, bytes_accessed=8 * n_req * slots * head_dim, transcendentals=n_req * n_tokens * slots),
        name="attend",
    )(prefix, valid, queries, keys_new, values_new, k_cache, v_cache)


REDUCE = ((2, 3, 1, 0), (2, 3, 0, 1), (1, 0, 3, 2), (1, 0, 2, 3))


def finish_body(o_ref, x_ref, gain_ref, w_gate_ref, w_up_ref, w_down_ref, w_o_ref, out_ref,
                rows_buf, part, attended, resid, acc, from_twin, from_line, from_lower, from_upper,
                gather_send, gather_recv, reduce_send, twin_recv, line_recv, lower_recv, upper_recv, swap_send, swap_recv, local_sem):
    where = place()
    dp, z, y, c = where
    rows, width = x_ref.shape
    head_dim = o_ref.shape[1]
    me = z * 4 + y * 2 + c
    piece = rows // CHUNKS
    load = pltpu.make_async_copy(w_o_ref, part.at[pl.ds(0, w_o_ref.shape[0])], local_sem)
    load.start()
    barrier = pltpu.get_barrier_semaphore()
    for k in range(1, 16):
        pl.semaphore_signal(barrier, 1, device_id=(dp, (me + k) % 16), device_id_type=MESH_ID)
    pl.semaphore_wait(barrier, 15)

    def block_rows(block):
        return pl.ds(pl.multiple_of(block * rows, 16), rows)

    mine = pl.ds(pl.multiple_of(me * head_dim, 128), head_dim)
    for k in range(1, 16):
        other = (me + k) % 16
        pltpu.make_async_remote_copy(
            src_ref=o_ref.at[block_rows(other)], dst_ref=attended.at[:, mine], send_sem=swap_send, recv_sem=swap_recv,
            device_id=(dp, other), device_id_type=MESH_ID).start()
    attended[:, mine] = o_ref[block_rows(me), :]
    load.wait()
    others = o_ref.at[pl.ds(0, 15 * rows)]
    swap = pltpu.make_async_remote_copy(src_ref=others, dst_ref=others, send_sem=swap_send, recv_sem=swap_recv, device_id=(dp, 0), device_id_type=MESH_ID)
    swap.wait_recv()
    swap.wait_send()

    @pl.loop(0, width // 256)
    def _(n):
        cols = pl.ds(pl.multiple_of(n * 256, 256), 256)
        out = jnp.dot(attended[...], part[pl.ds(0, w_o_ref.shape[0]), cols], preferred_element_type=jnp.float32).astype(jnp.bfloat16)
        resid[:, cols] = (x_ref[:, cols].astype(jnp.float32) + out.astype(jnp.float32)).astype(jnp.bfloat16)

    rows_buf[block_rows(me), :] = scaled_norm(resid[...].astype(jnp.float32), gain_ref[...].astype(jnp.float32))
    gather = RowGather(rows_buf, gather_send, gather_recv, where)
    gather.start()

    def partial_sums(block):
        hidden = rows_buf[block_rows(block), :]
        dims = (((1,), (1,)), ((), ()))
        gate = lax.dot_general(hidden, w_gate_ref[...], dims, preferred_element_type=jnp.float32)
        up = lax.dot_general(hidden, w_up_ref[...], dims, preferred_element_type=jnp.float32)
        act = (jax.nn.silu(gate) * up).astype(jnp.bfloat16)
        part[block_rows(block), :] = jnp.dot(act, w_down_ref[...], preferred_element_type=jnp.float32).astype(jnp.bfloat16)

    def twin_copy(block, slot):
        return pltpu.make_async_remote_copy(
            src_ref=part.at[block_rows(block)], dst_ref=from_twin.at[block_rows(slot)], send_sem=reduce_send.at[TO_TWIN], recv_sem=twin_recv.at[slot],
            device_id=(dp, z * 4 + y * 2 + 1 - c), device_id_type=MESH_ID)

    last = CHUNKS - 1

    def piece_rows(block, j):
        return pl.ds(pl.multiple_of(block * rows + j * piece, 16), piece)

    def line_copy(dest, j):
        return pltpu.make_async_remote_copy(
            src_ref=part.at[piece_rows(dest * 4 + (1 - y) * 2 + c, j)], dst_ref=from_line.at[piece_rows(dest, j)],
            send_sem=reduce_send.at[TO_OTHER_LINE], recv_sem=line_recv.at[dest * CHUNKS + j],
            device_id=(dp, target(TO_OTHER_LINE, z, y, c)), device_id_type=MESH_ID)

    def slot(dest, line, j):
        far = jnp.where(line == y, dest * CHUNKS + j, LINE * CHUNKS + dest)
        return far, pl.ds(pl.multiple_of(far * piece, 16), piece)

    def along_copy(dest, line, j, way):
        index, land = slot(dest, line, j)
        buf, sems = (from_lower, lower_recv) if way == TO_UPPER else (from_upper, upper_recv)
        return pltpu.make_async_remote_copy(
            src_ref=part.at[piece_rows(dest * 4 + line * 2 + c, j)], dst_ref=buf.at[land],
            send_sem=reduce_send.at[way], recv_sem=sems.at[index], device_id=(dp, target(way, z, y, c)), device_id_type=MESH_ID)

    def line_send(dest):
        for j in range(ALONG_FIRST):
            line_copy(dest, j).start()

    def chips(lo, hi):
        @pl.loop(lo, hi)
        def _(n):
            at, line = chip_in_order(n, z, y)
            block = at * 4 + line * 2 + c
            twin = at * 4 + line * 2 + 1 - c
            gather.twin_arrived(twin)
            partial_sums(twin)
            twin_copy(twin, at * 2 + line).start()
            partial_sums(block)
            twin_copy(block, at * 2 + line).wait_recv()
            total = part[block_rows(block), :].astype(jnp.float32) + from_twin[block_rows(at * 2 + line), :].astype(jnp.float32)
            part[block_rows(block), :] = total.astype(jnp.bfloat16)

    @pl.loop(0, LINE)
    def _(s):
        gather.step(s)
        pl.when(s == LINE - 1)(lambda: line_send(chip_at(REDUCE, z, 0)))
        chips(*stage_chips(s))

    for i in range(1, LINE):
        line_send(chip_at(REDUCE, z, i))

    def add_along(dest, line, j):
        _, land = slot(dest, line, j)

        @pl.when((dest >= z) & (z > 0))
        def _():
            along_copy(dest, line, j, TO_UPPER).wait_recv()
            acc[...] += from_lower[land, :].astype(jnp.float32)

        @pl.when((dest <= z) & (z < LINE - 1))
        def _():
            along_copy(dest, line, j, TO_LOWER).wait_recv()
            acc[...] += from_upper[land, :].astype(jnp.float32)

        @pl.when((dest != z) | (j == last))
        def _():
            part[piece_rows(dest * 4 + line * 2 + c, j), :] = acc[...].astype(jnp.bfloat16)

        pl.when(dest > z)(lambda: along_copy(dest, line, j, TO_UPPER).start())
        pl.when(dest < z)(lambda: along_copy(dest, line, j, TO_LOWER).start())

    def result(j):
        out = pl.ds(pl.multiple_of(j * piece, 16), piece)
        down = acc[...].astype(jnp.bfloat16).astype(jnp.float32)
        out_ref[out, :] = (resid[out, :].astype(jnp.float32) + down).astype(jnp.bfloat16)

    @pl.loop(0, 2 * LINE)
    def _(step):
        dest = chip_at(REDUCE, z, step // 2)
        line = (y + 1 + step) % 2
        acc[...] = part[piece_rows(dest * 4 + line * 2 + c, last), :].astype(jnp.float32)
        add_along(dest, line, last)
        pl.when((dest == z) & (line != y))(lambda: line_copy(dest, last).start())

    @pl.loop(0, LINE * ALONG_FIRST)
    def _(step):
        dest = chip_at(REDUCE, z, step // ALONG_FIRST)
        j = step % ALONG_FIRST
        line_copy(dest, j).wait_recv()
        acc[...] = part[piece_rows(dest * 4 + y * 2 + c, j), :].astype(jnp.float32) + from_line[piece_rows(dest, j), :].astype(jnp.float32)
        add_along(dest, y, j)
        pl.when(dest == z)(lambda: result(j))

    line_copy(z, last).wait_recv()
    acc[...] = part[piece_rows(me, last), :].astype(jnp.float32) + from_line[piece_rows(z, last), :].astype(jnp.float32)
    result(last)
    gather.drain()

    def sent(way, pieces):
        span = pl.ds(0, pieces * piece)
        pltpu.make_async_remote_copy(
            src_ref=part.at[span], dst_ref=part.at[span], send_sem=reduce_send.at[way], recv_sem=twin_recv.at[0],
            device_id=(dp, 0), device_id_type=MESH_ID).wait_send()

    for zc in range(LINE):

        @pl.when(z == zc)
        def _(zc=zc):
            if zc < LINE - 1:
                sent(TO_UPPER, (LINE - 1 - zc) * (CHUNKS + 1))
            if zc > 0:
                sent(TO_LOWER, zc * (CHUNKS + 1))

    sent(TO_OTHER_LINE, LINE * ALONG_FIRST + 1)
    sent(TO_TWIN, 2 * LINE * CHUNKS)


def finish(attended, x_rows, gain, w_gate, w_up, w_down, w_o):
    n_req, own_tokens, width = x_rows.shape
    rows = n_req * own_tokens
    head_dim = attended.shape[-1]
    vmem = pl.BlockSpec(memory_space=pltpu.VMEM)
    bf16, f32 = jnp.bfloat16, jnp.float32
    dma = pltpu.SemaphoreType.DMA
    out = pl.pallas_call(
        finish_body,
        out_shape=jax.ShapeDtypeStruct((rows, width), bf16),
        in_specs=[vmem] * 6 + [pl.BlockSpec(memory_space=pltpu.HBM)],
        out_specs=vmem,
        scratch_shapes=[
            pltpu.VMEM((16 * rows, width), bf16),
            pltpu.VMEM((16 * rows, width), bf16),
            pltpu.VMEM((rows, width), bf16),
            pltpu.VMEM((rows, width), bf16),
            pltpu.VMEM((rows // CHUNKS, width), f32),
            pltpu.VMEM((8 * rows, width), bf16),
            pltpu.VMEM((LINE * rows, width), bf16),
            pltpu.VMEM((LINE * (rows + rows // CHUNKS), width), bf16),
            pltpu.VMEM((LINE * (rows + rows // CHUNKS), width), bf16),
            dma((4,)), dma((16 * CHUNKS,)), dma((4,)), dma((8,)), dma((LINE * CHUNKS,)), dma((LINE * (CHUNKS + 1),)), dma((LINE * (CHUNKS + 1),)), dma, dma, dma,
        ],
        compiler_params=pltpu.CompilerParams(collective_id=1, has_side_effects=True, vmem_limit_bytes=62 * 2**20),
        cost_estimate=pl.CostEstimate(flops=2 * rows * width * (width + 16 * 3 * w_down.shape[0]), bytes_accessed=4 * width * width, transcendentals=0),
        name="finish",
    )(attended.reshape(16 * rows, head_dim), x_rows.reshape(rows, width), gain[None, :], w_gate.T, w_up.T, w_down, w_o)
    return out.reshape(x_rows.shape)


def solution(mesh):
    row_spec = P("dp", "tp", None)
    cache_spec = P("dp", None, "tp", None)
    req_spec = P("dp")
    rep_spec = P(None)
    col_spec = P(None, "tp")
    bias_spec = P("tp")
    down_spec = P("tp", None)

    def layer(x_rows, k_cache, v_cache, prefix, valid, g_attn, w_q, b_q, w_k, b_k, w_v, b_v, w_o, g_mlp, w_gate, w_up, w_down):
        bias_all = jnp.concatenate([b_q, b_k, b_v])
        (queries, keys_new, values_new), w_o_full = project_all(x_rows, g_attn, w_q, w_k, w_v, bias_all, w_o, prefix)
        flat = (k_cache.shape[0], k_cache.shape[1], k_cache.shape[3])
        attended, k_out, v_out = attend(queries, keys_new, values_new, k_cache.reshape(flat), v_cache.reshape(flat), prefix, valid)
        x_out = finish(attended, x_rows, g_mlp, w_gate, w_up, w_down, w_o_full)
        return x_out, k_out.reshape(k_cache.shape), v_out.reshape(v_cache.shape)

    in_specs = (row_spec, cache_spec, cache_spec, req_spec, req_spec, rep_spec, col_spec, bias_spec, col_spec, bias_spec, col_spec, bias_spec, down_spec, rep_spec, col_spec, col_spec, down_spec)
    return jax.shard_map(layer, mesh=mesh, in_specs=in_specs, out_specs=(row_spec, cache_spec, cache_spec), check_vma=False)
```

```python
import functools
import jax
import jax.numpy as jnp
import numpy as np
from jax import lax
from jax.experimental import pallas as pl
from jax.experimental.pallas import tpu as pltpu
from jax.sharding import PartitionSpec as P

ROPE_THETA = 1.0e6
NORM_EPS = 1.0e-6
KV_BLOCK = 1024
UPDATE_ROWS = 400
LOG2_E = 1.4426950408889634


MESH_ID = pl.DeviceIdType.MESH
LINE = 4
CHUNKS = 6
ALONG_FIRST = CHUNKS - 1
TO_UPPER, TO_LOWER, TO_OTHER_LINE, TO_TWIN, TO_OTHER_GROUP = range(5)
ARRIVAL = ((0, 1, 2, 3), (1, 0, 2, 3), (2, 1, 3, 0), (3, 2, 1, 0))


def scaled_norm(wide_vals, gain):
    inv_rms = lax.rsqrt(jnp.mean(wide_vals * wide_vals, axis=-1, keepdims=True) + NORM_EPS)
    return (wide_vals * inv_rms * gain).astype(jnp.bfloat16)


def place():
    me = lax.axis_index("tp")
    return lax.axis_index("dp"), me // 4, (me // 2) % 2, me % 2


def chip_at(table, z, m):
    packed = [sum(v << (2 * i) for i, v in enumerate(row)) for row in table]
    code = jnp.where(z == 0, packed[0], jnp.where(z == 1, packed[1], jnp.where(z == 2, packed[2], packed[3])))
    return (code >> (2 * m)) & 3


def has(way, zc):
    return zc < LINE - 1 if way == TO_UPPER else zc > 0


def target(way, zc, y, c):
    return {TO_UPPER: (zc + 1) * 4 + y * 2 + c, TO_LOWER: (zc - 1) * 4 + y * 2 + c, TO_OTHER_LINE: zc * 4 + (1 - y) * 2 + c, TO_TWIN: zc * 4 + y * 2 + 1 - c}[way]


def greet(where):
    dp, z, y, c = where
    barrier = pltpu.get_barrier_semaphore()
    pl.when(z > 0)(lambda: pl.semaphore_signal(barrier, 1, device_id=(dp, target(TO_LOWER, z, y, c)), device_id_type=MESH_ID))
    pl.when(z < LINE - 1)(lambda: pl.semaphore_signal(barrier, 1, device_id=(dp, target(TO_UPPER, z, y, c)), device_id_type=MESH_ID))
    for way in (TO_OTHER_LINE, TO_TWIN):
        pl.semaphore_signal(barrier, 1, device_id=(dp, target(way, z, y, c)), device_id_type=MESH_ID)
    pl.semaphore_signal(barrier, 1, device_id=(1 - dp, z * 4 + y * 2 + c), device_id_type=MESH_ID)


def meet(where):
    dp, z, y, c = where
    pl.semaphore_wait(pltpu.get_barrier_semaphore(), 3 + (z + 3) // 4 + (6 - z) // 4)


class RowGather:
    def __init__(self, buf, send_sem, recv_sem, where, weights=None):
        self.buf, self.send_sem, self.recv_sem, self.weights = buf, send_sem, recv_sem, weights
        self.dp, self.z, self.y, self.c = where
        self.rows = buf.shape[0] // 16
        self.piece = self.rows // CHUNKS

    def copy(self, block, j, way, device):
        rows = pl.ds(pl.multiple_of(block * self.rows + j * self.piece, 16), self.piece)
        return pltpu.make_async_remote_copy(
            src_ref=self.buf.at[rows],
            dst_ref=self.buf.at[rows],
            send_sem=self.send_sem.at[way],
            recv_sem=self.recv_sem.at[block * CHUNKS + j],
            device_id=(self.dp, device),
            device_id_type=MESH_ID,
        )

    def arrived(self, block, j):
        self.copy(block, j, 0, 0).wait_recv()

    def spread(self, block, j, zc, ways):
        for way in ways:
            self.copy(block, j, way, target(way, zc, self.y, self.c)).start()

    def line_block(self, zc, far, way_in):
        at = zc - far if way_in == TO_UPPER else zc + far
        return at * 4 + self.y * 2 + self.c, at * 4 + (1 - self.y) * 2 + self.c

    def start(self):
        for zc in range(LINE):

            @pl.when(self.z == zc)
            def _(zc=zc):
                own, other = self.line_block(zc, 0, TO_UPPER)
                along = tuple(way for way in (TO_UPPER, TO_LOWER) if has(way, zc))
                if self.weights is not None:
                    self.weights.own(zc, along)
                self.spread(own, CHUNKS - 1, zc, (TO_OTHER_LINE,) + along + (TO_TWIN,))
                for j in range(ALONG_FIRST):
                    self.spread(own, j, zc, along + (TO_OTHER_LINE, TO_TWIN))
                self.arrived(other, CHUNKS - 1)
                self.spread(other, CHUNKS - 1, zc, along + (TO_TWIN,))

    def across(self, zc, m):
        block = ARRIVAL[zc][m] * 4 + (1 - self.y) * 2 + self.c
        if self.weights is not None:
            self.weights.pass_on(block, zc, ())
        for j in range(ALONG_FIRST):
            self.arrived(block, j)
            self.spread(block, j, zc, (TO_TWIN,))

    def step(self, s):
        for far in range(1, LINE + 1):
            for zc in range(LINE):

                @pl.when((self.z == zc) & (s == far - 1))
                def _(zc=zc, far=far):
                    ways = [way for way in (TO_UPPER, TO_LOWER) if 0 <= (zc - far if way == TO_UPPER else zc + far) < LINE]
                    if self.weights is not None:
                        for way in ways:
                            self.weights.pass_on(self.line_block(zc, far, way)[0], zc, ((way,) if has(way, zc) else ()) + (TO_OTHER_LINE,))
                    for j in (CHUNKS - 1,) + tuple(range(ALONG_FIRST)):
                        for way in ways:
                            block = self.line_block(zc, far, way)[0]
                            onward = (way,) if has(way, zc) else ()
                            self.arrived(block, j)
                            self.spread(block, j, zc, onward + ((TO_OTHER_LINE,) if j < ALONG_FIRST else ()) + (TO_TWIN,))
                    for way in ways:
                        onward = (way,) if has(way, zc) else ()
                        block, other = self.line_block(zc, far, way)
                        self.arrived(other, CHUNKS - 1)
                        self.spread(other, CHUNKS - 1, zc, onward + (TO_TWIN,))
                    self.across(zc, far - 1)

    def twin_arrived(self, block):
        for j in range(CHUNKS):
            self.arrived(block, j)

    def drain(self):
        def sent(way, pieces):
            rows = pl.ds(0, pieces * self.piece)
            pltpu.make_async_remote_copy(
                src_ref=self.buf.at[rows],
                dst_ref=self.buf.at[rows],
                send_sem=self.send_sem.at[way],
                recv_sem=self.recv_sem.at[0],
                device_id=(self.dp, 0),
                device_id_type=MESH_ID,
            ).wait_send()

        for zc in range(LINE):

            @pl.when(self.z == zc)
            def _(zc=zc):
                if zc < LINE - 1:
                    sent(TO_UPPER, (zc + 1) * (CHUNKS + 1))
                if zc > 0:
                    sent(TO_LOWER, (LINE - zc) * (CHUNKS + 1))

        sent(TO_OTHER_LINE, LINE * ALONG_FIRST + 1)
        sent(TO_TWIN, 2 * LINE * CHUNKS)


class WeightGather:
    def __init__(self, own_ref, full, send_sem, recv_sem, local_sem, where):
        self.own_ref, self.full, self.send_sem, self.recv_sem, self.local_sem = own_ref, full, send_sem, recv_sem, local_sem
        self.dp, self.z, self.y, self.c = where
        self.half = own_ref.shape[0] // 2

    def rows(self, block, half):
        return pl.ds(pl.multiple_of((block * 2 + half) * self.half, 16), self.half)

    def copy(self, src, block, half, way, device, group):
        return pltpu.make_async_remote_copy(
            src_ref=src,
            dst_ref=self.full.at[self.rows(block, half)],
            send_sem=self.send_sem.at[way],
            recv_sem=self.recv_sem.at[block * 2 + half],
            device_id=(group, device),
            device_id_type=MESH_ID,
        )

    def keep(self):
        block = self.z * 4 + self.y * 2 + self.c
        rows = pl.ds(pl.multiple_of(block * 2 * self.half, 16), 2 * self.half)
        return pltpu.make_async_copy(self.own_ref, self.full.at[rows], self.local_sem)

    def own(self, zc, along):
        block = zc * 4 + self.y * 2 + self.c
        mine = self.own_ref.at[pl.ds(pl.multiple_of(self.dp * self.half, 16), self.half)]
        for way in along + (TO_OTHER_LINE,):
            self.copy(mine, block, self.dp, way, target(way, zc, self.y, self.c), self.dp).start()
        for half in range(2):
            src = self.own_ref.at[pl.ds(half * self.half, self.half)]
            self.copy(src, block, half, TO_TWIN, target(TO_TWIN, zc, self.y, self.c), self.dp).start()

    def pass_on(self, block, zc, ways):
        held = self.full.at[self.rows(block, self.dp)]
        self.copy(held, block, self.dp, 0, 0, self.dp).wait_recv()
        for way in ways + (TO_TWIN,):
            self.copy(held, block, self.dp, way, target(way, zc, self.y, self.c), self.dp).start()
        me = zc * 4 + self.y * 2 + self.c
        self.copy(held, block, self.dp, TO_OTHER_GROUP, me, 1 - self.dp).start()

    def swapped(self, place_z, line):
        block, half = place_z * 4 + line * 2 + self.c, 1 - self.dp
        held = self.full.at[self.rows(block, half)]
        self.copy(held, block, half, 0, 0, self.dp).wait_recv()
        self.copy(held, block, half, TO_TWIN, target(TO_TWIN, self.z, self.y, self.c), self.dp).start()

    def swap_early(self):
        for m in range(LINE - 1):
            self.swapped(chip_at(ARRIVAL, self.z, m + 1), self.y)
            self.swapped(chip_at(ARRIVAL, self.z, m), 1 - self.y)

    def finish(self):
        me = self.z * 4 + self.y * 2 + self.c
        self.swapped(chip_at(ARRIVAL, self.z, LINE - 1), 1 - self.y)
        for k in range(8):
            block = (me + 2 * k) % 16 + 1 - 2 * self.c
            for half in range(2):
                self.copy(self.full.at[self.rows(block, half)], block, half, 0, 0, self.dp).wait_recv()

        def sent(way, halves):
            rows = pl.ds(0, halves * self.half)
            pltpu.make_async_remote_copy(
                src_ref=self.full.at[rows], dst_ref=self.full.at[rows], send_sem=self.send_sem.at[way], recv_sem=self.recv_sem.at[0],
                device_id=(self.dp, 0), device_id_type=MESH_ID).wait_send()

        for zc in range(LINE):

            @pl.when(self.z == zc)
            def _(zc=zc):
                if zc < LINE - 1:
                    sent(TO_UPPER, zc + 1)
                if zc > 0:
                    sent(TO_LOWER, LINE - zc)

        sent(TO_OTHER_LINE, LINE)
        sent(TO_TWIN, 16)
        sent(TO_OTHER_GROUP, 7)
        self.keep().wait()


def stage_chips(s):
    return jnp.where(s == 0, 0, 2 * s + 1), jnp.where(s == LINE - 1, 8, 2 * s + 3)


def chip_in_order(n, z, y):
    own = (n < 2) | (n == 3) | (n == 5)
    m = jnp.where(own, (n + 1) // 2, (n - 1) // 2)
    return chip_at(ARRIVAL, z, m), jnp.where(own, y, 1 - y)


def project_body(x_ref, gain_ref, wq_ref, wk_ref, wv_ref, bq_ref, bk_ref, bv_ref, base_cos_ref, base_sin_ref, step_cos_hbm, step_sin_hbm, w_o_ref,
                 q_ref, k_ref, v_ref, w_o_full, rows_buf, w_buf, send_sem, recv_sem, w_send, w_recv, local_sem, load_sem, step_cos_ref, step_sin_ref):
    where = place()
    dp, z, y, c = where
    rows = x_ref.shape[0]
    head_dim = q_ref.shape[1]
    own_tokens = step_cos_ref.shape[0] // 16
    me = z * 4 + y * 2 + c
    loads = [pltpu.make_async_copy(ref, w_buf.at[:, pl.ds(i * head_dim, head_dim)], load_sem.at[i]) for i, ref in enumerate((wq_ref, wk_ref, wv_ref))]
    loads += [pltpu.make_async_copy(step_cos_hbm, step_cos_ref, load_sem.at[3]), pltpu.make_async_copy(step_sin_hbm, step_sin_ref, load_sem.at[4])]
    own = pl.ds(pl.multiple_of(me * rows, 16), rows)
    greet(where)
    weights = WeightGather(w_o_ref, w_o_full, w_send, w_recv, local_sem, where)
    weights.keep().start()
    for load in loads:
        load.start()
    rows_buf[own, :] = scaled_norm(x_ref[...].astype(jnp.float32), gain_ref[...].astype(jnp.float32))
    meet(where)
    gather = RowGather(rows_buf, send_sem, recv_sem, where, weights)
    gather.start()
    for load in loads:
        load.wait()

    def compute(block):
        at = pl.ds(pl.multiple_of(block * rows, 16), rows)
        out = jnp.dot(rows_buf[at, :], w_buf[...], preferred_element_type=jnp.float32)
        bias = jnp.concatenate([ref[...].astype(jnp.float32) for ref in (bq_ref, bk_ref, bv_ref)], axis=1)
        out = (out + bias).astype(jnp.bfloat16)
        steps = pl.ds(pl.multiple_of(block * own_tokens, 8), own_tokens)
        step_cos, step_sin = step_cos_ref[steps, :][None], step_sin_ref[steps, :][None]
        base_cos, base_sin = base_cos_ref[...][:, None, :], base_sin_ref[...][:, None, :]
        cos_t = (base_cos * step_cos - base_sin * step_sin).reshape(rows, head_dim)
        sin_t = (base_sin * step_cos + base_cos * step_sin).reshape(rows, head_dim)
        lane = lax.broadcasted_iota(jnp.int32, (rows, head_dim), 1)
        sin_t = jnp.where(lane < head_dim // 2, -sin_t, sin_t)
        for ref, i in ((q_ref, 0), (k_ref, 1)):
            wide = out[:, i * head_dim:(i + 1) * head_dim].astype(jnp.float32)
            ref[at, :] = (wide * cos_t + pltpu.roll(wide, head_dim // 2, 1) * sin_t).astype(jnp.bfloat16)
        v_ref[at, :] = out[:, 2 * head_dim:]

    @pl.loop(0, LINE)
    def _(s):
        gather.step(s)
        pl.when(s == LINE - 1)(weights.swap_early)

        @pl.loop(*stage_chips(s))
        def _(n):
            at, line = chip_in_order(n, z, y)
            compute(at * 4 + line * 2 + c)
            twin = at * 4 + line * 2 + 1 - c
            gather.twin_arrived(twin)
            compute(twin)

    weights.finish()
    gather.drain()


def inverse_frequencies(head_dim):
    steps = np.arange(head_dim // 2, dtype=np.float32) * np.float32(2.0) / np.float32(head_dim)
    half = np.power(np.float32(ROPE_THETA), -steps).astype(np.float32)
    return np.concatenate([half, half])[None, :]


def project_all(x_rows, gain, w_q, w_k, w_v, biases, w_o, prefix):
    n_req, own_tokens, width = x_rows.shape
    rows = n_req * own_tokens
    head_dim = w_q.shape[1]
    inv_freq = jnp.asarray(inverse_frequencies(head_dim))
    base = prefix.astype(jnp.float32)[:, None] * inv_freq
    step = np.arange(16 * own_tokens, dtype=np.float32)[:, None] * inverse_frequencies(head_dim)
    step_cos, step_sin = np.cos(step), np.sin(step)
    vmem = pl.BlockSpec(memory_space=pltpu.VMEM)
    hbm = pl.BlockSpec(memory_space=pltpu.HBM)
    out = jax.ShapeDtypeStruct((16 * rows, head_dim), jnp.bfloat16)
    dma = pltpu.SemaphoreType.DMA
    *outs, w_o_full = pl.pallas_call(
        project_body,
        out_shape=(out, out, out, jax.ShapeDtypeStruct((16 * w_o.shape[0], w_o.shape[1]), jnp.bfloat16)),
        in_specs=[vmem] * 2 + [hbm] * 3 + [vmem] * 5 + [hbm] * 2 + [vmem],
        out_specs=(vmem,) * 3 + (hbm,),
        scratch_shapes=[
            pltpu.VMEM((16 * rows, width), jnp.bfloat16),
            pltpu.VMEM((width, 3 * head_dim), jnp.bfloat16),
            dma((4,)), dma((16 * CHUNKS,)), dma((5,)), dma((32,)), dma, dma((5,)),
            pltpu.VMEM(step_cos.shape, jnp.float32), pltpu.VMEM(step_sin.shape, jnp.float32),
        ],
        compiler_params=pltpu.CompilerParams(collective_id=0, has_side_effects=True, vmem_limit_bytes=62 * 2**20),
        cost_estimate=pl.CostEstimate(flops=2 * 16 * rows * width * 3 * head_dim, bytes_accessed=4 * rows * width, transcendentals=0),
        name="project",
    )(x_rows.reshape(rows, width), gain.reshape(1, width), w_q, w_k, w_v, *biases, jnp.cos(base), jnp.sin(base), step_cos, step_sin, w_o)
    return tuple(o.reshape(16, n_req, own_tokens, head_dim) for o in outs), w_o_full


def token_rows(ref):
    rows = ref[:, 0].astype(jnp.float32)
    return rows.reshape(rows.shape[0] * rows.shape[1], rows.shape[2])


def attention_body(prefix_ref, valid_ref, q_ref, kn_ref, vn_ref, k_ref, v_ref, o_ref, ko_ref, vo_ref, scores, top, total, acc):
    req = pl.program_id(0)
    start = prefix_ref[req]
    count = valid_ref[req]
    head_dim = q_ref.shape[3]
    n_tokens = q_ref.shape[0] * q_ref.shape[2]
    slots = k_ref.shape[1]
    ko_ref[...] = k_ref[...]
    vo_ref[...] = v_ref[...]
    base = pl.multiple_of(jnp.minimum((start // 16) * 16, slots - UPDATE_ROWS), 16)
    shift = start - base
    row = lax.broadcasted_iota(jnp.int32, (UPDATE_ROWS, head_dim), 0) - shift
    keep = (row >= 0) & (row < count)
    for src, dst in ((kn_ref, ko_ref), (vn_ref, vo_ref)):
        fresh = jnp.concatenate([token_rows(src), jnp.zeros((UPDATE_ROWS - n_tokens, head_dim), jnp.float32)], axis=0)
        fresh = pltpu.roll(fresh, shift, 0)
        old = dst[0, pl.ds(base, UPDATE_ROWS), :].astype(jnp.float32)
        dst[0, pl.ds(base, UPDATE_ROWS), :] = jnp.where(keep, fresh, old).astype(jnp.bfloat16)

    n_open = (start + 1) // KV_BLOCK
    n_used = pl.cdiv(start + count, KV_BLOCK)
    queries = token_rows(q_ref).astype(jnp.bfloat16)
    lanes = KV_BLOCK // 128
    top[...] = jnp.full_like(top, -1.0e30)

    def score(blk, masked):
        keys = ko_ref[0, pl.ds(pl.multiple_of(blk * KV_BLOCK, KV_BLOCK), KV_BLOCK), :]
        s = lax.dot_general(queries, keys, (((1,), (1,)), ((), ())), preferred_element_type=jnp.float32)
        if masked:
            col = lax.broadcasted_iota(jnp.int32, (n_tokens, KV_BLOCK), 1) + blk * KV_BLOCK
            row_id = lax.broadcasted_iota(jnp.int32, (n_tokens, KV_BLOCK), 0)
            s = jnp.where(col <= start + jnp.minimum(row_id, count - 1), s, -1.0e30)
        scores[blk] = s
        best = top[...]
        for j in range(lanes):
            best = jnp.maximum(best, s[:, j * 128:(j + 1) * 128])
        top[...] = best

    pl.loop(0, n_open)(lambda blk: score(blk, False))
    pl.loop(n_open, n_used)(lambda blk: score(blk, True))
    top[...] = jnp.broadcast_to(jnp.max(top[...], axis=1, keepdims=True), top.shape)
    total[...] = jnp.zeros_like(total)
    acc[...] = jnp.zeros_like(acc)

    @pl.loop(0, n_used)
    def _(blk):
        best = top[...]
        part = total[...]
        pieces = []
        for j in range(lanes):
            e = jnp.exp2((scores[blk, :, j * 128:(j + 1) * 128] - best) * (LOG2_E * head_dim ** -0.5))
            part = part + e
            pieces.append(e.astype(jnp.bfloat16))
        total[...] = part
        vals = vo_ref[0, pl.ds(pl.multiple_of(blk * KV_BLOCK, KV_BLOCK), KV_BLOCK), :]
        acc[...] += jnp.dot(jnp.concatenate(pieces, axis=1), vals, preferred_element_type=jnp.float32)

    mixed = acc[...] / jnp.sum(total[...], axis=1, keepdims=True)
    o_ref[:, 0] = mixed.reshape(o_ref.shape[0], o_ref.shape[2], head_dim).astype(jnp.bfloat16)


def attend(queries, keys_new, values_new, k_cache, v_cache, prefix, valid):
    owners, n_req, own_tokens, head_dim = queries.shape
    n_tokens = owners * own_tokens
    slots = k_cache.shape[1]
    new_spec = pl.BlockSpec((owners, 1, own_tokens, head_dim), lambda r, *_: (0, r, 0, 0))
    cache_spec = pl.BlockSpec((1, slots, head_dim), lambda r, *_: (r, 0, 0))
    cache_out = jax.ShapeDtypeStruct(k_cache.shape, jnp.bfloat16)
    return pl.pallas_call(
        attention_body,
        out_shape=(jax.ShapeDtypeStruct(queries.shape, jnp.bfloat16), cache_out, cache_out),
        grid_spec=pltpu.PrefetchScalarGridSpec(
            num_scalar_prefetch=2,
            grid=(n_req,),
            in_specs=[new_spec, new_spec, new_spec, cache_spec, cache_spec],
            out_specs=(new_spec, cache_spec, cache_spec),
            scratch_shapes=[
                pltpu.VMEM((slots // KV_BLOCK, n_tokens, KV_BLOCK), jnp.float32),
                pltpu.VMEM((n_tokens, 128), jnp.float32),
                pltpu.VMEM((n_tokens, 128), jnp.float32),
                pltpu.VMEM((n_tokens, head_dim), jnp.float32),
            ],
        ),
        compiler_params=pltpu.CompilerParams(dimension_semantics=("arbitrary",), vmem_limit_bytes=62 * 2**20),
        cost_estimate=pl.CostEstimate(flops=2 * 2 * n_req * n_tokens * slots * head_dim, bytes_accessed=8 * n_req * slots * head_dim, transcendentals=n_req * n_tokens * slots),
        name="attend",
    )(prefix, valid, queries, keys_new, values_new, k_cache, v_cache)


REDUCE = ((2, 3, 1, 0), (2, 3, 0, 1), (1, 0, 3, 2), (1, 0, 2, 3))


def finish_body(o_ref, x_ref, gain_ref, w_gate_hbm, w_up_hbm, w_down_hbm, w_o_ref, out_ref,
                rows_buf, part, swapped, attended, resid, acc, from_twin, from_line, from_lower, from_upper,
                gather_send, gather_recv, reduce_send, twin_recv, line_recv, lower_recv, upper_recv, swap_send, swap_recv, local_sem, w_gate_ref, w_up_ref, w_down_ref):
    where = place()
    dp, z, y, c = where
    rows, width = x_ref.shape
    head_dim = o_ref.shape[1]
    me = z * 4 + y * 2 + c
    piece = rows // CHUNKS
    load = pltpu.make_async_copy(w_o_ref, part.at[pl.ds(0, w_o_ref.shape[0])], local_sem.at[0])
    load.start()
    pairs = ((w_gate_hbm, w_gate_ref), (w_up_hbm, w_up_ref), (w_down_hbm, w_down_ref))
    mlp_loads = [pltpu.make_async_copy(src, dst, local_sem.at[1 + i]) for i, (src, dst) in enumerate(pairs)]
    for mlp_load in mlp_loads:
        mlp_load.start()
    barrier = pltpu.get_barrier_semaphore()
    for k in range(1, 16):
        pl.semaphore_signal(barrier, 1, device_id=(dp, (me + k) % 16), device_id_type=MESH_ID)
    pl.semaphore_wait(barrier, 15)

    def block_rows(block):
        return pl.ds(pl.multiple_of(block * rows, 16), rows)

    for k in range(1, 16):
        other = (me + k) % 16
        pltpu.make_async_remote_copy(
            src_ref=o_ref.at[block_rows(other)], dst_ref=swapped.at[block_rows(me)], send_sem=swap_send, recv_sem=swap_recv,
            device_id=(dp, other), device_id_type=MESH_ID).start()
    swapped[block_rows(me), :] = o_ref[block_rows(me), :]
    load.wait()
    others = o_ref.at[pl.ds(0, 15 * rows)]
    swap = pltpu.make_async_remote_copy(src_ref=others, dst_ref=others, send_sem=swap_send, recv_sem=swap_recv, device_id=(dp, 0), device_id_type=MESH_ID)
    swap.wait_recv()
    swap.wait_send()
    for head in range(16):
        attended[:, head * head_dim:(head + 1) * head_dim] = swapped[head * rows:(head + 1) * rows, :]

    @pl.loop(0, width // 512)
    def _(n):
        cols = pl.ds(pl.multiple_of(n * 512, 512), 512)
        out = jnp.dot(attended[...], part[pl.ds(0, w_o_ref.shape[0]), cols], preferred_element_type=jnp.float32).astype(jnp.bfloat16)
        resid[:, cols] = (x_ref[:, cols].astype(jnp.float32) + out.astype(jnp.float32)).astype(jnp.bfloat16)

    rows_buf[block_rows(me), :] = scaled_norm(resid[...].astype(jnp.float32), gain_ref[...].astype(jnp.float32))
    gather = RowGather(rows_buf, gather_send, gather_recv, where)
    gather.start()
    for mlp_load in mlp_loads:
        mlp_load.wait()

    def partial_sums(block):
        hidden = rows_buf[block_rows(block), :]
        dims = (((1,), (1,)), ((), ()))
        gate = lax.dot_general(hidden, w_gate_ref[...], dims, preferred_element_type=jnp.float32)
        up = lax.dot_general(hidden, w_up_ref[...], dims, preferred_element_type=jnp.float32)
        act = (jax.nn.silu(gate) * up).astype(jnp.bfloat16)
        part[block_rows(block), :] = jnp.dot(act, w_down_ref[...], preferred_element_type=jnp.float32).astype(jnp.bfloat16)

    def twin_copy(block, slot):
        return pltpu.make_async_remote_copy(
            src_ref=part.at[block_rows(block)], dst_ref=from_twin.at[block_rows(slot)], send_sem=reduce_send.at[TO_TWIN], recv_sem=twin_recv.at[slot],
            device_id=(dp, z * 4 + y * 2 + 1 - c), device_id_type=MESH_ID)

    last = CHUNKS - 1

    def piece_rows(block, j):
        return pl.ds(pl.multiple_of(block * rows + j * piece, 16), piece)

    def line_copy(dest, j):
        return pltpu.make_async_remote_copy(
            src_ref=part.at[piece_rows(dest * 4 + (1 - y) * 2 + c, j)], dst_ref=from_line.at[piece_rows(dest, j)],
            send_sem=reduce_send.at[TO_OTHER_LINE], recv_sem=line_recv.at[dest * CHUNKS + j],
            device_id=(dp, target(TO_OTHER_LINE, z, y, c)), device_id_type=MESH_ID)

    def slot(dest, line, j):
        far = jnp.where(line == y, dest * CHUNKS + j, LINE * CHUNKS + dest)
        return far, pl.ds(pl.multiple_of(far * piece, 16), piece)

    def along_copy(dest, line, j, way):
        index, land = slot(dest, line, j)
        buf, sems = (from_lower, lower_recv) if way == TO_UPPER else (from_upper, upper_recv)
        return pltpu.make_async_remote_copy(
            src_ref=part.at[piece_rows(dest * 4 + line * 2 + c, j)], dst_ref=buf.at[land],
            send_sem=reduce_send.at[way], recv_sem=sems.at[index], device_id=(dp, target(way, z, y, c)), device_id_type=MESH_ID)

    def line_send(dest):
        for j in range(ALONG_FIRST):
            line_copy(dest, j).start()

    def chips(lo, hi):
        @pl.loop(lo, hi)
        def _(n):
            at, line = chip_in_order(n, z, y)
            block = at * 4 + line * 2 + c
            twin = at * 4 + line * 2 + 1 - c
            gather.twin_arrived(twin)
            partial_sums(twin)
            twin_copy(twin, at * 2 + line).start()
            partial_sums(block)
            twin_copy(block, at * 2 + line).wait_recv()
            total = part[block_rows(block), :].astype(jnp.float32) + from_twin[block_rows(at * 2 + line), :].astype(jnp.float32)
            part[block_rows(block), :] = total.astype(jnp.bfloat16)

    def add_along(dest, line, j):
        _, land = slot(dest, line, j)

        @pl.when((dest >= z) & (z > 0))
        def _():
            along_copy(dest, line, j, TO_UPPER).wait_recv()
            acc[...] += from_lower[land, :].astype(jnp.float32)

        @pl.when((dest <= z) & (z < LINE - 1))
        def _():
            along_copy(dest, line, j, TO_LOWER).wait_recv()
            acc[...] += from_upper[land, :].astype(jnp.float32)

        @pl.when((dest != z) | (j == last))
        def _():
            part[piece_rows(dest * 4 + line * 2 + c, j), :] = acc[...].astype(jnp.bfloat16)

        pl.when(dest > z)(lambda: along_copy(dest, line, j, TO_UPPER).start())
        pl.when(dest < z)(lambda: along_copy(dest, line, j, TO_LOWER).start())

    def result(j):
        out = pl.ds(pl.multiple_of(j * piece, 16), piece)
        down = acc[...].astype(jnp.bfloat16).astype(jnp.float32)
        out_ref[out, :] = (resid[out, :].astype(jnp.float32) + down).astype(jnp.bfloat16)

    at_end = (z == 0) | (z == LINE - 1)

    def last_piece(step):
        dest = chip_at(REDUCE, z, step // 2)
        line = (y + 1 + step) % 2
        acc[...] = part[piece_rows(dest * 4 + line * 2 + c, last), :].astype(jnp.float32)
        add_along(dest, line, last)
        pl.when((dest == z) & (line != y))(lambda: line_copy(dest, last).start())

    def before_last():
        line_send(chip_at(REDUCE, z, 0))

        @pl.when(at_end)
        def _():
            last_piece(0)
            last_piece(1)
            last_piece(3)

    @pl.loop(0, LINE)
    def _(s):
        pl.when(s == LINE - 1)(before_last)
        gather.step(s)
        chips(*stage_chips(s))

    for i in range(1, LINE):
        line_send(chip_at(REDUCE, z, i))

    @pl.loop(0, 2 * LINE - 2)
    def _(step):
        pl.when(jnp.logical_not(at_end) | (step == 2) | (step >= 4))(lambda: last_piece(step))

    @pl.loop(0, LINE * ALONG_FIRST + 2)
    def _(n):
        swing = (LINE - 1) * ALONG_FIRST

        @pl.when((n >= swing) & (n < swing + 2))
        def _():
            last_piece(2 * LINE - 2 + n - swing)

        @pl.when((n < swing) | (n >= swing + 2))
        def _():
            step = jnp.where(n < swing, n, n - 2)
            dest = chip_at(REDUCE, z, step // ALONG_FIRST)
            j = step % ALONG_FIRST
            line_copy(dest, j).wait_recv()
            acc[...] = part[piece_rows(dest * 4 + y * 2 + c, j), :].astype(jnp.float32) + from_line[piece_rows(dest, j), :].astype(jnp.float32)
            add_along(dest, y, j)
            pl.when(dest == z)(lambda: result(j))

    line_copy(z, last).wait_recv()
    acc[...] = part[piece_rows(me, last), :].astype(jnp.float32) + from_line[piece_rows(z, last), :].astype(jnp.float32)
    result(last)
    gather.drain()

    def sent(way, pieces):
        span = pl.ds(0, pieces * piece)
        pltpu.make_async_remote_copy(
            src_ref=part.at[span], dst_ref=part.at[span], send_sem=reduce_send.at[way], recv_sem=twin_recv.at[0],
            device_id=(dp, 0), device_id_type=MESH_ID).wait_send()

    for zc in range(LINE):

        @pl.when(z == zc)
        def _(zc=zc):
            if zc < LINE - 1:
                sent(TO_UPPER, (LINE - 1 - zc) * (CHUNKS + 1))
            if zc > 0:
                sent(TO_LOWER, zc * (CHUNKS + 1))

    sent(TO_OTHER_LINE, LINE * ALONG_FIRST + 1)
    sent(TO_TWIN, 2 * LINE * CHUNKS)


def finish(attended, x_rows, gain, w_gate, w_up, w_down, w_o):
    n_req, own_tokens, width = x_rows.shape
    rows = n_req * own_tokens
    head_dim = attended.shape[-1]
    vmem = pl.BlockSpec(memory_space=pltpu.VMEM)
    bf16, f32 = jnp.bfloat16, jnp.float32
    dma = pltpu.SemaphoreType.DMA
    out = pl.pallas_call(
        finish_body,
        out_shape=jax.ShapeDtypeStruct((rows, width), bf16),
        in_specs=[vmem] * 3 + [pl.BlockSpec(memory_space=pltpu.HBM)] * 4,
        out_specs=vmem,
        scratch_shapes=[
            pltpu.VMEM((16 * rows, width), bf16),
            pltpu.VMEM((16 * rows, width), bf16),
            pltpu.VMEM((16 * rows, head_dim), bf16),
            pltpu.VMEM((rows, width), bf16),
            pltpu.VMEM((rows, width), bf16),
            pltpu.VMEM((rows // CHUNKS, width), f32),
            pltpu.VMEM((8 * rows, width), bf16),
            pltpu.VMEM((LINE * rows, width), bf16),
            pltpu.VMEM((LINE * (rows + rows // CHUNKS), width), bf16),
            pltpu.VMEM((LINE * (rows + rows // CHUNKS), width), bf16),
            dma((4,)), dma((16 * CHUNKS,)), dma((4,)), dma((8,)), dma((LINE * CHUNKS,)), dma((LINE * (CHUNKS + 1),)), dma((LINE * (CHUNKS + 1),)), dma, dma, dma((4,)),
            pltpu.VMEM(w_gate.T.shape, bf16), pltpu.VMEM(w_up.T.shape, bf16), pltpu.VMEM(w_down.shape, bf16),
        ],
        compiler_params=pltpu.CompilerParams(collective_id=1, has_side_effects=True, vmem_limit_bytes=62 * 2**20),
        cost_estimate=pl.CostEstimate(flops=2 * rows * width * (width + 16 * 3 * w_down.shape[0]), bytes_accessed=4 * width * width, transcendentals=0),
        name="finish",
    )(attended.reshape(16 * rows, head_dim), x_rows.reshape(rows, width), gain[None, :], w_gate.T, w_up.T, w_down, w_o)
    return out.reshape(x_rows.shape)


def solution(mesh):
    row_spec = P("dp", "tp", None)
    cache_spec = P("dp", None, "tp", None)
    req_spec = P("dp")
    rep_spec = P(None)
    col_spec = P(None, "tp")
    bias_spec = P("tp")
    down_spec = P("tp", None)

    def layer(x_rows, k_cache, v_cache, prefix, valid, g_attn, w_q, b_q, w_k, b_k, w_v, b_v, w_o, g_mlp, w_gate, w_up, w_down):
        biases = [b.reshape(1, -1) for b in (b_q, b_k, b_v)]
        (queries, keys_new, values_new), w_o_full = project_all(x_rows, g_attn, w_q, w_k, w_v, biases, w_o, prefix)
        flat = (k_cache.shape[0], k_cache.shape[1], k_cache.shape[3])
        attended, k_out, v_out = attend(queries, keys_new, values_new, k_cache.reshape(flat), v_cache.reshape(flat), prefix, valid)
        x_out = finish(attended, x_rows, g_mlp, w_gate, w_up, w_down, w_o_full)
        return x_out, k_out.reshape(k_cache.shape), v_out.reshape(v_cache.shape)

    in_specs = (row_spec, cache_spec, cache_spec, req_spec, req_spec, rep_spec, col_spec, bias_spec, col_spec, bias_spec, col_spec, bias_spec, down_spec, rep_spec, col_spec, col_spec, down_spec)
    return jax.shard_map(layer, mesh=mesh, in_specs=in_specs, out_specs=(row_spec, cache_spec, cache_spec), check_vma=False)
```

```python
import functools
import jax
import jax.numpy as jnp
import numpy as np
from jax import lax
from jax.experimental import pallas as pl
from jax.experimental.pallas import tpu as pltpu
from jax.sharding import PartitionSpec as P

ROPE_THETA = 1.0e6
NORM_EPS = 1.0e-6
KV_BLOCK = 1024
UPDATE_ROWS = 400
LOG2_E = 1.4426950408889634


MESH_ID = pl.DeviceIdType.MESH
LINE = 4
CHUNKS = 6
ALONG_FIRST = CHUNKS - 1
TO_UPPER, TO_LOWER, TO_OTHER_LINE, TO_TWIN, TO_OTHER_GROUP = range(5)
ARRIVAL = ((0, 1, 2, 3), (1, 0, 2, 3), (2, 1, 3, 0), (3, 2, 1, 0))


def scaled_norm(wide_vals, gain):
    inv_rms = lax.rsqrt(jnp.mean(wide_vals * wide_vals, axis=-1, keepdims=True) + NORM_EPS)
    return (wide_vals * inv_rms * gain).astype(jnp.bfloat16)


def place():
    me = lax.axis_index("tp")
    return lax.axis_index("dp"), me // 4, (me // 2) % 2, me % 2


def chip_at(table, z, m):
    packed = [sum(v << (2 * i) for i, v in enumerate(row)) for row in table]
    code = jnp.where(z == 0, packed[0], jnp.where(z == 1, packed[1], jnp.where(z == 2, packed[2], packed[3])))
    return (code >> (2 * m)) & 3


def has(way, zc):
    return zc < LINE - 1 if way == TO_UPPER else zc > 0


def target(way, zc, y, c):
    return {TO_UPPER: (zc + 1) * 4 + y * 2 + c, TO_LOWER: (zc - 1) * 4 + y * 2 + c, TO_OTHER_LINE: zc * 4 + (1 - y) * 2 + c, TO_TWIN: zc * 4 + y * 2 + 1 - c}[way]


def greet(where):
    dp, z, y, c = where
    barrier = pltpu.get_barrier_semaphore()
    pl.when(z > 0)(lambda: pl.semaphore_signal(barrier, 1, device_id=(dp, target(TO_LOWER, z, y, c)), device_id_type=MESH_ID))
    pl.when(z < LINE - 1)(lambda: pl.semaphore_signal(barrier, 1, device_id=(dp, target(TO_UPPER, z, y, c)), device_id_type=MESH_ID))
    for way in (TO_OTHER_LINE, TO_TWIN):
        pl.semaphore_signal(barrier, 1, device_id=(dp, target(way, z, y, c)), device_id_type=MESH_ID)
    pl.semaphore_signal(barrier, 1, device_id=(1 - dp, z * 4 + y * 2 + c), device_id_type=MESH_ID)


def meet(where):
    dp, z, y, c = where
    pl.semaphore_wait(pltpu.get_barrier_semaphore(), 3 + (z + 3) // 4 + (6 - z) // 4)


class RowGather:
    def __init__(self, buf, send_sem, recv_sem, where, weights=None):
        self.buf, self.send_sem, self.recv_sem, self.weights = buf, send_sem, recv_sem, weights
        self.dp, self.z, self.y, self.c = where
        self.rows = buf.shape[0] // 16
        self.piece = self.rows // CHUNKS

    def copy(self, block, j, way, device):
        rows = pl.ds(pl.multiple_of(block * self.rows + j * self.piece, 16), self.piece)
        return pltpu.make_async_remote_copy(
            src_ref=self.buf.at[rows],
            dst_ref=self.buf.at[rows],
            send_sem=self.send_sem.at[way],
            recv_sem=self.recv_sem.at[block * CHUNKS + j],
            device_id=(self.dp, device),
            device_id_type=MESH_ID,
        )

    def arrived(self, block, j):
        self.copy(block, j, 0, 0).wait_recv()

    def spread(self, block, j, zc, ways):
        for way in ways:
            self.copy(block, j, way, target(way, zc, self.y, self.c)).start()

    def line_block(self, zc, far, way_in):
        at = zc - far if way_in == TO_UPPER else zc + far
        return at * 4 + self.y * 2 + self.c, at * 4 + (1 - self.y) * 2 + self.c

    def start(self):
        for zc in range(LINE):

            @pl.when(self.z == zc)
            def _(zc=zc):
                own, other = self.line_block(zc, 0, TO_UPPER)
                along = tuple(way for way in (TO_UPPER, TO_LOWER) if has(way, zc))
                if self.weights is not None:
                    self.weights.own(zc, along)
                self.spread(own, CHUNKS - 1, zc, (TO_OTHER_LINE,) + along + (TO_TWIN,))
                for j in range(ALONG_FIRST):
                    self.spread(own, j, zc, along + (TO_OTHER_LINE, TO_TWIN))
                self.arrived(other, CHUNKS - 1)
                self.spread(other, CHUNKS - 1, zc, along + (TO_TWIN,))

    def across(self, zc, m):
        block = ARRIVAL[zc][m] * 4 + (1 - self.y) * 2 + self.c
        if self.weights is not None:
            self.weights.pass_on(block, zc, ())
        for j in range(ALONG_FIRST):
            self.arrived(block, j)
            self.spread(block, j, zc, (TO_TWIN,))

    def step(self, s):
        for far in range(1, LINE + 1):
            for zc in range(LINE):

                @pl.when((self.z == zc) & (s == far - 1))
                def _(zc=zc, far=far):
                    ways = [way for way in (TO_UPPER, TO_LOWER) if 0 <= (zc - far if way == TO_UPPER else zc + far) < LINE]
                    if self.weights is not None:
                        for way in ways:
                            self.weights.pass_on(self.line_block(zc, far, way)[0], zc, ((way,) if has(way, zc) else ()) + (TO_OTHER_LINE,))
                    for j in (CHUNKS - 1,) + tuple(range(ALONG_FIRST)):
                        for way in ways:
                            block = self.line_block(zc, far, way)[0]
                            onward = (way,) if has(way, zc) else ()
                            self.arrived(block, j)
                            self.spread(block, j, zc, onward + ((TO_OTHER_LINE,) if j < ALONG_FIRST else ()) + (TO_TWIN,))
                    for way in ways:
                        onward = (way,) if has(way, zc) else ()
                        block, other = self.line_block(zc, far, way)
                        self.arrived(other, CHUNKS - 1)
                        self.spread(other, CHUNKS - 1, zc, onward + (TO_TWIN,))
                    self.across(zc, far - 1)

    def twin_arrived(self, block):
        for j in range(CHUNKS):
            self.arrived(block, j)

    def drain(self):
        def sent(way, pieces):
            rows = pl.ds(0, pieces * self.piece)
            pltpu.make_async_remote_copy(
                src_ref=self.buf.at[rows],
                dst_ref=self.buf.at[rows],
                send_sem=self.send_sem.at[way],
                recv_sem=self.recv_sem.at[0],
                device_id=(self.dp, 0),
                device_id_type=MESH_ID,
            ).wait_send()

        for zc in range(LINE):

            @pl.when(self.z == zc)
            def _(zc=zc):
                if zc < LINE - 1:
                    sent(TO_UPPER, (zc + 1) * (CHUNKS + 1))
                if zc > 0:
                    sent(TO_LOWER, (LINE - zc) * (CHUNKS + 1))

        sent(TO_OTHER_LINE, LINE * ALONG_FIRST + 1)
        sent(TO_TWIN, 2 * LINE * CHUNKS)


class WeightGather:
    def __init__(self, own_ref, full, send_sem, recv_sem, local_sem, where):
        self.own_ref, self.full, self.send_sem, self.recv_sem, self.local_sem = own_ref, full, send_sem, recv_sem, local_sem
        self.dp, self.z, self.y, self.c = where
        self.half = own_ref.shape[0] // 2

    def rows(self, block, half):
        return pl.ds(pl.multiple_of((block * 2 + half) * self.half, 16), self.half)

    def copy(self, src, block, half, way, device, group):
        return pltpu.make_async_remote_copy(
            src_ref=src,
            dst_ref=self.full.at[self.rows(block, half)],
            send_sem=self.send_sem.at[way],
            recv_sem=self.recv_sem.at[block * 2 + half],
            device_id=(group, device),
            device_id_type=MESH_ID,
        )

    def keep(self):
        block = self.z * 4 + self.y * 2 + self.c
        rows = pl.ds(pl.multiple_of(block * 2 * self.half, 16), 2 * self.half)
        return pltpu.make_async_copy(self.own_ref, self.full.at[rows], self.local_sem)

    def own(self, zc, along):
        block = zc * 4 + self.y * 2 + self.c
        mine = self.own_ref.at[pl.ds(pl.multiple_of(self.dp * self.half, 16), self.half)]
        for way in along + (TO_OTHER_LINE,):
            self.copy(mine, block, self.dp, way, target(way, zc, self.y, self.c), self.dp).start()
        for half in range(2):
            src = self.own_ref.at[pl.ds(half * self.half, self.half)]
            self.copy(src, block, half, TO_TWIN, target(TO_TWIN, zc, self.y, self.c), self.dp).start()

    def pass_on(self, block, zc, ways):
        held = self.full.at[self.rows(block, self.dp)]
        self.copy(held, block, self.dp, 0, 0, self.dp).wait_recv()
        for way in ways + (TO_TWIN,):
            self.copy(held, block, self.dp, way, target(way, zc, self.y, self.c), self.dp).start()
        me = zc * 4 + self.y * 2 + self.c
        self.copy(held, block, self.dp, TO_OTHER_GROUP, me, 1 - self.dp).start()

    def swapped(self, place_z, line):
        block, half = place_z * 4 + line * 2 + self.c, 1 - self.dp
        held = self.full.at[self.rows(block, half)]
        self.copy(held, block, half, 0, 0, self.dp).wait_recv()
        self.copy(held, block, half, TO_TWIN, target(TO_TWIN, self.z, self.y, self.c), self.dp).start()

    def swap_early(self):
        for m in range(LINE - 1):
            self.swapped(chip_at(ARRIVAL, self.z, m + 1), self.y)
            self.swapped(chip_at(ARRIVAL, self.z, m), 1 - self.y)

    def finish(self):
        me = self.z * 4 + self.y * 2 + self.c
        self.swapped(chip_at(ARRIVAL, self.z, LINE - 1), 1 - self.y)
        for k in range(8):
            block = (me + 2 * k) % 16 + 1 - 2 * self.c
            for half in range(2):
                self.copy(self.full.at[self.rows(block, half)], block, half, 0, 0, self.dp).wait_recv()

        def sent(way, halves):
            rows = pl.ds(0, halves * self.half)
            pltpu.make_async_remote_copy(
                src_ref=self.full.at[rows], dst_ref=self.full.at[rows], send_sem=self.send_sem.at[way], recv_sem=self.recv_sem.at[0],
                device_id=(self.dp, 0), device_id_type=MESH_ID).wait_send()

        for zc in range(LINE):

            @pl.when(self.z == zc)
            def _(zc=zc):
                if zc < LINE - 1:
                    sent(TO_UPPER, zc + 1)
                if zc > 0:
                    sent(TO_LOWER, LINE - zc)

        sent(TO_OTHER_LINE, LINE)
        sent(TO_TWIN, 16)
        sent(TO_OTHER_GROUP, 7)
        self.keep().wait()


def stage_chips(s):
    return jnp.where(s == 0, 0, 2 * s + 1), jnp.where(s == LINE - 1, 8, 2 * s + 3)


def chip_in_order(n, z, y):
    own = (n < 2) | (n == 3) | (n == 5)
    m = jnp.where(own, (n + 1) // 2, (n - 1) // 2)
    return chip_at(ARRIVAL, z, m), jnp.where(own, y, 1 - y)


def project_body(x_ref, gain_ref, wq_ref, wk_ref, wv_ref, bq_ref, bk_ref, bv_ref, prefix_ref, coarse_cos_ref, coarse_sin_ref, step_cos_hbm, step_sin_hbm, w_o_ref,
                 q_ref, k_ref, v_ref, w_o_full, rows_buf, w_buf, send_sem, recv_sem, w_send, w_recv, local_sem, load_sem, step_cos_ref, step_sin_ref, base_cos_ref, base_sin_ref):
    where = place()
    dp, z, y, c = where
    rows = x_ref.shape[0]
    head_dim = q_ref.shape[1]
    own_tokens = step_cos_ref.shape[0] // 16
    me = z * 4 + y * 2 + c
    loads = [pltpu.make_async_copy(ref, w_buf.at[:, pl.ds(i * head_dim, head_dim)], load_sem.at[i]) for i, ref in enumerate((wq_ref, wk_ref, wv_ref))]
    loads += [pltpu.make_async_copy(step_cos_hbm, step_cos_ref, load_sem.at[3]), pltpu.make_async_copy(step_sin_hbm, step_sin_ref, load_sem.at[4])]
    own = pl.ds(pl.multiple_of(me * rows, 16), rows)
    greet(where)
    weights = WeightGather(w_o_ref, w_o_full, w_send, w_recv, local_sem, where)
    weights.keep().start()
    for load in loads:
        load.start()
    rows_buf[own, :] = scaled_norm(x_ref[...].astype(jnp.float32), gain_ref[...].astype(jnp.float32))
    meet(where)
    gather = RowGather(rows_buf, send_sem, recv_sem, where, weights)
    gather.start()
    for load in loads:
        load.wait()
    for r in range(base_cos_ref.shape[0]):
        first = prefix_ref[r]
        high, low = pl.ds(first // step_cos_ref.shape[0], 1), pl.ds(first % step_cos_ref.shape[0], 1)
        coarse_cos, coarse_sin, fine_cos, fine_sin = coarse_cos_ref[high, :], coarse_sin_ref[high, :], step_cos_ref[low, :], step_sin_ref[low, :]
        base_cos_ref[r:r + 1, :] = coarse_cos * fine_cos - coarse_sin * fine_sin
        base_sin_ref[r:r + 1, :] = coarse_sin * fine_cos + coarse_cos * fine_sin

    def compute(block):
        at = pl.ds(pl.multiple_of(block * rows, 16), rows)
        out = jnp.dot(rows_buf[at, :], w_buf[...], preferred_element_type=jnp.float32)
        bias = jnp.concatenate([ref[...].astype(jnp.float32) for ref in (bq_ref, bk_ref, bv_ref)], axis=1)
        out = (out + bias).astype(jnp.bfloat16)
        steps = pl.ds(pl.multiple_of(block * own_tokens, 8), own_tokens)
        step_cos, step_sin = step_cos_ref[steps, :][None], step_sin_ref[steps, :][None]
        base_cos, base_sin = base_cos_ref[...][:, None, :], base_sin_ref[...][:, None, :]
        cos_t = (base_cos * step_cos - base_sin * step_sin).reshape(rows, head_dim)
        sin_t = (base_sin * step_cos + base_cos * step_sin).reshape(rows, head_dim)
        lane = lax.broadcasted_iota(jnp.int32, (rows, head_dim), 1)
        sin_t = jnp.where(lane < head_dim // 2, -sin_t, sin_t)
        for ref, i in ((q_ref, 0), (k_ref, 1)):
            wide = out[:, i * head_dim:(i + 1) * head_dim].astype(jnp.float32)
            ref[at, :] = (wide * cos_t + pltpu.roll(wide, head_dim // 2, 1) * sin_t).astype(jnp.bfloat16)
        v_ref[at, :] = out[:, 2 * head_dim:]

    @pl.loop(0, LINE)
    def _(s):
        gather.step(s)
        pl.when(s == LINE - 1)(weights.swap_early)

        @pl.loop(*stage_chips(s))
        def _(n):
            at, line = chip_in_order(n, z, y)
            compute(at * 4 + line * 2 + c)
            twin = at * 4 + line * 2 + 1 - c
            gather.twin_arrived(twin)
            compute(twin)

    weights.finish()
    gather.drain()


def inverse_frequencies(head_dim):
    half = ROPE_THETA ** (-2.0 * np.arange(head_dim // 2) / head_dim)
    return np.concatenate([half, half])[None, :]


def project_all(x_rows, gain, w_q, w_k, w_v, biases, w_o, prefix, k_slots):
    n_req, own_tokens, width = x_rows.shape
    rows = n_req * own_tokens
    head_dim = w_q.shape[1]
    inv_freq = inverse_frequencies(head_dim)
    n_tokens = 16 * own_tokens
    step = np.arange(n_tokens)[:, None] * inv_freq
    coarse = np.arange(-(-k_slots // n_tokens))[:, None] * n_tokens * inv_freq
    step_cos, step_sin, coarse_cos, coarse_sin = (np.asarray(t, np.float32) for t in (np.cos(step), np.sin(step), np.cos(coarse), np.sin(coarse)))
    vmem = pl.BlockSpec(memory_space=pltpu.VMEM)
    hbm = pl.BlockSpec(memory_space=pltpu.HBM)
    out = jax.ShapeDtypeStruct((16 * rows, head_dim), jnp.bfloat16)
    dma = pltpu.SemaphoreType.DMA
    *outs, w_o_full = pl.pallas_call(
        project_body,
        out_shape=(out, out, out, jax.ShapeDtypeStruct((16 * w_o.shape[0], w_o.shape[1]), jnp.bfloat16)),
        in_specs=[vmem] * 2 + [hbm] * 3 + [vmem] * 3 + [pl.BlockSpec(memory_space=pltpu.SMEM)] + [vmem] * 2 + [hbm] * 2 + [vmem],
        out_specs=(vmem,) * 3 + (hbm,),
        scratch_shapes=[
            pltpu.VMEM((16 * rows, width), jnp.bfloat16),
            pltpu.VMEM((width, 3 * head_dim), jnp.bfloat16),
            dma((4,)), dma((16 * CHUNKS,)), dma((5,)), dma((32,)), dma, dma((5,)),
            pltpu.VMEM(step_cos.shape, jnp.float32), pltpu.VMEM(step_sin.shape, jnp.float32),
            pltpu.VMEM((n_req, head_dim), jnp.float32), pltpu.VMEM((n_req, head_dim), jnp.float32),
        ],
        compiler_params=pltpu.CompilerParams(collective_id=0, has_side_effects=True, vmem_limit_bytes=62 * 2**20),
        cost_estimate=pl.CostEstimate(flops=2 * 16 * rows * width * 3 * head_dim, bytes_accessed=4 * rows * width, transcendentals=0),
        name="project",
    )(x_rows.reshape(rows, width), gain.reshape(1, width), w_q, w_k, w_v, *biases, prefix, coarse_cos, coarse_sin, step_cos, step_sin, w_o)
    return tuple(o.reshape(16, n_req, own_tokens, head_dim) for o in outs), w_o_full


def token_rows(ref):
    rows = ref[:, 0].astype(jnp.float32)
    return rows.reshape(rows.shape[0] * rows.shape[1], rows.shape[2])


def attention_body(prefix_ref, valid_ref, q_ref, kn_ref, vn_ref, k_ref, v_ref, o_ref, ko_ref, vo_ref, scores, top, total, acc, staged, take_sem, put_sem):
    req = pl.program_id(0)
    start = prefix_ref[req]
    count = valid_ref[req]
    head_dim = q_ref.shape[3]
    n_tokens = q_ref.shape[0] * q_ref.shape[2]
    slots = k_ref.shape[1]
    last = pl.num_programs(0) - 1

    def take(r):
        return [pltpu.make_async_copy(ref.at[r], staged.at[r * 2 + i], take_sem.at[r * 2 + i]) for i, ref in enumerate((k_ref, v_ref))]

    def put(r):
        return [pltpu.make_async_copy(staged.at[r * 2 + i], ref.at[r], put_sem.at[r * 2 + i]) for i, ref in enumerate((ko_ref, vo_ref))]

    @pl.when(req == 0)
    def _():
        for move in take(0) + take(1):
            move.start()

    @pl.when(req + 2 <= last)
    def _():
        for move in take(req + 2):
            move.start()

    for move in take(req):
        move.wait()
    base = pl.multiple_of(jnp.minimum((start // 16) * 16, slots - UPDATE_ROWS), 16)
    shift = start - base
    row = lax.broadcasted_iota(jnp.int32, (UPDATE_ROWS, head_dim), 0) - shift
    keep = (row >= 0) & (row < count)
    for i, src in enumerate((kn_ref, vn_ref)):
        fresh = jnp.concatenate([token_rows(src), jnp.zeros((UPDATE_ROWS - n_tokens, head_dim), jnp.float32)], axis=0)
        fresh = pltpu.roll(fresh, shift, 0)
        old = staged[req * 2 + i, pl.ds(base, UPDATE_ROWS), :].astype(jnp.float32)
        staged[req * 2 + i, pl.ds(base, UPDATE_ROWS), :] = jnp.where(keep, fresh, old).astype(jnp.bfloat16)

    for move in put(req):
        move.start()
    n_open = (start + 1) // KV_BLOCK
    n_used = pl.cdiv(start + count, KV_BLOCK)
    queries = token_rows(q_ref).astype(jnp.bfloat16)
    lanes = KV_BLOCK // 128
    top[...] = jnp.full_like(top, -1.0e30)

    def score(blk, masked):
        keys = staged[req * 2, pl.ds(pl.multiple_of(blk * KV_BLOCK, KV_BLOCK), KV_BLOCK), :]
        s = lax.dot_general(queries, keys, (((1,), (1,)), ((), ())), preferred_element_type=jnp.float32)
        if masked:
            col = lax.broadcasted_iota(jnp.int32, (n_tokens, KV_BLOCK), 1) + blk * KV_BLOCK
            row_id = lax.broadcasted_iota(jnp.int32, (n_tokens, KV_BLOCK), 0)
            s = jnp.where(col <= start + jnp.minimum(row_id, count - 1), s, -1.0e30)
        scores[blk] = s
        best = top[...]
        for j in range(lanes):
            best = jnp.maximum(best, s[:, j * 128:(j + 1) * 128])
        top[...] = best

    pl.loop(0, n_open)(lambda blk: score(blk, False))
    pl.loop(n_open, n_used)(lambda blk: score(blk, True))
    top[...] = jnp.broadcast_to(jnp.max(top[...], axis=1, keepdims=True), top.shape)
    total[...] = jnp.zeros_like(total)
    acc[...] = jnp.zeros_like(acc)

    @pl.loop(0, n_used)
    def _(blk):
        best = top[...]
        part = total[...]
        pieces = []
        for j in range(lanes):
            e = jnp.exp2((scores[blk, :, j * 128:(j + 1) * 128] - best) * (LOG2_E * head_dim ** -0.5))
            part = part + e
            pieces.append(e.astype(jnp.bfloat16))
        total[...] = part
        vals = staged[req * 2 + 1, pl.ds(pl.multiple_of(blk * KV_BLOCK, KV_BLOCK), KV_BLOCK), :]
        acc[...] += jnp.dot(jnp.concatenate(pieces, axis=1), vals, preferred_element_type=jnp.float32)

    mixed = acc[...] / jnp.sum(total[...], axis=1, keepdims=True)
    o_ref[:, 0] = mixed.reshape(o_ref.shape[0], o_ref.shape[2], head_dim).astype(jnp.bfloat16)

    @pl.when(req == last)
    def _():
        for r in range(k_ref.shape[0]):
            for move in put(r):
                move.wait()


def attend(queries, keys_new, values_new, k_cache, v_cache, prefix, valid):
    owners, n_req, own_tokens, head_dim = queries.shape
    n_tokens = owners * own_tokens
    slots = k_cache.shape[1]
    new_spec = pl.BlockSpec((owners, 1, own_tokens, head_dim), lambda r, *_: (0, r, 0, 0))
    cache_spec = pl.BlockSpec(memory_space=pltpu.HBM)
    cache_out = jax.ShapeDtypeStruct(k_cache.shape, jnp.bfloat16)
    return pl.pallas_call(
        attention_body,
        out_shape=(jax.ShapeDtypeStruct(queries.shape, jnp.bfloat16), cache_out, cache_out),
        grid_spec=pltpu.PrefetchScalarGridSpec(
            num_scalar_prefetch=2,
            grid=(n_req,),
            in_specs=[new_spec, new_spec, new_spec, cache_spec, cache_spec],
            out_specs=(new_spec, cache_spec, cache_spec),
            scratch_shapes=[
                pltpu.VMEM((slots // KV_BLOCK, n_tokens, KV_BLOCK), jnp.float32),
                pltpu.VMEM((n_tokens, 128), jnp.float32),
                pltpu.VMEM((n_tokens, 128), jnp.float32),
                pltpu.VMEM((n_tokens, head_dim), jnp.float32),
                pltpu.VMEM((2 * n_req, slots, head_dim), jnp.bfloat16),
                pltpu.SemaphoreType.DMA((2 * n_req,)),
                pltpu.SemaphoreType.DMA((2 * n_req,)),
            ],
        ),
        compiler_params=pltpu.CompilerParams(dimension_semantics=("arbitrary",), vmem_limit_bytes=62 * 2**20),
        cost_estimate=pl.CostEstimate(flops=2 * 2 * n_req * n_tokens * slots * head_dim, bytes_accessed=8 * n_req * slots * head_dim, transcendentals=n_req * n_tokens * slots),
        name="attend",
    )(prefix, valid, queries, keys_new, values_new, k_cache, v_cache)


REDUCE = ((2, 3, 1, 0), (2, 3, 0, 1), (1, 0, 3, 2), (1, 0, 2, 3))


def finish_body(o_ref, x_ref, gain_ref, w_gate_hbm, w_up_hbm, w_down_hbm, w_o_ref, out_ref,
                rows_buf, part, swapped, attended, resid, acc, from_twin, from_line, from_lower, from_upper,
                gather_send, gather_recv, reduce_send, twin_recv, line_recv, lower_recv, upper_recv, swap_send, swap_recv, local_sem, w_gate_ref, w_up_ref, w_down_ref):
    where = place()
    dp, z, y, c = where
    rows, width = x_ref.shape
    head_dim = o_ref.shape[1]
    me = z * 4 + y * 2 + c
    piece = rows // CHUNKS
    load = pltpu.make_async_copy(w_o_ref, part.at[pl.ds(0, w_o_ref.shape[0])], local_sem.at[0])
    load.start()
    pairs = ((w_gate_hbm, w_gate_ref), (w_up_hbm, w_up_ref), (w_down_hbm, w_down_ref))
    mlp_loads = [pltpu.make_async_copy(src, dst, local_sem.at[1 + i]) for i, (src, dst) in enumerate(pairs)]
    for mlp_load in mlp_loads:
        mlp_load.start()
    barrier = pltpu.get_barrier_semaphore()
    for k in range(1, 16):
        pl.semaphore_signal(barrier, 1, device_id=(dp, (me + k) % 16), device_id_type=MESH_ID)
    pl.semaphore_wait(barrier, 15)

    def block_rows(block):
        return pl.ds(pl.multiple_of(block * rows, 16), rows)

    for k in range(1, 16):
        other = (me + k) % 16
        pltpu.make_async_remote_copy(
            src_ref=o_ref.at[block_rows(other)], dst_ref=swapped.at[block_rows(me)], send_sem=swap_send, recv_sem=swap_recv,
            device_id=(dp, other), device_id_type=MESH_ID).start()
    swapped[block_rows(me), :] = o_ref[block_rows(me), :]
    load.wait()
    others = o_ref.at[pl.ds(0, 15 * rows)]
    swap = pltpu.make_async_remote_copy(src_ref=others, dst_ref=others, send_sem=swap_send, recv_sem=swap_recv, device_id=(dp, 0), device_id_type=MESH_ID)
    swap.wait_recv()
    swap.wait_send()
    for head in range(16):
        attended[:, head * head_dim:(head + 1) * head_dim] = swapped[head * rows:(head + 1) * rows, :]

    @pl.loop(0, width // 512)
    def _(n):
        cols = pl.ds(pl.multiple_of(n * 512, 512), 512)
        out = jnp.dot(attended[...], part[pl.ds(0, w_o_ref.shape[0]), cols], preferred_element_type=jnp.float32).astype(jnp.bfloat16)
        resid[:, cols] = (x_ref[:, cols].astype(jnp.float32) + out.astype(jnp.float32)).astype(jnp.bfloat16)

    rows_buf[block_rows(me), :] = scaled_norm(resid[...].astype(jnp.float32), gain_ref[...].astype(jnp.float32))
    gather = RowGather(rows_buf, gather_send, gather_recv, where)
    gather.start()
    for mlp_load in mlp_loads:
        mlp_load.wait()

    def partial_sums(block):
        hidden = rows_buf[block_rows(block), :]
        dims = (((1,), (1,)), ((), ()))
        gate = lax.dot_general(hidden, w_gate_ref[...], dims, preferred_element_type=jnp.float32)
        up = lax.dot_general(hidden, w_up_ref[...], dims, preferred_element_type=jnp.float32)
        act = (jax.nn.silu(gate) * up).astype(jnp.bfloat16)
        part[block_rows(block), :] = jnp.dot(act, w_down_ref[...], preferred_element_type=jnp.float32).astype(jnp.bfloat16)

    def twin_copy(block, slot):
        return pltpu.make_async_remote_copy(
            src_ref=part.at[block_rows(block)], dst_ref=from_twin.at[block_rows(slot)], send_sem=reduce_send.at[TO_TWIN], recv_sem=twin_recv.at[slot],
            device_id=(dp, z * 4 + y * 2 + 1 - c), device_id_type=MESH_ID)

    last = CHUNKS - 1

    def piece_rows(block, j):
        return pl.ds(pl.multiple_of(block * rows + j * piece, 16), piece)

    def line_copy(dest, j):
        return pltpu.make_async_remote_copy(
            src_ref=part.at[piece_rows(dest * 4 + (1 - y) * 2 + c, j)], dst_ref=from_line.at[piece_rows(dest, j)],
            send_sem=reduce_send.at[TO_OTHER_LINE], recv_sem=line_recv.at[dest * CHUNKS + j],
            device_id=(dp, target(TO_OTHER_LINE, z, y, c)), device_id_type=MESH_ID)

    def slot(dest, line, j):
        far = jnp.where(line == y, dest * CHUNKS + j, LINE * CHUNKS + dest)
        return far, pl.ds(pl.multiple_of(far * piece, 16), piece)

    def along_copy(dest, line, j, way):
        index, land = slot(dest, line, j)
        buf, sems = (from_lower, lower_recv) if way == TO_UPPER else (from_upper, upper_recv)
        return pltpu.make_async_remote_copy(
            src_ref=part.at[piece_rows(dest * 4 + line * 2 + c, j)], dst_ref=buf.at[land],
            send_sem=reduce_send.at[way], recv_sem=sems.at[index], device_id=(dp, target(way, z, y, c)), device_id_type=MESH_ID)

    def line_send(dest):
        for j in range(ALONG_FIRST):
            line_copy(dest, j).start()

    def chips(lo, hi):
        @pl.loop(lo, hi)
        def _(n):
            at, line = chip_in_order(n, z, y)
            block = at * 4 + line * 2 + c
            twin = at * 4 + line * 2 + 1 - c
            gather.twin_arrived(twin)
            partial_sums(twin)
            twin_copy(twin, at * 2 + line).start()
            partial_sums(block)
            twin_copy(block, at * 2 + line).wait_recv()
            total = part[block_rows(block), :].astype(jnp.float32) + from_twin[block_rows(at * 2 + line), :].astype(jnp.float32)
            part[block_rows(block), :] = total.astype(jnp.bfloat16)

    def add_along(dest, line, j):
        _, land = slot(dest, line, j)

        @pl.when((dest >= z) & (z > 0))
        def _():
            along_copy(dest, line, j, TO_UPPER).wait_recv()
            acc[...] += from_lower[land, :].astype(jnp.float32)

        @pl.when((dest <= z) & (z < LINE - 1))
        def _():
            along_copy(dest, line, j, TO_LOWER).wait_recv()
            acc[...] += from_upper[land, :].astype(jnp.float32)

        @pl.when((dest != z) | (j == last))
        def _():
            part[piece_rows(dest * 4 + line * 2 + c, j), :] = acc[...].astype(jnp.bfloat16)

        pl.when(dest > z)(lambda: along_copy(dest, line, j, TO_UPPER).start())
        pl.when(dest < z)(lambda: along_copy(dest, line, j, TO_LOWER).start())

    def result(j):
        out = pl.ds(pl.multiple_of(j * piece, 16), piece)
        down = acc[...].astype(jnp.bfloat16).astype(jnp.float32)
        out_ref[out, :] = (resid[out, :].astype(jnp.float32) + down).astype(jnp.bfloat16)

    at_end = (z == 0) | (z == LINE - 1)

    def last_piece(step):
        dest = chip_at(REDUCE, z, step // 2)
        line = (y + 1 + step) % 2
        acc[...] = part[piece_rows(dest * 4 + line * 2 + c, last), :].astype(jnp.float32)
        add_along(dest, line, last)
        pl.when((dest == z) & (line != y))(lambda: line_copy(dest, last).start())

    def before_last():
        line_send(chip_at(REDUCE, z, 0))

        @pl.when(at_end)
        def _():
            last_piece(0)
            last_piece(1)
            last_piece(3)

    @pl.loop(0, LINE)
    def _(s):
        pl.when(s == LINE - 1)(before_last)
        gather.step(s)
        chips(*stage_chips(s))

    for i in range(1, LINE):
        line_send(chip_at(REDUCE, z, i))

    @pl.loop(0, 2 * LINE - 2)
    def _(step):
        pl.when(jnp.logical_not(at_end) | (step == 2) | (step >= 4))(lambda: last_piece(step))

    @pl.loop(0, LINE * ALONG_FIRST + 2)
    def _(n):
        swing = (LINE - 1) * ALONG_FIRST

        @pl.when((n >= swing) & (n < swing + 2))
        def _():
            last_piece(2 * LINE - 2 + n - swing)

        @pl.when((n < swing) | (n >= swing + 2))
        def _():
            step = jnp.where(n < swing, n, n - 2)
            dest = chip_at(REDUCE, z, step // ALONG_FIRST)
            j = step % ALONG_FIRST
            line_copy(dest, j).wait_recv()
            acc[...] = part[piece_rows(dest * 4 + y * 2 + c, j), :].astype(jnp.float32) + from_line[piece_rows(dest, j), :].astype(jnp.float32)
            add_along(dest, y, j)
            pl.when(dest == z)(lambda: result(j))

    line_copy(z, last).wait_recv()
    acc[...] = part[piece_rows(me, last), :].astype(jnp.float32) + from_line[piece_rows(z, last), :].astype(jnp.float32)
    result(last)
    gather.drain()

    def sent(way, pieces):
        span = pl.ds(0, pieces * piece)
        pltpu.make_async_remote_copy(
            src_ref=part.at[span], dst_ref=part.at[span], send_sem=reduce_send.at[way], recv_sem=twin_recv.at[0],
            device_id=(dp, 0), device_id_type=MESH_ID).wait_send()

    for zc in range(LINE):

        @pl.when(z == zc)
        def _(zc=zc):
            if zc < LINE - 1:
                sent(TO_UPPER, (LINE - 1 - zc) * (CHUNKS + 1))
            if zc > 0:
                sent(TO_LOWER, zc * (CHUNKS + 1))

    sent(TO_OTHER_LINE, LINE * ALONG_FIRST + 1)
    sent(TO_TWIN, 2 * LINE * CHUNKS)


def finish(attended, x_rows, gain, w_gate, w_up, w_down, w_o):
    n_req, own_tokens, width = x_rows.shape
    rows = n_req * own_tokens
    head_dim = attended.shape[-1]
    vmem = pl.BlockSpec(memory_space=pltpu.VMEM)
    bf16, f32 = jnp.bfloat16, jnp.float32
    dma = pltpu.SemaphoreType.DMA
    out = pl.pallas_call(
        finish_body,
        out_shape=jax.ShapeDtypeStruct((rows, width), bf16),
        in_specs=[vmem] * 3 + [pl.BlockSpec(memory_space=pltpu.HBM)] * 4,
        out_specs=vmem,
        scratch_shapes=[
            pltpu.VMEM((16 * rows, width), bf16),
            pltpu.VMEM((16 * rows, width), bf16),
            pltpu.VMEM((16 * rows, head_dim), bf16),
            pltpu.VMEM((rows, width), bf16),
            pltpu.VMEM((rows, width), bf16),
            pltpu.VMEM((rows // CHUNKS, width), f32),
            pltpu.VMEM((8 * rows, width), bf16),
            pltpu.VMEM((LINE * rows, width), bf16),
            pltpu.VMEM((LINE * (rows + rows // CHUNKS), width), bf16),
            pltpu.VMEM((LINE * (rows + rows // CHUNKS), width), bf16),
            dma((4,)), dma((16 * CHUNKS,)), dma((4,)), dma((8,)), dma((LINE * CHUNKS,)), dma((LINE * (CHUNKS + 1),)), dma((LINE * (CHUNKS + 1),)), dma, dma, dma((4,)),
            pltpu.VMEM(w_gate.T.shape, bf16), pltpu.VMEM(w_up.T.shape, bf16), pltpu.VMEM(w_down.shape, bf16),
        ],
        compiler_params=pltpu.CompilerParams(collective_id=1, has_side_effects=True, vmem_limit_bytes=62 * 2**20),
        cost_estimate=pl.CostEstimate(flops=2 * rows * width * (width + 16 * 3 * w_down.shape[0]), bytes_accessed=4 * width * width, transcendentals=0),
        name="finish",
    )(attended.reshape(16 * rows, head_dim), x_rows.reshape(rows, width), gain[None, :], w_gate.T, w_up.T, w_down, w_o)
    return out.reshape(x_rows.shape)


def solution(mesh):
    row_spec = P("dp", "tp", None)
    cache_spec = P("dp", None, "tp", None)
    req_spec = P("dp")
    rep_spec = P(None)
    col_spec = P(None, "tp")
    bias_spec = P("tp")
    down_spec = P("tp", None)

    def layer(x_rows, k_cache, v_cache, prefix, valid, g_attn, w_q, b_q, w_k, b_k, w_v, b_v, w_o, g_mlp, w_gate, w_up, w_down):
        biases = [b.reshape(1, -1) for b in (b_q, b_k, b_v)]
        (queries, keys_new, values_new), w_o_full = project_all(x_rows, g_attn, w_q, w_k, w_v, biases, w_o, prefix, k_cache.shape[1])
        flat = (k_cache.shape[0], k_cache.shape[1], k_cache.shape[3])
        attended, k_out, v_out = attend(queries, keys_new, values_new, k_cache.reshape(flat), v_cache.reshape(flat), prefix, valid)
        x_out = finish(attended, x_rows, g_mlp, w_gate, w_up, w_down, w_o_full)
        return x_out, k_out.reshape(k_cache.shape), v_out.reshape(v_cache.shape)

    in_specs = (row_spec, cache_spec, cache_spec, req_spec, req_spec, rep_spec, col_spec, bias_spec, col_spec, bias_spec, col_spec, bias_spec, down_spec, rep_spec, col_spec, col_spec, down_spec)
    return jax.shard_map(layer, mesh=mesh, in_specs=in_specs, out_specs=(row_spec, cache_spec, cache_spec), check_vma=False)
```

```python
import functools
import jax
import jax.numpy as jnp
import numpy as np
from jax import lax
from jax.experimental import pallas as pl
from jax.experimental.pallas import tpu as pltpu
from jax.sharding import PartitionSpec as P

ROPE_THETA = 1.0e6
NORM_EPS = 1.0e-6
KV_BLOCK = 1024
UPDATE_ROWS = 400
LOG2_E = 1.4426950408889634


MESH_ID = pl.DeviceIdType.MESH
LINE = 4
CHUNKS = 6
ALONG_FIRST = CHUNKS - 1
TO_UPPER, TO_LOWER, TO_OTHER_LINE, TO_TWIN, TO_OTHER_GROUP = range(5)
ARRIVAL = ((0, 1, 2, 3), (1, 0, 2, 3), (2, 1, 3, 0), (3, 2, 1, 0))


def scaled_norm(wide_vals, gain):
    inv_rms = lax.rsqrt(jnp.mean(wide_vals * wide_vals, axis=-1, keepdims=True) + NORM_EPS)
    return (wide_vals * inv_rms * gain).astype(jnp.bfloat16)


def flat_gain(ref):
    wide = ref[...].astype(jnp.float32)
    return jnp.concatenate([wide[i:i + 1, :] for i in range(wide.shape[0])], axis=1)


def place():
    me = lax.axis_index("tp")
    return lax.axis_index("dp"), me // 4, (me // 2) % 2, me % 2


def chip_at(table, z, m):
    packed = [sum(v << (2 * i) for i, v in enumerate(row)) for row in table]
    code = jnp.where(z == 0, packed[0], jnp.where(z == 1, packed[1], jnp.where(z == 2, packed[2], packed[3])))
    return (code >> (2 * m)) & 3


def has(way, zc):
    return zc < LINE - 1 if way == TO_UPPER else zc > 0


def target(way, zc, y, c):
    return {TO_UPPER: (zc + 1) * 4 + y * 2 + c, TO_LOWER: (zc - 1) * 4 + y * 2 + c, TO_OTHER_LINE: zc * 4 + (1 - y) * 2 + c, TO_TWIN: zc * 4 + y * 2 + 1 - c}[way]


def greet(where):
    dp, z, y, c = where
    barrier = pltpu.get_barrier_semaphore()
    pl.when(z > 0)(lambda: pl.semaphore_signal(barrier, 1, device_id=(dp, target(TO_LOWER, z, y, c)), device_id_type=MESH_ID))
    pl.when(z < LINE - 1)(lambda: pl.semaphore_signal(barrier, 1, device_id=(dp, target(TO_UPPER, z, y, c)), device_id_type=MESH_ID))
    for way in (TO_OTHER_LINE, TO_TWIN):
        pl.semaphore_signal(barrier, 1, device_id=(dp, target(way, z, y, c)), device_id_type=MESH_ID)
    pl.semaphore_signal(barrier, 1, device_id=(1 - dp, z * 4 + y * 2 + c), device_id_type=MESH_ID)


def meet(where):
    dp, z, y, c = where
    pl.semaphore_wait(pltpu.get_barrier_semaphore(), 3 + (z + 3) // 4 + (6 - z) // 4)


class RowGather:
    def __init__(self, buf, send_sem, recv_sem, where, weights=None):
        self.buf, self.send_sem, self.recv_sem, self.weights = buf, send_sem, recv_sem, weights
        self.dp, self.z, self.y, self.c = where
        self.rows = buf.shape[0] // 16
        self.piece = self.rows // CHUNKS

    def copy(self, block, j, way, device):
        rows = pl.ds(pl.multiple_of(block * self.rows + j * self.piece, 16), self.piece)
        return pltpu.make_async_remote_copy(
            src_ref=self.buf.at[rows],
            dst_ref=self.buf.at[rows],
            send_sem=self.send_sem.at[way],
            recv_sem=self.recv_sem.at[block * CHUNKS + j],
            device_id=(self.dp, device),
            device_id_type=MESH_ID,
        )

    def arrived(self, block, j):
        self.copy(block, j, 0, 0).wait_recv()

    def spread(self, block, j, zc, ways):
        for way in ways:
            self.copy(block, j, way, target(way, zc, self.y, self.c)).start()

    def line_block(self, zc, far, way_in):
        at = zc - far if way_in == TO_UPPER else zc + far
        return at * 4 + self.y * 2 + self.c, at * 4 + (1 - self.y) * 2 + self.c

    def start(self):
        for zc in range(LINE):

            @pl.when(self.z == zc)
            def _(zc=zc):
                own, other = self.line_block(zc, 0, TO_UPPER)
                along = tuple(way for way in (TO_UPPER, TO_LOWER) if has(way, zc))
                if self.weights is not None:
                    self.weights.own(zc, along)
                self.spread(own, CHUNKS - 1, zc, (TO_OTHER_LINE,) + along + (TO_TWIN,))
                for j in range(ALONG_FIRST):
                    self.spread(own, j, zc, along + (TO_OTHER_LINE, TO_TWIN))
                self.arrived(other, CHUNKS - 1)
                self.spread(other, CHUNKS - 1, zc, along + (TO_TWIN,))

    def across(self, zc, m):
        block = ARRIVAL[zc][m] * 4 + (1 - self.y) * 2 + self.c
        if self.weights is not None:
            self.weights.pass_on(block, zc, ())
        for j in range(ALONG_FIRST):
            self.arrived(block, j)
            self.spread(block, j, zc, (TO_TWIN,))

    def step(self, s):
        for far in range(1, LINE + 1):
            for zc in range(LINE):

                @pl.when((self.z == zc) & (s == far - 1))
                def _(zc=zc, far=far):
                    ways = [way for way in (TO_UPPER, TO_LOWER) if 0 <= (zc - far if way == TO_UPPER else zc + far) < LINE]
                    if self.weights is not None:
                        for way in ways:
                            self.weights.pass_on(self.line_block(zc, far, way)[0], zc, ((way,) if has(way, zc) else ()) + (TO_OTHER_LINE,))
                    for j in (CHUNKS - 1,) + tuple(range(ALONG_FIRST)):
                        for way in ways:
                            block = self.line_block(zc, far, way)[0]
                            onward = (way,) if has(way, zc) else ()
                            self.arrived(block, j)
                            self.spread(block, j, zc, onward + ((TO_OTHER_LINE,) if j < ALONG_FIRST else ()) + (TO_TWIN,))
                    for way in ways:
                        onward = (way,) if has(way, zc) else ()
                        block, other = self.line_block(zc, far, way)
                        self.arrived(other, CHUNKS - 1)
                        self.spread(other, CHUNKS - 1, zc, onward + (TO_TWIN,))
                    self.across(zc, far - 1)

    def twin_arrived(self, block):
        for j in range(CHUNKS):
            self.arrived(block, j)

    def drain(self):
        def sent(way, pieces):
            rows = pl.ds(0, pieces * self.piece)
            pltpu.make_async_remote_copy(
                src_ref=self.buf.at[rows],
                dst_ref=self.buf.at[rows],
                send_sem=self.send_sem.at[way],
                recv_sem=self.recv_sem.at[0],
                device_id=(self.dp, 0),
                device_id_type=MESH_ID,
            ).wait_send()

        for zc in range(LINE):

            @pl.when(self.z == zc)
            def _(zc=zc):
                if zc < LINE - 1:
                    sent(TO_UPPER, (zc + 1) * (CHUNKS + 1))
                if zc > 0:
                    sent(TO_LOWER, (LINE - zc) * (CHUNKS + 1))

        sent(TO_OTHER_LINE, LINE * ALONG_FIRST + 1)
        sent(TO_TWIN, 2 * LINE * CHUNKS)


class WeightGather:
    def __init__(self, own_ref, full, send_sem, recv_sem, local_sem, where):
        self.own_ref, self.full, self.send_sem, self.recv_sem, self.local_sem = own_ref, full, send_sem, recv_sem, local_sem
        self.dp, self.z, self.y, self.c = where
        self.half = own_ref.shape[0] // 2

    def rows(self, block, half):
        return pl.ds(pl.multiple_of((block * 2 + half) * self.half, 16), self.half)

    def copy(self, src, block, half, way, device, group):
        return pltpu.make_async_remote_copy(
            src_ref=src,
            dst_ref=self.full.at[self.rows(block, half)],
            send_sem=self.send_sem.at[way],
            recv_sem=self.recv_sem.at[block * 2 + half],
            device_id=(group, device),
            device_id_type=MESH_ID,
        )

    def keep(self):
        block = self.z * 4 + self.y * 2 + self.c
        rows = pl.ds(pl.multiple_of(block * 2 * self.half, 16), 2 * self.half)
        return pltpu.make_async_copy(self.own_ref, self.full.at[rows], self.local_sem)

    def own(self, zc, along):
        block = zc * 4 + self.y * 2 + self.c
        mine = self.own_ref.at[pl.ds(pl.multiple_of(self.dp * self.half, 16), self.half)]
        for way in along + (TO_OTHER_LINE,):
            self.copy(mine, block, self.dp, way, target(way, zc, self.y, self.c), self.dp).start()
        for half in range(2):
            src = self.own_ref.at[pl.ds(half * self.half, self.half)]
            self.copy(src, block, half, TO_TWIN, target(TO_TWIN, zc, self.y, self.c), self.dp).start()

    def pass_on(self, block, zc, ways):
        held = self.full.at[self.rows(block, self.dp)]
        self.copy(held, block, self.dp, 0, 0, self.dp).wait_recv()
        for way in ways + (TO_TWIN,):
            self.copy(held, block, self.dp, way, target(way, zc, self.y, self.c), self.dp).start()
        me = zc * 4 + self.y * 2 + self.c
        self.copy(held, block, self.dp, TO_OTHER_GROUP, me, 1 - self.dp).start()

    def swapped(self, place_z, line):
        block, half = place_z * 4 + line * 2 + self.c, 1 - self.dp
        held = self.full.at[self.rows(block, half)]
        self.copy(held, block, half, 0, 0, self.dp).wait_recv()
        self.copy(held, block, half, TO_TWIN, target(TO_TWIN, self.z, self.y, self.c), self.dp).start()

    def swap_early(self):
        for m in range(LINE - 1):
            self.swapped(chip_at(ARRIVAL, self.z, m + 1), self.y)
            self.swapped(chip_at(ARRIVAL, self.z, m), 1 - self.y)

    def finish(self):
        me = self.z * 4 + self.y * 2 + self.c
        self.swapped(chip_at(ARRIVAL, self.z, LINE - 1), 1 - self.y)
        for k in range(8):
            block = (me + 2 * k) % 16 + 1 - 2 * self.c
            for half in range(2):
                self.copy(self.full.at[self.rows(block, half)], block, half, 0, 0, self.dp).wait_recv()

        def sent(way, halves):
            rows = pl.ds(0, halves * self.half)
            pltpu.make_async_remote_copy(
                src_ref=self.full.at[rows], dst_ref=self.full.at[rows], send_sem=self.send_sem.at[way], recv_sem=self.recv_sem.at[0],
                device_id=(self.dp, 0), device_id_type=MESH_ID).wait_send()

        for zc in range(LINE):

            @pl.when(self.z == zc)
            def _(zc=zc):
                if zc < LINE - 1:
                    sent(TO_UPPER, zc + 1)
                if zc > 0:
                    sent(TO_LOWER, LINE - zc)

        sent(TO_OTHER_LINE, LINE)
        sent(TO_TWIN, 16)
        sent(TO_OTHER_GROUP, 7)
        self.keep().wait()


def stage_chips(s):
    return jnp.where(s == 0, 0, 2 * s + 1), jnp.where(s == LINE - 1, 8, 2 * s + 3)


def chip_in_order(n, z, y):
    own = (n < 2) | (n == 3) | (n == 5)
    m = jnp.where(own, (n + 1) // 2, (n - 1) // 2)
    return chip_at(ARRIVAL, z, m), jnp.where(own, y, 1 - y)


def project_body(x_ref, gain_ref, wq_ref, wk_ref, wv_ref, bq_ref, bk_ref, bv_ref, prefix_ref, coarse_cos_ref, coarse_sin_ref, step_cos_hbm, step_sin_hbm, w_o_ref,
                 q_ref, k_ref, v_ref, w_o_full, rows_buf, w_buf, send_sem, recv_sem, w_send, w_recv, local_sem, load_sem, step_cos_ref, step_sin_ref, base_cos_ref, base_sin_ref):
    where = place()
    dp, z, y, c = where
    rows = x_ref.shape[0]
    head_dim = q_ref.shape[1]
    own_tokens = step_cos_ref.shape[0] // 16
    me = z * 4 + y * 2 + c
    loads = [pltpu.make_async_copy(ref, w_buf.at[:, pl.ds(i * head_dim, head_dim)], load_sem.at[i]) for i, ref in enumerate((wq_ref, wk_ref, wv_ref))]
    loads += [pltpu.make_async_copy(step_cos_hbm, step_cos_ref, load_sem.at[3]), pltpu.make_async_copy(step_sin_hbm, step_sin_ref, load_sem.at[4])]
    own = pl.ds(pl.multiple_of(me * rows, 16), rows)
    greet(where)
    weights = WeightGather(w_o_ref, w_o_full, w_send, w_recv, local_sem, where)
    weights.keep().start()
    for load in loads:
        load.start()
    rows_buf[own, :] = scaled_norm(x_ref[...].astype(jnp.float32), flat_gain(gain_ref))
    meet(where)
    gather = RowGather(rows_buf, send_sem, recv_sem, where, weights)
    gather.start()
    for load in loads:
        load.wait()
    for r in range(base_cos_ref.shape[0]):
        first = prefix_ref[r]
        high, low = pl.ds(first // step_cos_ref.shape[0], 1), pl.ds(first % step_cos_ref.shape[0], 1)
        coarse_cos, coarse_sin, fine_cos, fine_sin = coarse_cos_ref[high, :], coarse_sin_ref[high, :], step_cos_ref[low, :], step_sin_ref[low, :]
        base_cos_ref[r:r + 1, :] = coarse_cos * fine_cos - coarse_sin * fine_sin
        base_sin_ref[r:r + 1, :] = coarse_sin * fine_cos + coarse_cos * fine_sin

    def compute(block):
        at = pl.ds(pl.multiple_of(block * rows, 16), rows)
        out = jnp.dot(rows_buf[at, :], w_buf[...], preferred_element_type=jnp.float32)
        bias = jnp.concatenate([ref[...].astype(jnp.float32) for ref in (bq_ref, bk_ref, bv_ref)], axis=1)
        out = (out + bias).astype(jnp.bfloat16)
        steps = pl.ds(pl.multiple_of(block * own_tokens, 8), own_tokens)
        step_cos, step_sin = step_cos_ref[steps, :][None], step_sin_ref[steps, :][None]
        base_cos, base_sin = base_cos_ref[...][:, None, :], base_sin_ref[...][:, None, :]
        cos_t = (base_cos * step_cos - base_sin * step_sin).reshape(rows, head_dim)
        sin_t = (base_sin * step_cos + base_cos * step_sin).reshape(rows, head_dim)
        lane = lax.broadcasted_iota(jnp.int32, (rows, head_dim), 1)
        sin_t = jnp.where(lane < head_dim // 2, -sin_t, sin_t)
        for ref, i in ((q_ref, 0), (k_ref, 1)):
            wide = out[:, i * head_dim:(i + 1) * head_dim].astype(jnp.float32)
            ref[at, :] = (wide * cos_t + pltpu.roll(wide, head_dim // 2, 1) * sin_t).astype(jnp.bfloat16)
        v_ref[at, :] = out[:, 2 * head_dim:]

    @pl.loop(0, LINE)
    def _(s):
        gather.step(s)
        pl.when(s == LINE - 1)(weights.swap_early)

        @pl.loop(*stage_chips(s))
        def _(n):
            at, line = chip_in_order(n, z, y)
            compute(at * 4 + line * 2 + c)
            twin = at * 4 + line * 2 + 1 - c
            gather.twin_arrived(twin)
            compute(twin)

    weights.finish()
    gather.drain()


def inverse_frequencies(head_dim):
    half = ROPE_THETA ** (-2.0 * np.arange(head_dim // 2) / head_dim)
    return np.concatenate([half, half])[None, :]


def project_all(x_rows, gain, w_q, w_k, w_v, biases, w_o, prefix, k_slots):
    n_req, own_tokens, width = x_rows.shape
    rows = n_req * own_tokens
    head_dim = w_q.shape[1]
    inv_freq = inverse_frequencies(head_dim)
    n_tokens = 16 * own_tokens
    step = np.arange(n_tokens)[:, None] * inv_freq
    coarse = np.arange(-(-k_slots // n_tokens))[:, None] * n_tokens * inv_freq
    step_cos, step_sin, coarse_cos, coarse_sin = (np.asarray(t, np.float32) for t in (np.cos(step), np.sin(step), np.cos(coarse), np.sin(coarse)))
    vmem = pl.BlockSpec(memory_space=pltpu.VMEM)
    hbm = pl.BlockSpec(memory_space=pltpu.HBM)
    out = jax.ShapeDtypeStruct((16 * rows, head_dim), jnp.bfloat16)
    dma = pltpu.SemaphoreType.DMA
    *outs, w_o_full = pl.pallas_call(
        project_body,
        out_shape=(out, out, out, jax.ShapeDtypeStruct((16 * w_o.shape[0], w_o.shape[1]), jnp.bfloat16)),
        in_specs=[vmem] * 2 + [hbm] * 3 + [vmem] * 3 + [pl.BlockSpec(memory_space=pltpu.SMEM)] + [vmem] * 2 + [hbm] * 2 + [vmem],
        out_specs=(vmem,) * 3 + (hbm,),
        scratch_shapes=[
            pltpu.VMEM((16 * rows, width), jnp.bfloat16),
            pltpu.VMEM((width, 3 * head_dim), jnp.bfloat16),
            dma((4,)), dma((16 * CHUNKS,)), dma((5,)), dma((32,)), dma, dma((5,)),
            pltpu.VMEM(step_cos.shape, jnp.float32), pltpu.VMEM(step_sin.shape, jnp.float32),
            pltpu.VMEM((n_req, head_dim), jnp.float32), pltpu.VMEM((n_req, head_dim), jnp.float32),
        ],
        compiler_params=pltpu.CompilerParams(collective_id=0, has_side_effects=True, vmem_limit_bytes=62 * 2**20),
        cost_estimate=pl.CostEstimate(flops=2 * 16 * rows * width * 3 * head_dim, bytes_accessed=4 * rows * width, transcendentals=0),
        name="project",
    )(x_rows.reshape(rows, width), gain.reshape(width // 128, 128), w_q, w_k, w_v, *biases, prefix, coarse_cos, coarse_sin, step_cos, step_sin, w_o)
    return tuple(o.reshape(16, n_req, own_tokens, head_dim) for o in outs), w_o_full


def token_rows(ref):
    rows = ref[:, 0].astype(jnp.float32)
    return rows.reshape(rows.shape[0] * rows.shape[1], rows.shape[2])


def attention_body(prefix_ref, valid_ref, q_ref, kn_ref, vn_ref, k_ref, v_ref, o_ref, ko_ref, vo_ref, scores, top, total, acc, staged, take_sem, put_sem):
    req = pl.program_id(0)
    start = prefix_ref[req]
    count = valid_ref[req]
    head_dim = q_ref.shape[3]
    n_tokens = q_ref.shape[0] * q_ref.shape[2]
    slots = k_ref.shape[1]
    last = pl.num_programs(0) - 1

    def take(r):
        return [pltpu.make_async_copy(ref.at[r], staged.at[r * 2 + i], take_sem.at[r * 2 + i]) for i, ref in enumerate((k_ref, v_ref))]

    def put(r):
        return [pltpu.make_async_copy(staged.at[r * 2 + i], ref.at[r], put_sem.at[r * 2 + i]) for i, ref in enumerate((ko_ref, vo_ref))]

    @pl.when(req == 0)
    def _():
        for move in take(0) + take(1):
            move.start()

    @pl.when(req + 2 <= last)
    def _():
        for move in take(req + 2):
            move.start()

    for move in take(req):
        move.wait()
    base = pl.multiple_of(jnp.minimum((start // 16) * 16, slots - UPDATE_ROWS), 16)
    shift = start - base
    row = lax.broadcasted_iota(jnp.int32, (UPDATE_ROWS, head_dim), 0) - shift
    keep = (row >= 0) & (row < count)
    for i, src in enumerate((kn_ref, vn_ref)):
        fresh = jnp.concatenate([token_rows(src), jnp.zeros((UPDATE_ROWS - n_tokens, head_dim), jnp.float32)], axis=0)
        fresh = pltpu.roll(fresh, shift, 0)
        old = staged[req * 2 + i, pl.ds(base, UPDATE_ROWS), :].astype(jnp.float32)
        staged[req * 2 + i, pl.ds(base, UPDATE_ROWS), :] = jnp.where(keep, fresh, old).astype(jnp.bfloat16)

    for move in put(req):
        move.start()
    n_open = (start + 1) // KV_BLOCK
    n_used = pl.cdiv(start + count, KV_BLOCK)
    queries = token_rows(q_ref).astype(jnp.bfloat16)
    lanes = KV_BLOCK // 128
    top[...] = jnp.full_like(top, -1.0e30)

    def score(blk, masked):
        keys = staged[req * 2, pl.ds(pl.multiple_of(blk * KV_BLOCK, KV_BLOCK), KV_BLOCK), :]
        s = lax.dot_general(queries, keys, (((1,), (1,)), ((), ())), preferred_element_type=jnp.float32)
        if masked:
            col = lax.broadcasted_iota(jnp.int32, (n_tokens, KV_BLOCK), 1) + blk * KV_BLOCK
            row_id = lax.broadcasted_iota(jnp.int32, (n_tokens, KV_BLOCK), 0)
            s = jnp.where(col <= start + jnp.minimum(row_id, count - 1), s, -1.0e30)
        scores[blk] = s
        best = top[...]
        for j in range(lanes):
            best = jnp.maximum(best, s[:, j * 128:(j + 1) * 128])
        top[...] = best

    pl.loop(0, n_open)(lambda blk: score(blk, False))
    pl.loop(n_open, n_used)(lambda blk: score(blk, True))
    top[...] = jnp.broadcast_to(jnp.max(top[...], axis=1, keepdims=True), top.shape)
    total[...] = jnp.zeros_like(total)
    acc[...] = jnp.zeros_like(acc)

    @pl.loop(0, n_used)
    def _(blk):
        best = top[...]
        part = total[...]
        pieces = []
        for j in range(lanes):
            e = jnp.exp2((scores[blk, :, j * 128:(j + 1) * 128] - best) * (LOG2_E * head_dim ** -0.5))
            part = part + e
            pieces.append(e.astype(jnp.bfloat16))
        total[...] = part
        vals = staged[req * 2 + 1, pl.ds(pl.multiple_of(blk * KV_BLOCK, KV_BLOCK), KV_BLOCK), :]
        acc[...] += jnp.dot(jnp.concatenate(pieces, axis=1), vals, preferred_element_type=jnp.float32)

    mixed = acc[...] / jnp.sum(total[...], axis=1, keepdims=True)
    o_ref[:, 0] = mixed.reshape(o_ref.shape[0], o_ref.shape[2], head_dim).astype(jnp.bfloat16)

    @pl.when(req == last)
    def _():
        for r in range(k_ref.shape[0]):
            for move in put(r):
                move.wait()


def attend(queries, keys_new, values_new, k_cache, v_cache, prefix, valid):
    owners, n_req, own_tokens, head_dim = queries.shape
    n_tokens = owners * own_tokens
    slots = k_cache.shape[1]
    new_spec = pl.BlockSpec((owners, 1, own_tokens, head_dim), lambda r, *_: (0, r, 0, 0))
    cache_spec = pl.BlockSpec(memory_space=pltpu.HBM)
    cache_out = jax.ShapeDtypeStruct(k_cache.shape, jnp.bfloat16)
    return pl.pallas_call(
        attention_body,
        out_shape=(jax.ShapeDtypeStruct(queries.shape, jnp.bfloat16), cache_out, cache_out),
        grid_spec=pltpu.PrefetchScalarGridSpec(
            num_scalar_prefetch=2,
            grid=(n_req,),
            in_specs=[new_spec, new_spec, new_spec, cache_spec, cache_spec],
            out_specs=(new_spec, cache_spec, cache_spec),
            scratch_shapes=[
                pltpu.VMEM((slots // KV_BLOCK, n_tokens, KV_BLOCK), jnp.float32),
                pltpu.VMEM((n_tokens, 128), jnp.float32),
                pltpu.VMEM((n_tokens, 128), jnp.float32),
                pltpu.VMEM((n_tokens, head_dim), jnp.float32),
                pltpu.VMEM((2 * n_req, slots, head_dim), jnp.bfloat16),
                pltpu.SemaphoreType.DMA((2 * n_req,)),
                pltpu.SemaphoreType.DMA((2 * n_req,)),
            ],
        ),
        compiler_params=pltpu.CompilerParams(dimension_semantics=("arbitrary",), vmem_limit_bytes=62 * 2**20),
        cost_estimate=pl.CostEstimate(flops=2 * 2 * n_req * n_tokens * slots * head_dim, bytes_accessed=8 * n_req * slots * head_dim, transcendentals=n_req * n_tokens * slots),
        name="attend",
    )(prefix, valid, queries, keys_new, values_new, k_cache, v_cache)


REDUCE = ((2, 3, 1, 0), (2, 3, 0, 1), (1, 0, 3, 2), (1, 0, 2, 3))


def finish_body(o_ref, x_ref, gain_ref, w_gate_hbm, w_up_hbm, w_down_hbm, w_o_ref, out_ref,
                rows_buf, part, swapped, attended, resid, acc, from_twin, from_line, from_lower, from_upper,
                gather_send, gather_recv, reduce_send, twin_recv, line_recv, lower_recv, upper_recv, swap_send, swap_recv, local_sem, w_gate_ref, w_up_ref, w_down_ref):
    where = place()
    dp, z, y, c = where
    rows, width = x_ref.shape
    head_dim = o_ref.shape[1]
    me = z * 4 + y * 2 + c
    piece = rows // CHUNKS
    load = pltpu.make_async_copy(w_o_ref, part.at[pl.ds(0, w_o_ref.shape[0])], local_sem.at[0])
    load.start()
    pairs = ((w_gate_hbm, w_gate_ref), (w_up_hbm, w_up_ref), (w_down_hbm, w_down_ref))
    mlp_loads = [pltpu.make_async_copy(src, dst, local_sem.at[1 + i]) for i, (src, dst) in enumerate(pairs)]
    for mlp_load in mlp_loads:
        mlp_load.start()
    barrier = pltpu.get_barrier_semaphore()
    for k in range(1, 16):
        pl.semaphore_signal(barrier, 1, device_id=(dp, (me + k) % 16), device_id_type=MESH_ID)
    pl.semaphore_wait(barrier, 15)

    def block_rows(block):
        return pl.ds(pl.multiple_of(block * rows, 16), rows)

    for k in range(1, 16):
        other = (me + k) % 16
        pltpu.make_async_remote_copy(
            src_ref=o_ref.at[block_rows(other)], dst_ref=swapped.at[block_rows(me)], send_sem=swap_send, recv_sem=swap_recv,
            device_id=(dp, other), device_id_type=MESH_ID).start()
    swapped[block_rows(me), :] = o_ref[block_rows(me), :]
    load.wait()
    others = o_ref.at[pl.ds(0, 15 * rows)]
    swap = pltpu.make_async_remote_copy(src_ref=others, dst_ref=others, send_sem=swap_send, recv_sem=swap_recv, device_id=(dp, 0), device_id_type=MESH_ID)
    swap.wait_recv()
    swap.wait_send()
    for head in range(16):
        attended[:, head * head_dim:(head + 1) * head_dim] = swapped[head * rows:(head + 1) * rows, :]

    @pl.loop(0, width // 512)
    def _(n):
        cols = pl.ds(pl.multiple_of(n * 512, 512), 512)
        out = jnp.dot(attended[...], part[pl.ds(0, w_o_ref.shape[0]), cols], preferred_element_type=jnp.float32).astype(jnp.bfloat16)
        resid[:, cols] = (x_ref[:, cols].astype(jnp.float32) + out.astype(jnp.float32)).astype(jnp.bfloat16)

    rows_buf[block_rows(me), :] = scaled_norm(resid[...].astype(jnp.float32), flat_gain(gain_ref))
    gather = RowGather(rows_buf, gather_send, gather_recv, where)
    gather.start()
    for mlp_load in mlp_loads:
        mlp_load.wait()

    def partial_sums(block):
        hidden = rows_buf[block_rows(block), :]
        dims = (((1,), (1,)), ((), ()))
        gate = lax.dot_general(hidden, w_gate_ref[...], dims, preferred_element_type=jnp.float32)
        up = lax.dot_general(hidden, w_up_ref[...], dims, preferred_element_type=jnp.float32)
        act = (jax.nn.silu(gate) * up).astype(jnp.bfloat16)
        part[block_rows(block), :] = jnp.dot(act, w_down_ref[...], preferred_element_type=jnp.float32).astype(jnp.bfloat16)

    def twin_copy(block, slot):
        return pltpu.make_async_remote_copy(
            src_ref=part.at[block_rows(block)], dst_ref=from_twin.at[block_rows(slot)], send_sem=reduce_send.at[TO_TWIN], recv_sem=twin_recv.at[slot],
            device_id=(dp, z * 4 + y * 2 + 1 - c), device_id_type=MESH_ID)

    last = CHUNKS - 1

    def piece_rows(block, j):
        return pl.ds(pl.multiple_of(block * rows + j * piece, 16), piece)

    def line_copy(dest, j):
        return pltpu.make_async_remote_copy(
            src_ref=part.at[piece_rows(dest * 4 + (1 - y) * 2 + c, j)], dst_ref=from_line.at[piece_rows(dest, j)],
            send_sem=reduce_send.at[TO_OTHER_LINE], recv_sem=line_recv.at[dest * CHUNKS + j],
            device_id=(dp, target(TO_OTHER_LINE, z, y, c)), device_id_type=MESH_ID)

    def slot(dest, line, j):
        far = jnp.where(line == y, dest * CHUNKS + j, LINE * CHUNKS + dest)
        return far, pl.ds(pl.multiple_of(far * piece, 16), piece)

    def along_copy(dest, line, j, way):
        index, land = slot(dest, line, j)
        buf, sems = (from_lower, lower_recv) if way == TO_UPPER else (from_upper, upper_recv)
        return pltpu.make_async_remote_copy(
            src_ref=part.at[piece_rows(dest * 4 + line * 2 + c, j)], dst_ref=buf.at[land],
            send_sem=reduce_send.at[way], recv_sem=sems.at[index], device_id=(dp, target(way, z, y, c)), device_id_type=MESH_ID)

    def line_send(dest):
        for j in range(ALONG_FIRST):
            line_copy(dest, j).start()

    def chips(lo, hi):
        @pl.loop(lo, hi)
        def _(n):
            at, line = chip_in_order(n, z, y)
            block = at * 4 + line * 2 + c
            twin = at * 4 + line * 2 + 1 - c
            gather.twin_arrived(twin)
            partial_sums(twin)
            twin_copy(twin, at * 2 + line).start()
            partial_sums(block)
            twin_copy(block, at * 2 + line).wait_recv()
            total = part[block_rows(block), :].astype(jnp.float32) + from_twin[block_rows(at * 2 + line), :].astype(jnp.float32)
            part[block_rows(block), :] = total.astype(jnp.bfloat16)

    def add_along(dest, line, j):
        _, land = slot(dest, line, j)

        @pl.when((dest >= z) & (z > 0))
        def _():
            along_copy(dest, line, j, TO_UPPER).wait_recv()
            acc[...] += from_lower[land, :].astype(jnp.float32)

        @pl.when((dest <= z) & (z < LINE - 1))
        def _():
            along_copy(dest, line, j, TO_LOWER).wait_recv()
            acc[...] += from_upper[land, :].astype(jnp.float32)

        @pl.when((dest != z) | (j == last))
        def _():
            part[piece_rows(dest * 4 + line * 2 + c, j), :] = acc[...].astype(jnp.bfloat16)

        pl.when(dest > z)(lambda: along_copy(dest, line, j, TO_UPPER).start())
        pl.when(dest < z)(lambda: along_copy(dest, line, j, TO_LOWER).start())

    def result(j):
        out = pl.ds(pl.multiple_of(j * piece, 16), piece)
        down = acc[...].astype(jnp.bfloat16).astype(jnp.float32)
        out_ref[out, :] = (resid[out, :].astype(jnp.float32) + down).astype(jnp.bfloat16)

    at_end = (z == 0) | (z == LINE - 1)

    def last_piece(step):
        dest = chip_at(REDUCE, z, step // 2)
        line = (y + 1 + step) % 2
        acc[...] = part[piece_rows(dest * 4 + line * 2 + c, last), :].astype(jnp.float32)
        add_along(dest, line, last)
        pl.when((dest == z) & (line != y))(lambda: line_copy(dest, last).start())

    def before_last():
        line_send(chip_at(REDUCE, z, 0))

        @pl.when(at_end)
        def _():
            last_piece(0)
            last_piece(1)
            last_piece(3)

    @pl.loop(0, LINE)
    def _(s):
        pl.when(s == LINE - 1)(before_last)
        gather.step(s)
        chips(*stage_chips(s))

    for i in range(1, LINE):
        line_send(chip_at(REDUCE, z, i))

    @pl.loop(0, 2 * LINE - 2)
    def _(step):
        pl.when(jnp.logical_not(at_end) | (step == 2) | (step >= 4))(lambda: last_piece(step))

    @pl.loop(0, LINE * ALONG_FIRST + 2)
    def _(n):
        swing = (LINE - 1) * ALONG_FIRST

        @pl.when((n >= swing) & (n < swing + 2))
        def _():
            last_piece(2 * LINE - 2 + n - swing)

        @pl.when((n < swing) | (n >= swing + 2))
        def _():
            step = jnp.where(n < swing, n, n - 2)
            dest = chip_at(REDUCE, z, step // ALONG_FIRST)
            j = step % ALONG_FIRST
            line_copy(dest, j).wait_recv()
            acc[...] = part[piece_rows(dest * 4 + y * 2 + c, j), :].astype(jnp.float32) + from_line[piece_rows(dest, j), :].astype(jnp.float32)
            add_along(dest, y, j)
            pl.when(dest == z)(lambda: result(j))

    line_copy(z, last).wait_recv()
    acc[...] = part[piece_rows(me, last), :].astype(jnp.float32) + from_line[piece_rows(z, last), :].astype(jnp.float32)
    result(last)
    gather.drain()

    def sent(way, pieces):
        span = pl.ds(0, pieces * piece)
        pltpu.make_async_remote_copy(
            src_ref=part.at[span], dst_ref=part.at[span], send_sem=reduce_send.at[way], recv_sem=twin_recv.at[0],
            device_id=(dp, 0), device_id_type=MESH_ID).wait_send()

    for zc in range(LINE):

        @pl.when(z == zc)
        def _(zc=zc):
            if zc < LINE - 1:
                sent(TO_UPPER, (LINE - 1 - zc) * (CHUNKS + 1))
            if zc > 0:
                sent(TO_LOWER, zc * (CHUNKS + 1))

    sent(TO_OTHER_LINE, LINE * ALONG_FIRST + 1)
    sent(TO_TWIN, 2 * LINE * CHUNKS)


def finish(attended, x_rows, gain, w_gate, w_up, w_down, w_o):
    n_req, own_tokens, width = x_rows.shape
    rows = n_req * own_tokens
    head_dim = attended.shape[-1]
    vmem = pl.BlockSpec(memory_space=pltpu.VMEM)
    bf16, f32 = jnp.bfloat16, jnp.float32
    dma = pltpu.SemaphoreType.DMA
    out = pl.pallas_call(
        finish_body,
        out_shape=jax.ShapeDtypeStruct((rows, width), bf16),
        in_specs=[vmem] * 3 + [pl.BlockSpec(memory_space=pltpu.HBM)] * 4,
        out_specs=vmem,
        scratch_shapes=[
            pltpu.VMEM((16 * rows, width), bf16),
            pltpu.VMEM((16 * rows, width), bf16),
            pltpu.VMEM((16 * rows, head_dim), bf16),
            pltpu.VMEM((rows, width), bf16),
            pltpu.VMEM((rows, width), bf16),
            pltpu.VMEM((rows // CHUNKS, width), f32),
            pltpu.VMEM((8 * rows, width), bf16),
            pltpu.VMEM((LINE * rows, width), bf16),
            pltpu.VMEM((LINE * (rows + rows // CHUNKS), width), bf16),
            pltpu.VMEM((LINE * (rows + rows // CHUNKS), width), bf16),
            dma((4,)), dma((16 * CHUNKS,)), dma((4,)), dma((8,)), dma((LINE * CHUNKS,)), dma((LINE * (CHUNKS + 1),)), dma((LINE * (CHUNKS + 1),)), dma, dma, dma((4,)),
            pltpu.VMEM(w_gate.T.shape, bf16), pltpu.VMEM(w_up.T.shape, bf16), pltpu.VMEM(w_down.shape, bf16),
        ],
        compiler_params=pltpu.CompilerParams(collective_id=1, has_side_effects=True, vmem_limit_bytes=62 * 2**20),
        cost_estimate=pl.CostEstimate(flops=2 * rows * width * (width + 16 * 3 * w_down.shape[0]), bytes_accessed=4 * width * width, transcendentals=0),
        name="finish",
    )(attended.reshape(16 * rows, head_dim), x_rows.reshape(rows, width), gain.reshape(width // 128, 128), w_gate.T, w_up.T, w_down, w_o)
    return out.reshape(x_rows.shape)


def solution(mesh):
    row_spec = P("dp", "tp", None)
    cache_spec = P("dp", None, "tp", None)
    req_spec = P("dp")
    rep_spec = P(None)
    col_spec = P(None, "tp")
    bias_spec = P("tp")
    down_spec = P("tp", None)

    def layer(x_rows, k_cache, v_cache, prefix, valid, g_attn, w_q, b_q, w_k, b_k, w_v, b_v, w_o, g_mlp, w_gate, w_up, w_down):
        biases = [b.reshape(1, -1) for b in (b_q, b_k, b_v)]
        (queries, keys_new, values_new), w_o_full = project_all(x_rows, g_attn, w_q, w_k, w_v, biases, w_o, prefix, k_cache.shape[1])
        flat = (k_cache.shape[0], k_cache.shape[1], k_cache.shape[3])
        attended, k_out, v_out = attend(queries, keys_new, values_new, k_cache.reshape(flat), v_cache.reshape(flat), prefix, valid)
        x_out = finish(attended, x_rows, g_mlp, w_gate, w_up, w_down, w_o_full)
        return x_out, k_out.reshape(k_cache.shape), v_out.reshape(v_cache.shape)

    in_specs = (row_spec, cache_spec, cache_spec, req_spec, req_spec, rep_spec, col_spec, bias_spec, col_spec, bias_spec, col_spec, bias_spec, down_spec, rep_spec, col_spec, col_spec, down_spec)
    return jax.shard_map(layer, mesh=mesh, in_specs=in_specs, out_specs=(row_spec, cache_spec, cache_spec), check_vma=False)
```
